32 devices in a mesh: scene: 2 (over y), tile: 4 (over z), half: 2 (over x), band: 2 (over core).
Axes of the slice: x: 2, y: 2, z: 4, core: 2. Of those that a mesh axis runs over, the one named last changes fastest.
Arguments:
- optical: bfloat16 [16, 2, 512, 512], P(('scene', 'tile'), 'band', 'half'), parts along dimension 0, may hold values from -64 to 64
- sar: bfloat16 [2, 8192, 512], P('band', ('scene', 'tile', 'half')), parts along dimension 1, may hold values from -64 to 64
- destination: int32 [128], P('scene'), parts along dimension 0, may hold values from 0 to 63, as said below
- peaks: int32 [16, 2, 8], P(('scene', 'tile', 'band')), parts along dimension 0, may hold values from 0 to 511
Outputs:
- surface: float32 [16, 512, 512], P(('scene', 'tile', 'band'), 'half'), parts along dimension 0
- peak_values: float32 [16, 8], P(('scene', 'tile', 'band')), parts along dimension 0
The draws below stay inside these ranges and needn't reach their ends.
There are 2 independent parts, one for each index of `scene`. The reference program is written for one: setup_inputs(seed, part) draws one part's arguments, and reference() takes and returns one part's arrays. A program takes and returns all parts, laid end to end along the dimension named above; each array names one. Nothing has to cross between parts.
Inputs may be any that keep to these rules, and one draw needn't show every extreme that they name: destination holds every block position 0 to 63 once; the 8 blocks that start at each multiple of 8 are sent one into each run of 8 positions that starts at a multiple of 8.
All inputs are finite; a program needn't handle non-finite values.
Results may differ from the reference program's by a relative error of at most 0.014.
Values may be sent and summed in bfloat16 or wider, within the bound.
A program may use at most 64 MiB of HBM per device.

```python
import math
import jax
import jax.numpy as jnp
from jax import lax

PATCH_SIZE = 512
BAND_COUNT = 2
PATCH_DEV = 2
PEAK_COUNT = 8
PATCHES = 8
GROUP_DEVICES = 8
BLOCK_LINES = 64
BLOCKS = 64
SLANT_LINES = 4096
N_TILE = 4
N_HALF = 2


def one_order(subkey):
    return jax.random.permutation(subkey, GROUP_DEVICES).astype(jnp.int32)


def draw_destination(key, part):
    subkeys = jax.random.split(jax.random.fold_in(key, 7), 2)
    sending = jax.vmap(one_order)(jax.random.split(subkeys[0], GROUP_DEVICES))
    slotting = jax.vmap(one_order)(jax.random.split(subkeys[1], GROUP_DEVICES))
    senders = jnp.arange(GROUP_DEVICES, dtype=jnp.int32)[:, None]
    slot_index = slotting[sending, senders]
    return (sending * GROUP_DEVICES + slot_index).reshape(BLOCKS).astype(jnp.int32)


def draw_optical(key, part):
    full_shape = (PATCHES, BAND_COUNT, PATCH_SIZE, PATCH_SIZE)
    line_frac = jnp.arange(PATCH_SIZE, dtype=jnp.float32)[:, None] / (PATCH_SIZE - 1)
    subkeys = jax.random.split(jax.random.fold_in(key, 3), 1)
    noise_draw = jnp.clip(jax.random.normal(subkeys[0], full_shape, jnp.float32), -5.0, 5.0)
    values = noise_draw * jnp.exp(math.log(3.0) * line_frac - 0.5 * math.log(3.0))
    return values.astype(jnp.bfloat16)


def draw_sar(key, part):
    full_shape = (BAND_COUNT, SLANT_LINES, PATCH_SIZE)
    line_frac = jnp.arange(SLANT_LINES, dtype=jnp.float32)[:, None] / (SLANT_LINES - 1)
    subkeys = jax.random.split(jax.random.fold_in(key, 5), 1)
    noise_draw = jnp.clip(jax.random.normal(subkeys[0], full_shape, jnp.float32), -5.0, 5.0)
    values = noise_draw * jnp.exp(math.log(3.0) * line_frac - 0.5 * math.log(3.0))
    return values.astype(jnp.bfloat16)


def place_ends(entries, own_key, low, high):
    index_at = [jax.random.randint(jax.random.fold_in(own_key, axis), (), 0, length) for axis, length in enumerate(entries.shape)]
    longest = entries.shape.index(max(entries.shape))
    neighbour = index_at[:longest] + [(index_at[longest] + 1) % entries.shape[longest]] + index_at[longest + 1:]
    return entries.at[tuple(index_at)].set(low).at[tuple(neighbour)].set(high)


def setup_inputs(seed: int = 0, part: int = 0) -> dict:
    key_list = jax.random.split(jax.random.key(seed), 5)
    part_splits = jax.random.split(jax.random.fold_in(key_list[4], part), 5)
    optical = draw_optical(jax.random.fold_in(jax.random.fold_in(key_list[4], part), 71), part)
    sar = draw_sar(jax.random.fold_in(jax.random.fold_in(key_list[4], part), 71), part)
    destination = draw_destination(jax.random.fold_in(jax.random.fold_in(key_list[4], part), 71), part)
    peaks = place_ends(jax.random.randint(part_splits[3], (PATCHES, 2, PEAK_COUNT), 0, PATCH_SIZE), jax.random.fold_in(part_splits[3], 1), 0, PATCH_SIZE - 1).astype(jnp.int32)
    return dict(optical=optical, sar=sar, destination=destination, peaks=peaks)


EPSILON = 1e-06

def column_pair(samples):
    spectrum = jnp.fft.fft(samples.astype(jnp.float32), axis=-1)
    return (jnp.real(spectrum).astype(jnp.bfloat16), jnp.imag(spectrum).astype(jnp.bfloat16))

def line_spectrum(samples):
    real_part, imag_part = column_pair(samples)
    joined = real_part.astype(jnp.float32) + 1j * imag_part.astype(jnp.float32)
    spectrum = jnp.fft.fft(joined, axis=-2)
    return spectrum.at[..., 0, 0].set(0.0)

def band_energy(samples):
    values = samples.astype(jnp.float32)
    total_sums = lax.optimization_barrier(jnp.sum(values, axis=(2, 3)))
    squares = lax.optimization_barrier(jnp.sum(values * values, axis=(2, 3)))
    pixel_count = PATCH_SIZE * PATCH_SIZE
    centered = squares - total_sums * total_sums / pixel_count
    return lax.optimization_barrier(jnp.sum(centered, axis=1)) / (BAND_COUNT * pixel_count)

def reference(optical, sar, destination, peaks):
    blocks = sar.reshape(BAND_COUNT, BLOCKS, BLOCK_LINES, PATCH_SIZE)
    placed = jnp.zeros_like(blocks).at[:, destination].set(blocks)
    sar_map = placed.reshape(BAND_COUNT, N_TILE, N_HALF, PATCH_DEV, PATCH_SIZE // N_HALF, PATCH_SIZE)
    sar_map = jnp.transpose(sar_map, (1, 3, 0, 2, 4, 5)).reshape(PATCHES, BAND_COUNT, PATCH_SIZE, PATCH_SIZE)
    opt_spec = line_spectrum(optical)
    sar_spec = line_spectrum(sar_map)
    opt_energy = band_energy(optical)
    sar_energy = band_energy(sar_map)
    cross_sum = lax.optimization_barrier(jnp.sum(jnp.conj(opt_spec) * sar_spec, axis=1))
    correlation = jnp.real(jnp.fft.ifft2(cross_sum, axes=(-2, -1)))
    pixel_count = PATCH_SIZE * PATCH_SIZE
    norm_scale = lax.rsqrt(BAND_COUNT * pixel_count * (opt_energy + EPSILON) * (sar_energy + EPSILON))
    surface = (correlation * norm_scale[:, None, None]).astype(jnp.float32)
    flattened = surface.reshape(PATCHES, pixel_count)
    spots = (peaks[:, 0, :] * PATCH_SIZE + peaks[:, 1, :]).astype(jnp.int32)
    peak_values = jnp.take_along_axis(flattened, spots, axis=1)
    return (surface, peak_values)
```

```python
import functools
import math

import jax
import jax.numpy as jnp
import numpy as np
from jax import lax
from jax.experimental import pallas as pl
from jax.experimental.pallas import tpu as pltpu
from jax.sharding import PartitionSpec as P

MESH = pl.DeviceIdType.MESH

precise = lax.Precision.HIGHEST
EPSILON = 1e-06


def fourier_tables(extent):
    places = jnp.arange(extent, dtype=jnp.int32)
    phases = places[:, None] * places[None, :] % extent
    angles = phases.astype(jnp.float32) * (2.0 * math.pi / extent)
    return (jnp.cos(angles), jnp.sin(angles))


def fourier_pair(table):
    upper = table.astype(jnp.bfloat16)
    lower = (table - upper.astype(jnp.float32)).astype(jnp.bfloat16)
    return (upper, lower)


def column_spectrum(samples, table_upper, table_lower):
    extent = samples.shape[-1]
    values = samples.reshape(-1, extent)
    spectrum = jnp.dot(values, table_upper, preferred_element_type=jnp.float32) + jnp.dot(
        values, table_lower, preferred_element_type=jnp.float32
    )
    return spectrum.astype(jnp.bfloat16).reshape(samples.shape[:-1] + (2 * extent,))


def row_spectrum(columns, table_upper, table_lower):
    line_count = columns.shape[-3]
    stacked = jnp.concatenate([columns[..., 0, :], columns[..., 1, :]], axis=-2)
    result = jnp.einsum("kr,...rc->...kc", table_upper, stacked, preferred_element_type=jnp.float32)
    result = result + jnp.einsum(
        "kr,...rc->...kc", table_lower, stacked, preferred_element_type=jnp.float32
    )
    return (result[..., :line_count, :], result[..., line_count:, :])


def relay_blocks(parcel):
    layout = parcel.shape
    merged = parcel.reshape(layout[:1] + (layout[1] * layout[2],) + layout[3:])
    arrived = lax.all_to_all(merged, ("tile", "half"), split_axis=1, concat_axis=1, tiled=True)
    return arrived.reshape(layout)


def generic(optical, sar, destination, peaks):
    tile_count = lax.axis_size("tile")
    half_count = lax.axis_size("half")
    band_count = lax.axis_size("band")
    group_size = tile_count * half_count
    patch_dev, local_bands, quarter, extent = optical.shape
    col_width = extent // half_count
    block_lines = sar.shape[1] // group_size
    band_total = local_bands * band_count
    pixel_count = extent * extent
    patch_total = patch_dev * tile_count
    kept_patches = patch_dev // band_count
    cosine_table, sine_table = fourier_tables(extent)
    col_upper, col_lower = fourier_pair(jnp.concatenate([cosine_table, -sine_table], axis=1))
    row_full = jnp.concatenate(
        [
            jnp.concatenate([cosine_table, sine_table], axis=1),
            jnp.concatenate([-sine_table, cosine_table], axis=1),
        ],
        axis=0,
    )
    row_upper, row_lower = fourier_pair(row_full)
    tile_at = lax.axis_index("tile")
    half_at = lax.axis_index("half")
    band_at = lax.axis_index("band")
    device_at = lax.axis_index(("tile", "half"))
    own_blocks = lax.dynamic_slice_in_dim(destination, device_at * group_size, group_size)
    send_order = jnp.argsort(own_blocks // group_size)
    inverse = (
        jnp.zeros_like(destination)
        .at[destination]
        .set(jnp.arange(destination.shape[0], dtype=jnp.int32))
    )
    opt_values = optical.astype(jnp.float32)
    opt_sums = jnp.sum(opt_values, axis=(2, 3))
    opt_squares = jnp.sum(opt_values * opt_values, axis=(2, 3))
    sar_values = sar.astype(jnp.float32).reshape(local_bands, group_size, block_lines * extent)
    sar_sums = jnp.sum(sar_values, axis=2)
    sar_squares = jnp.sum(sar_values * sar_values, axis=2)
    map_device = own_blocks // group_size
    map_patch = (
        map_device // half_count * patch_dev + own_blocks % group_size * block_lines // quarter
    )
    member = (map_patch[:, None] == jnp.arange(patch_total, dtype=jnp.int32)[None, :]).astype(
        jnp.float32
    )
    sar_stats = jnp.dot(
        jnp.stack([sar_sums, sar_squares]).reshape(2 * local_bands, group_size),
        member,
        precision=precise,
        preferred_element_type=jnp.float32,
    )
    statistics = jnp.zeros((2, 2, band_total, patch_total), jnp.float32)
    opt_part = jnp.transpose(jnp.stack([opt_sums, opt_squares]), (0, 2, 1))
    statistics = lax.dynamic_update_slice(
        statistics, opt_part[None], (0, 0, band_at * local_bands, tile_at * patch_dev)
    )
    statistics = lax.dynamic_update_slice(
        statistics,
        sar_stats.reshape(2, local_bands, patch_total)[None],
        (1, 0, band_at * local_bands, 0),
    )
    totals = lax.psum(statistics, ("tile", "half", "band"))
    centered = totals[:, 1] - totals[:, 0] * totals[:, 0] / pixel_count
    energy = jnp.sum(centered, axis=1) / (band_total * pixel_count)
    norm_scale = lax.rsqrt(band_total * pixel_count * (energy[0] + EPSILON) * (energy[1] + EPSILON))
    first_patch = tile_at * patch_dev + band_at * kept_patches
    norm_mine = lax.dynamic_slice_in_dim(norm_scale, first_patch, kept_patches)
    slant_spectra = column_spectrum(sar, col_upper, col_lower).reshape(
        local_bands, group_size, block_lines, 2, half_count, col_width
    )
    outgoing = jnp.take(slant_spectra, send_order, axis=1).reshape(
        local_bands, tile_count, half_count, block_lines, 2, half_count, col_width
    )
    outgoing = jnp.transpose(outgoing, (0, 1, 5, 2, 3, 4, 6))
    arrived = relay_blocks(outgoing).reshape(
        local_bands, group_size * half_count, block_lines, 2, col_width
    )
    sources = lax.dynamic_slice_in_dim(
        inverse, tile_at * half_count * group_size, half_count * group_size
    )
    slot_index = (
        sources // group_size * half_count
        + jnp.arange(half_count * group_size, dtype=jnp.int32) // group_size
    )
    placed = jnp.take(arrived, slot_index, axis=1).reshape(
        local_bands, half_count, patch_dev, quarter, 2, col_width
    )
    placed = jnp.transpose(placed, (2, 0, 1, 3, 4, 5)).reshape(
        patch_dev, local_bands, extent, 2, col_width
    )
    sar_real, sar_imag = row_spectrum(placed, row_upper, row_lower)
    spectra = column_spectrum(optical, col_upper, col_lower).reshape(
        patch_dev, local_bands, quarter, 2, half_count, col_width
    )
    real_part, imag_part = row_spectrum(
        jnp.squeeze(
            lax.all_to_all(spectra, "half", split_axis=4, concat_axis=2, tiled=True), axis=4
        ),
        row_upper,
        row_lower,
    )
    opt_real = real_part
    opt_imag = imag_part
    rows_at = jnp.arange(extent, dtype=jnp.int32)[:, None]
    cols_at = half_at * col_width + jnp.arange(col_width, dtype=jnp.int32)[None, :]
    keep_mask = jnp.where((rows_at == 0) & (cols_at == 0), 0.0, 1.0).astype(jnp.float32)
    opt_real = opt_real * keep_mask
    opt_imag = opt_imag * keep_mask
    sar_real = sar_real * keep_mask
    sar_imag = sar_imag * keep_mask
    cross_real = jnp.sum(opt_real * sar_real + opt_imag * sar_imag, axis=1)
    cross_imag = jnp.sum(opt_real * sar_imag - opt_imag * sar_real, axis=1)
    cross_term = jnp.stack([cross_real, cross_imag], axis=1)
    cross_sum = lax.psum_scatter(cross_term, "band", scatter_dimension=0, tiled=True)
    lag_real = (
        jnp.einsum("uk,pkc->puc", cosine_table, cross_sum[:, 0], precision=precise)
        - jnp.einsum("uk,pkc->puc", sine_table, cross_sum[:, 1], precision=precise)
    ) / extent
    lag_imag = (
        jnp.einsum("uk,pkc->puc", cosine_table, cross_sum[:, 1], precision=precise)
        + jnp.einsum("uk,pkc->puc", sine_table, cross_sum[:, 0], precision=precise)
    ) / extent
    lagged = jnp.stack([lag_real, lag_imag], axis=2).reshape(
        kept_patches, half_count, quarter, 2, col_width
    )
    pieces = lax.all_to_all(lagged, "half", split_axis=1, concat_axis=4, tiled=True)
    real_in = pieces[:, 0, :, 0, :]
    imag_in = pieces[:, 0, :, 1, :]
    correlation = (
        jnp.einsum("puc,cv->puv", real_in, cosine_table, precision=precise)
        - jnp.einsum("puc,cv->puv", imag_in, sine_table, precision=precise)
    ) / extent
    surface = correlation * norm_mine[:, None, None]
    local_rows = peaks[:, 0, :] - half_at * quarter
    row_hit = (
        local_rows[:, :, None] == jnp.arange(quarter, dtype=jnp.int32)[None, None, :]
    ).astype(jnp.float32)
    picked = jnp.einsum("pkr,prc->pkc", row_hit, surface, precision=precise)
    col_hit = (peaks[:, 1, :, None] == jnp.arange(extent, dtype=jnp.int32)[None, None, :]).astype(
        jnp.float32
    )
    local_values = jnp.sum(picked * col_hit, axis=2)
    peak_values = lax.psum(local_values, "half")
    return (surface, peak_values)


def dft_tables(extent, parts):
    points = extent // 2
    cols = points // parts // 2
    places = np.arange(extent)
    phases = (places[:, None] * places[None, :]) % extent
    cosine = np.cos(phases * (2.0 * np.pi / extent))
    sine = np.sin(phases * (2.0 * np.pi / extent))
    forward, backward = [], [[], []]
    for part in range(parts):
        for turn in range(2):
            first = (2 * part + turn) * cols
            span = slice(first, first + cols)
            real, imag = cosine[:, span].copy(), -sine[:, span]
            real_back, imag_back = 2.0 * cosine[span], -2.0 * sine[span]
            if first == 0:
                imag[:, 0] = cosine[:, points]
                real_back[0] = 1.0
                imag_back[0] = cosine[points]
            forward += [real, imag]
            backward[turn] += [real_back, imag_back]
    col_table = np.concatenate(forward, axis=1)
    back_table = np.stack([np.concatenate(b, axis=0) for b in backward])
    row_sine = sine[:points, :points].copy()
    row_sine[0] = cosine[points, :points]
    row_table = np.concatenate([cosine[:points, :points], row_sine], axis=0)
    lag_cosine, lag_sine = 2.0 * cosine[:, :points], 2.0 * sine[:, :points]
    lag_cosine[:, 0] = 1.0
    lag_sine[:, 0] = cosine[:, points]
    lag_table = np.concatenate([lag_cosine, lag_sine], axis=1)
    return tuple(t.astype(jnp.bfloat16) for t in (col_table, row_table, lag_table, back_table))


def kernel(
    sizes,
    dest_hbm,
    peaks_hbm,
    sar_hbm,
    opt_hbm,
    col_hbm,
    row_hbm,
    lag_hbm,
    back_hbm,
    surface_ref,
    total_ref,
    dest_ref,
    peaks_ref,
    sar_v,
    opt_v,
    col_v,
    row_v,
    lag_v,
    back_v,
    send_0,
    send_1,
    arrived_0,
    arrived_1,
    opt_send,
    opt_in,
    opt_waves,
    sar_cols,
    sar_rows,
    cross,
    lags,
    lag_send,
    lag_in,
    spot_send,
    spot_recv,
    last_mine,
    last_other,
    last_in,
    load_sem,
    sar_ssem,
    sar_rsem,
    opt_ssem,
    opt_rsem,
    lag_ssem,
    lag_rsem,
    last_ssem,
    last_rsem,
    spot_ssem,
    spot_rsem,
    near_sem,
    far_sem,
):
    tiles, halves, bands, patch_dev, quarter, extent, lines, peak_count = sizes
    group = tiles * halves
    parts = halves * bands
    wide = extent // parts
    side = wide // 2
    cols = wide // 4
    points = extent // 2
    per_patch = group // patch_dev
    send, arrived = (send_0, send_1), (arrived_0, arrived_1)
    f32, bf = jnp.float32, jnp.bfloat16
    tile, half, band = lax.axis_index("tile"), lax.axis_index("half"), lax.axis_index("band")
    me = tile * halves + half
    part = half * bands + band
    other_half = 1 - half
    other_band = 1 - band

    def place(step, shift, swap):
        return (
            lax.rem(tile + step, tiles),
            lax.rem(half + shift, halves),
            lax.rem(band + swap, bands),
        )

    def device(step, shift, swap):
        return dict(zip(("tile", "half", "band"), place(step, shift, swap)))

    others = tiles * parts - 1
    near = [(0, shift, swap) for shift in (1, 0) for swap in range(bands) if shift or swap]

    loads = [
        pltpu.make_async_copy(a, b, load_sem.at[i])
        for i, (a, b) in enumerate(
            [(dest_hbm, dest_ref), (sar_hbm, sar_v), (col_hbm, col_v), (opt_hbm, opt_v),
             (row_hbm, row_v), (peaks_hbm, peaks_ref), (lag_hbm, lag_v), (back_hbm, back_v)]
        )
    ]
    for i in (3, 2, 0, 1):
        loads[i].start()

    barrier = pltpu.get_barrier_semaphore()
    first_band, last_band = jnp.int32(0), jnp.int32(bands - 1)

    def tell(semaphore, **where):
        pl.semaphore_signal(semaphore, inc=1, device_id=where, device_id_type=MESH)

    for shift in range(1, halves):
        tell(barrier, half=lax.rem(half + shift, halves), band=first_band)
    pl.when(band != first_band)(lambda: tell(barrier, band=first_band))
    for step in sorted(range(1, tiles), key=lambda s: -min(s, tiles - s)):
        for shift in range(halves):
            tell(
                barrier,
                tile=lax.rem(tile + step, tiles),
                half=lax.rem(half + shift, halves),
                band=last_band,
            )

    def remote(src, dst, ssem, rsem, peer):
        return pltpu.make_async_remote_copy(
            src_ref=src,
            dst_ref=dst,
            send_sem=ssem,
            recv_sem=rsem,
            device_id=device(*peer),
            device_id_type=MESH,
        )

    source_at = me * bands + band

    def sar_copy(turn, to_tile, to_half, to_band):
        return pltpu.make_async_remote_copy(
            src_ref=send[turn].at[to_tile * parts + to_half * bands + to_band],
            dst_ref=arrived[turn].at[source_at],
            send_sem=sar_ssem.at[turn],
            recv_sem=sar_rsem.at[turn],
            device_id={"tile": to_tile, "half": to_half, "band": to_band},
            device_id_type=MESH,
        )

    low = lax.broadcasted_iota(jnp.int32, (1, wide), 1) < side

    def pair(a, b):
        first = jnp.concatenate([a[:, :side], b[:, :side]], axis=1)
        second = jnp.concatenate([a[:, side:], b[:, side:]], axis=1)
        return first, second

    def whole(ref, count, ssem, rsem):
        ref = ref.at[pl.ds(0, count)]
        return remote(ref, ref, ssem, rsem, (0, 1, 0))

    loads[0].wait()
    own_runs = [lax.div(dest_ref[me * group + j], group) for j in range(group)]

    def block_for(run):
        found = jnp.int32(0)
        for j in range(group):
            found = jnp.where(own_runs[j] == run, j, found)
        return found

    def sar_columns(to_tile):
        if to_tile == 0:
            loads[1].wait()
        samples = jnp.concatenate(
            [sar_v[block_for(to_tile * halves + run)] for run in range(halves)], axis=0
        )
        spectra = jnp.dot(samples, col_v[...], preferred_element_type=f32).astype(bf)
        for to in range(parts):
            at = slice(to * wide, (to + 1) * wide)
            first, second = pair(spectra[:lines, at], spectra[lines:, at])
            send_0[to_tile * parts + to] = first
            send_1[to_tile * parts + to] = second

    def sar_sends(turn, to_tile, shifts):
        for shift in shifts:
            to_half = lax.rem(half + shift, halves)
            for swap in range(bands):
                to_band = lax.rem(band + swap, bands)
                copy = sar_copy(turn, to_tile, to_half, to_band)
                if shift or swap:
                    copy.start()
                else:
                    pl.when(tile != to_tile)(copy.start)

    def opt_copy(turn, peer):
        _, to_half, to_band = place(*peer)
        return remote(
            opt_send.at[turn, to_half * bands + to_band],
            opt_in.at[turn, part],
            opt_ssem.at[turn],
            opt_rsem.at[turn],
            peer,
        )

    def opt_sends(turn):
        for peer in near:
            opt_copy(turn, peer).start()

    loads[3].wait()
    loads[2].wait()
    opt_spectra = [
        jnp.dot(opt_v[patch], col_v[...], preferred_element_type=f32).astype(bf)
        for patch in range(patch_dev)
    ]
    for to in range(parts):
        at = slice(to * wide, (to + 1) * wide)
        first, second = pair(*[s[:, at] for s in opt_spectra])
        opt_send[0, to] = first
        opt_send[1, to] = second
    @pl.when(band == first_band)
    def _():
        pl.semaphore_wait(barrier, parts - 1)
        tell(near_sem, band=last_band)

    @pl.when(band == last_band)
    def _():
        pl.semaphore_wait(near_sem, 1)

    opt_sends(0)
    opt_sends(1)
    sar_columns(0)
    for i in (4, 5, 6, 7):
        loads[i].start()

    @pl.when(band == last_band)
    def _():
        pl.semaphore_wait(barrier, (tiles - 1) * parts)
        tell(far_sem, band=first_band)

    @pl.when(band == first_band)
    def _():
        pl.semaphore_wait(far_sem, 1)

    sar_sends(0, 0, (0, 1))
    for to_tile in range(1, tiles):
        sar_columns(to_tile)
        sar_sends(0, to_tile, (0, 1))
    for to_tile in range(tiles):
        sar_sends(1, to_tile, (0,))
    arrived_0[source_at] = send_0[tile * parts + part]
    arrived_1[source_at] = send_1[tile * parts + part]
    for turn in range(2):
        opt_in[turn, part] = opt_send[turn, part]

    slot_of = []
    for run in range(halves):
        places = []
        for source in range(group):
            found = jnp.int32(0)
            for j in range(group):
                spot = dest_ref[source * group + j]
                found = jnp.where(
                    lax.div(spot, group) == tile * halves + run, lax.rem(spot, group), found
                )
            places.append(found)
        for slot in range(group):
            found = jnp.int32(0)
            for source in range(group):
                found = jnp.where(places[source] == slot, source, found)
            slot_of.append(found)

    spots = lax.broadcasted_iota(jnp.int32, (peak_count, extent), 1)
    ranks = lax.broadcasted_iota(jnp.int32, (peak_count, extent), 0)
    loads[5].wait()
    for which in range(2):
        wanted = jnp.zeros((peak_count, extent), jnp.int32)
        for j in range(peak_count):
            wanted = jnp.where(ranks == j, peaks_ref[0, which, j], wanted)
        spot_send[which * peak_count : (which + 1) * peak_count, :] = jnp.where(
            spots == wanted, 1.0, 0.0
        ).astype(bf)
    spot_copy = remote(spot_send, spot_recv, spot_ssem, spot_rsem, (0, 0, 1))
    spot_copy.start()

    lane = lax.broadcasted_iota(jnp.int32, (1, wide), 1)
    inner = lax.rem(lane, side)
    real_lane = inner < cols
    row_at = lax.broadcasted_iota(jnp.int32, (points, 1), 0)
    sign = jnp.where(lax.rem(row_at, 2) == 0, 1.0, -1.0)
    edge_real = [((inner + part + turn) == 0) for turn in range(2)]
    edge_imag = [((jnp.abs(inner - cols) + part + turn) == 0) for turn in range(2)]
    weights = [
        jnp.where(edge_real[turn] | edge_imag[turn], 1.0, 2.0) * float(extent)
        for turn in range(2)
    ]

    def turned(z, turn):
        ahead = pltpu.roll(z, wide - cols, 1)
        behind = pltpu.roll(z, cols, 1)
        return jnp.where(real_lane, -ahead, behind)

    opt_energy = [0.0, 0.0]

    def optical(turn):
        whole(opt_in.at[turn], parts - 1, opt_ssem.at[turn], opt_rsem.at[turn]).wait_recv()
        if turn == 0:
            for to_tile in range(tiles):
                sar_sends(1, to_tile, (1,))
        for source in range(bands):
            both = jnp.concatenate(
                [opt_in[turn, run * bands + source] for run in range(halves)], axis=1
            )
            rows = jnp.dot(row_v[...], both, preferred_element_type=f32)
            mean = jnp.where(
                edge_real[turn], (rows[0:1, :wide] + rows[0:1, wide:]) / float(extent), 0.0
            )
            total = 0.0
            for run in range(halves):
                moved = both[:, run * wide : (run + 1) * wide].astype(f32) - mean
                total = total + jnp.sum(moved * moved, axis=0, keepdims=True)
            opt_energy[turn] = opt_energy[turn] + total * weights[turn]
            for kind in range(2):
                at = slice(kind * points, (kind + 1) * points)
                near_rows, far_rows = rows[at, :wide], rows[at, wide:] * sign
                z = near_rows + far_rows
                z_far = pltpu.roll(z, side, 1)
                signed, signed_far = z * sign, z_far * sign
                for patch in range(patch_dev):
                    if patch == 0:
                        own = jnp.where(low, z, signed_far)
                    else:
                        own = jnp.where(low, z_far, signed)
                    other = jnp.where(
                        edge_real[turn], 0.0, jnp.where(edge_imag[turn], own, turned(own, turn))
                    )
                    own = jnp.where(edge_imag[turn], 0.0, own)
                    if kind == 0:
                        own = jnp.where(edge_real[turn] & (row_at == 0), 0.0, own)
                    opt_waves[turn, patch, source, kind] = own
                    opt_waves[turn, patch, source, 2 + kind] = other

    block = points // 4
    top = lax.broadcasted_iota(jnp.int32, (block, 1), 0) == 0

    def fold(a, b, c, d):
        def halve(u, v):
            return jnp.where(low, u, v) + pltpu.roll(jnp.where(low, v, u), side, 1)

        u, v = halve(a, c), halve(b, d)
        rest = jnp.where(real_lane, v, u)
        rest = jnp.where(
            real_lane, pltpu.roll(rest, wide - cols, 1), pltpu.roll(rest, cols, 1)
        )
        return jnp.where(real_lane, u, v) + rest

    def slant(turn):
        whole(arrived[turn], others, sar_ssem.at[turn], sar_rsem.at[turn]).wait_recv()
        if turn:
            for shift in (1, 0):
                lag_sends(0, shift)
        for slot in range(group):
            patch, at = slot // per_patch, slot % per_patch * lines
            for source in range(bands):
                pieces = [
                    arrived[turn][slot_of[run * group + slot] * bands + source]
                    for run in range(halves)
                ]
                sar_cols[turn, patch, at : at + lines, source * wide : (source + 1) * wide] = (
                    jnp.concatenate([pieces[0][:, :side], pieces[1][:, side:]], axis=1)
                )
        for patch in range(patch_dev):
            sar_rows[turn, patch] = jnp.dot(
                row_v[...], sar_cols[turn, patch], preferred_element_type=f32
            )
        for b in range(points // block):
            at = slice(b * block, (b + 1) * block)
            lower = slice(points + b * block, points + (b + 1) * block)
            sums = [[], [], [], []]
            for patch in range(patch_dev):
                e_re, e_im, d_lo, d_hi = 0.0, 0.0, 0.0, 0.0
                for source in range(bands):
                    lanes = slice(source * wide, (source + 1) * wide)
                    yc, ys = sar_rows[turn, patch, at, lanes], sar_rows[turn, patch, lower, lanes]
                    zc, zs, tc, ts = [opt_waves[turn, patch, source, k, at] for k in range(4)]
                    if b == 0:
                        zs_e = jnp.where(top, 0.0, zs)
                        ts_e = jnp.where(top, 0.0, ts)
                        zc_d = jnp.where(top, zs, zc)
                        tc_d = jnp.where(top, ts, tc)
                    else:
                        zs_e, ts_e, zc_d, tc_d = zs, ts, zc, tc
                    e_re = e_re + (zc * yc + zs_e * ys)
                    e_im = e_im + (tc * yc + ts_e * ys)
                    d_lo = d_lo + (zc_d * ys - zs_e * yc)
                    d_hi = d_hi + (tc_d * ys - ts_e * yc)
                for k, term in enumerate((e_re, e_im, d_lo, d_hi)):
                    sums[k].append(term)
            cross[turn, at, :] = fold(sums[0][0], sums[1][0], sums[0][1], sums[1][1]).astype(bf)
            cross[turn, lower, :] = fold(sums[2][0], sums[3][0], sums[2][1], sums[3][1]).astype(bf)

    def lag_copy(turn, peer):
        _, to_half, to_band = place(*peer)
        return remote(
            lag_send.at[turn, to_half * bands + to_band],
            lag_in.at[turn, part],
            lag_ssem.at[turn],
            lag_rsem.at[turn, peer[1]],
            peer,
        )

    def lag_sends(turn, shift):
        for swap in range(bands):
            if shift or swap:
                lag_copy(turn, (0, shift, swap)).start()

    def spread(turn):
        for shift, to_half in ((1, other_half), (0, half)):
            at = pl.ds(pl.multiple_of(to_half * quarter, quarter), quarter)
            values = jnp.dot(lag_v[at, :], cross[turn], preferred_element_type=f32).astype(bf)
            lags[turn, at, :] = values
            for patch, piece in enumerate(pair(values[: quarter // 2], values[quarter // 2 :])):
                lag_send[turn, to_half * bands + patch] = piece
            if turn:
                lag_sends(turn, shift)
        lag_in[turn, part] = lag_send[turn, part]

    def gather(turn, shift, first):
        from_half = lax.rem(half + shift, halves)
        count = bands if shift else bands - 1
        whole(lag_in.at[turn], count, lag_ssem.at[turn], lag_rsem.at[turn, shift]).wait_recv()
        upper, lower = pair(*[lag_in[turn, from_half * bands + b] for b in range(bands)])
        table = back_v[turn, pl.ds(pl.multiple_of(from_half * wide, wide), wide), :]
        values = jnp.dot(
            jnp.concatenate([upper, lower], axis=0), table, preferred_element_type=f32
        )
        if first:
            surface_ref[0] = values
        else:
            surface_ref[0] = surface_ref[0] + values

    loads[4].wait()
    optical(0)
    slant(0)
    loads[6].wait()
    spread(0)
    loads[7].wait()
    optical(1)
    slant(1)
    spread(1)

    sar_energy = []
    for patch in range(patch_dev):
        energy = 0.0
        for turn in range(2):
            for source in range(bands):
                lanes = slice(source * wide, (source + 1) * wide)
                head = sar_rows[turn, patch, 0:1, lanes]
                head = (head + pltpu.roll(head, side, 1)) / float(extent)
                mean = jnp.where(edge_real[turn], head, 0.0)
                moved = sar_cols[turn, patch, :, lanes].astype(f32) - mean
                energy = energy + jnp.sum(moved * moved, axis=0, keepdims=True) * weights[turn]
        sar_energy.append(energy)
    opt_total = opt_energy[0] + opt_energy[1]

    spot_copy.wait_recv()
    hits = jnp.concatenate([spot_send[...], spot_recv[...]], axis=0)
    found = 0.0
    for turn in range(2):
        picked = jnp.dot(hits, lags[turn], preferred_element_type=f32)
        rows_back = back_v[turn, pl.ds(pl.multiple_of(part * side, side), side), :]
        waves = lax.dot_general(
            hits,
            jnp.concatenate([rows_back, rows_back], axis=0),
            (((1,), (1,)), ((), ())),
            preferred_element_type=f32,
        )
        found = found + jnp.concatenate(
            [
                picked[:peak_count] * waves[peak_count : 2 * peak_count],
                picked[2 * peak_count : 3 * peak_count] * waves[3 * peak_count :],
            ],
            axis=0,
        )
    for which, patch, ref in ((0, band, last_mine), (1, other_band, last_other)):
        mine = lax.div(lane, side) == patch
        ref[0:8, :] = jnp.zeros((8, wide), f32)
        ref[0:1, :] = jnp.where(mine, opt_total, 0.0)
        ref[1:2, :] = jnp.where(patch == 0, sar_energy[0], sar_energy[1])
        value = jnp.where(mine, found[which * peak_count : (which + 1) * peak_count], 0.0)
        ref[8 : 8 + peak_count, :] = jnp.broadcast_to(
            jnp.sum(value, axis=1, keepdims=True), (peak_count, wide)
        )
    for peer in near:
        remote(
            last_other if peer[2] else last_mine, last_in.at[part], last_ssem, last_rsem, peer
        ).start()

    gather(0, 0, True)
    gather(1, 0, False)
    gather(0, 1, False)
    gather(1, 1, False)
    whole(last_in, parts - 1, last_ssem, last_rsem).wait_recv()
    last_in[part] = last_mine[...]
    total_ref[...] = sum(last_in[i] for i in range(1, parts)) + last_in[0]
    for turn in range(2):
        whole(send[turn], others, sar_ssem.at[turn], sar_rsem.at[turn]).wait_send()
        whole(opt_in.at[turn], parts - 1, opt_ssem.at[turn], opt_rsem.at[turn]).wait_send()
        whole(lag_in.at[turn], parts - 1, lag_ssem.at[turn], lag_rsem.at[turn, 0]).wait_send()
    whole(last_in, parts - 1, last_ssem, last_rsem).wait_send()
    spot_copy.wait_send()


def finish(bands, pieces, surface_ref, total_ref, out_ref, peak_ref, scaled, sem):
    _, lines, extent = surface_ref.shape
    pixels = extent * extent
    peak_count = peak_ref.shape[1]
    width = total_ref.shape[1]
    o_all = jnp.sum(total_ref[0:1, :], axis=1, keepdims=True) / (float(pixels) * bands * pixels)
    s_all = jnp.sum(total_ref[1:2, :], axis=1, keepdims=True) / (float(pixels) * bands * pixels)
    norm = lax.rsqrt(bands * pixels * (o_all + EPSILON) * (s_all + EPSILON)) / pixels
    part = lines // pieces
    copies = []
    for i in range(pieces):
        at = pl.ds(i * part, part)
        scaled[at, :] = surface_ref[0, at, :] * norm
        copy = pltpu.make_async_copy(scaled.at[at], out_ref.at[0, at], sem.at[i])
        copy.start()
        copies.append(copy)
    values = total_ref[8 : 8 + peak_count, :] * norm
    lane = lax.broadcasted_iota(jnp.int32, (peak_count, width), 1)
    rank = lax.broadcasted_iota(jnp.int32, (peak_count, width), 0)
    row = jnp.sum(jnp.where(lane == rank, values, 0.0), axis=0, keepdims=True)
    peak_ref[...] = row[:, :peak_count]
    for copy in copies:
        copy.wait()


def fused(mesh, optical, sar, destination, peaks):
    tiles, halves, bands = mesh.shape["tile"], mesh.shape["half"], mesh.shape["band"]
    patch_dev, _, quarter, extent = optical.shape
    group = tiles * halves
    parts = halves * bands
    lines = sar.shape[1] // group
    peak_count = peaks.shape[2]
    wide = extent // parts
    points = extent // 2
    sizes = (tiles, halves, bands, patch_dev, quarter, extent, lines, peak_count)
    tables = dft_tables(extent, parts)
    bf, f32 = jnp.bfloat16, jnp.float32
    vmem = pltpu.VMEM
    dma = pltpu.SemaphoreType.DMA
    raw, totals = pl.pallas_call(
        functools.partial(kernel, sizes),
        out_shape=(
            jax.ShapeDtypeStruct((1, quarter, extent), f32),
            jax.ShapeDtypeStruct((8 + peak_count, wide), f32),
        ),
        in_specs=[pl.BlockSpec(memory_space=pltpu.HBM)] * 8,
        out_specs=(pl.BlockSpec(memory_space=pltpu.VMEM), pl.BlockSpec(memory_space=pltpu.VMEM)),
        scratch_shapes=[
            pltpu.SMEM(destination.shape, jnp.int32),
            pltpu.SMEM(peaks.shape, jnp.int32),
            vmem((group, lines, extent), bf),
            vmem((patch_dev, quarter, extent), bf),
            vmem((extent, extent), bf),
            vmem((extent, points), bf),
            vmem((extent, extent), bf),
            vmem((2, points, extent), bf),
            vmem((tiles * parts, lines, wide), bf),
            vmem((tiles * parts, lines, wide), bf),
            vmem((group * bands, lines, wide), bf),
            vmem((group * bands, lines, wide), bf),
            vmem((2, parts, quarter, wide), bf),
            vmem((2, parts, quarter, wide), bf),
            vmem((2, patch_dev, bands, 4, points, wide), f32),
            vmem((2, patch_dev, points, bands * wide), bf),
            vmem((2, patch_dev, extent, bands * wide), f32),
            vmem((2, extent, wide), bf),
            vmem((2, extent, wide), bf),
            vmem((2, parts, quarter // 2, wide), bf),
            vmem((2, parts, quarter // 2, wide), bf),
            vmem((2 * peak_count, extent), bf),
            vmem((2 * peak_count, extent), bf),
            vmem((8 + peak_count, wide), f32),
            vmem((8 + peak_count, wide), f32),
            vmem((parts, 8 + peak_count, wide), f32),
            dma((8,)),
            dma((2,)),
            dma((2,)),
            dma((2,)),
            dma((2,)),
            dma((2,)),
            dma((2, 2)),
            dma,
            dma,
            dma,
            dma,
            pltpu.SemaphoreType.REGULAR,
            pltpu.SemaphoreType.REGULAR,
        ],
        compiler_params=pltpu.CompilerParams(
            collective_id=0, has_side_effects=True, vmem_limit_bytes=50 * 1024 * 1024
        ),
    )(
        *[
            pltpu.with_memory_space_constraint(x, pltpu.HBM)
            for x in (
                destination,
                peaks,
                sar.reshape(group, lines, extent),
                optical.reshape(patch_dev, quarter, extent),
                *[jnp.asarray(t) for t in tables],
            )
        ]
    )
    pieces = 4
    return pl.pallas_call(
        functools.partial(finish, bands, pieces),
        out_shape=(
            jax.ShapeDtypeStruct((1, quarter, extent), f32),
            jax.ShapeDtypeStruct((1, peak_count), f32),
        ),
        in_specs=[pl.BlockSpec(memory_space=pltpu.VMEM)] * 2,
        out_specs=(pl.BlockSpec(memory_space=pltpu.HBM), pl.BlockSpec(memory_space=pltpu.VMEM)),
        scratch_shapes=[vmem((quarter, extent), f32), dma((pieces,))],
    )(*[pltpu.with_memory_space_constraint(x, pltpu.VMEM) for x in (raw, totals)])


def fits(mesh, optical, sar, peaks):
    group = mesh.shape["tile"] * mesh.shape["half"]
    patch_dev, local_bands, quarter, extent = optical.shape
    lines = sar.shape[1] // group
    return (
        mesh.shape["half"] == 2
        and mesh.shape["band"] == 2
        and patch_dev == 2
        and local_bands == 1
        and lines % 16 == 0
        and quarter * 2 == extent
        and group * lines == patch_dev * quarter
        and extent % 512 == 0
        and peaks.shape[0] == 1
        and peaks.shape[2] % 8 == 0
    )


def solution(mesh):
    def local(optical, sar, destination, peaks):
        if fits(mesh, optical, sar, peaks):
            return fused(mesh, optical, sar, destination, peaks)
        return generic(optical, sar, destination, peaks)

    in_specs = (
        P(("scene", "tile"), "band", "half", None),
        P("band", ("scene", "tile", "half"), None),
        P("scene"),
        P(("scene", "tile", "band"), None, None),
    )
    out_specs = (P(("scene", "tile", "band"), "half", None), P(("scene", "tile", "band"), None))
    return jax.shard_map(local, mesh=mesh, in_specs=in_specs, out_specs=out_specs, check_vma=False)
```

```python
import functools
import math

import jax
import jax.numpy as jnp
import numpy as np
from jax import lax
from jax.experimental import pallas as pl
from jax.experimental.pallas import tpu as pltpu
from jax.sharding import PartitionSpec as P

MESH = pl.DeviceIdType.MESH

precise = lax.Precision.HIGHEST
EPSILON = 1e-06
BLOCK = 16


def fourier_tables(extent):
    places = jnp.arange(extent, dtype=jnp.int32)
    phases = places[:, None] * places[None, :] % extent
    angles = phases.astype(jnp.float32) * (2.0 * math.pi / extent)
    return (jnp.cos(angles), jnp.sin(angles))


def fourier_pair(table):
    upper = table.astype(jnp.bfloat16)
    lower = (table - upper.astype(jnp.float32)).astype(jnp.bfloat16)
    return (upper, lower)


def column_spectrum(samples, table_upper, table_lower):
    extent = samples.shape[-1]
    values = samples.reshape(-1, extent)
    spectrum = jnp.dot(values, table_upper, preferred_element_type=jnp.float32) + jnp.dot(
        values, table_lower, preferred_element_type=jnp.float32
    )
    return spectrum.astype(jnp.bfloat16).reshape(samples.shape[:-1] + (2 * extent,))


def row_spectrum(columns, table_upper, table_lower):
    line_count = columns.shape[-3]
    stacked = jnp.concatenate([columns[..., 0, :], columns[..., 1, :]], axis=-2)
    result = jnp.einsum("kr,...rc->...kc", table_upper, stacked, preferred_element_type=jnp.float32)
    result = result + jnp.einsum(
        "kr,...rc->...kc", table_lower, stacked, preferred_element_type=jnp.float32
    )
    return (result[..., :line_count, :], result[..., line_count:, :])


def relay_blocks(parcel):
    layout = parcel.shape
    merged = parcel.reshape(layout[:1] + (layout[1] * layout[2],) + layout[3:])
    arrived = lax.all_to_all(merged, ("tile", "half"), split_axis=1, concat_axis=1, tiled=True)
    return arrived.reshape(layout)


def generic(optical, sar, destination, peaks):
    tile_count = lax.axis_size("tile")
    half_count = lax.axis_size("half")
    band_count = lax.axis_size("band")
    group_size = tile_count * half_count
    patch_dev, local_bands, quarter, extent = optical.shape
    col_width = extent // half_count
    block_lines = sar.shape[1] // group_size
    band_total = local_bands * band_count
    pixel_count = extent * extent
    patch_total = patch_dev * tile_count
    kept_patches = patch_dev // band_count
    cosine_table, sine_table = fourier_tables(extent)
    col_upper, col_lower = fourier_pair(jnp.concatenate([cosine_table, -sine_table], axis=1))
    row_full = jnp.concatenate(
        [
            jnp.concatenate([cosine_table, sine_table], axis=1),
            jnp.concatenate([-sine_table, cosine_table], axis=1),
        ],
        axis=0,
    )
    row_upper, row_lower = fourier_pair(row_full)
    tile_at = lax.axis_index("tile")
    half_at = lax.axis_index("half")
    band_at = lax.axis_index("band")
    device_at = lax.axis_index(("tile", "half"))
    own_blocks = lax.dynamic_slice_in_dim(destination, device_at * group_size, group_size)
    send_order = jnp.argsort(own_blocks // group_size)
    inverse = (
        jnp.zeros_like(destination)
        .at[destination]
        .set(jnp.arange(destination.shape[0], dtype=jnp.int32))
    )
    opt_values = optical.astype(jnp.float32)
    opt_sums = jnp.sum(opt_values, axis=(2, 3))
    opt_squares = jnp.sum(opt_values * opt_values, axis=(2, 3))
    sar_values = sar.astype(jnp.float32).reshape(local_bands, group_size, block_lines * extent)
    sar_sums = jnp.sum(sar_values, axis=2)
    sar_squares = jnp.sum(sar_values * sar_values, axis=2)
    map_device = own_blocks // group_size
    map_patch = (
        map_device // half_count * patch_dev + own_blocks % group_size * block_lines // quarter
    )
    member = (map_patch[:, None] == jnp.arange(patch_total, dtype=jnp.int32)[None, :]).astype(
        jnp.float32
    )
    sar_stats = jnp.dot(
        jnp.stack([sar_sums, sar_squares]).reshape(2 * local_bands, group_size),
        member,
        precision=precise,
        preferred_element_type=jnp.float32,
    )
    statistics = jnp.zeros((2, 2, band_total, patch_total), jnp.float32)
    opt_part = jnp.transpose(jnp.stack([opt_sums, opt_squares]), (0, 2, 1))
    statistics = lax.dynamic_update_slice(
        statistics, opt_part[None], (0, 0, band_at * local_bands, tile_at * patch_dev)
    )
    statistics = lax.dynamic_update_slice(
        statistics,
        sar_stats.reshape(2, local_bands, patch_total)[None],
        (1, 0, band_at * local_bands, 0),
    )
    totals = lax.psum(statistics, ("tile", "half", "band"))
    centered = totals[:, 1] - totals[:, 0] * totals[:, 0] / pixel_count
    energy = jnp.sum(centered, axis=1) / (band_total * pixel_count)
    norm_scale = lax.rsqrt(band_total * pixel_count * (energy[0] + EPSILON) * (energy[1] + EPSILON))
    first_patch = tile_at * patch_dev + band_at * kept_patches
    norm_mine = lax.dynamic_slice_in_dim(norm_scale, first_patch, kept_patches)
    slant_spectra = column_spectrum(sar, col_upper, col_lower).reshape(
        local_bands, group_size, block_lines, 2, half_count, col_width
    )
    outgoing = jnp.take(slant_spectra, send_order, axis=1).reshape(
        local_bands, tile_count, half_count, block_lines, 2, half_count, col_width
    )
    outgoing = jnp.transpose(outgoing, (0, 1, 5, 2, 3, 4, 6))
    arrived = relay_blocks(outgoing).reshape(
        local_bands, group_size * half_count, block_lines, 2, col_width
    )
    sources = lax.dynamic_slice_in_dim(
        inverse, tile_at * half_count * group_size, half_count * group_size
    )
    slot_index = (
        sources // group_size * half_count
        + jnp.arange(half_count * group_size, dtype=jnp.int32) // group_size
    )
    placed = jnp.take(arrived, slot_index, axis=1).reshape(
        local_bands, half_count, patch_dev, quarter, 2, col_width
    )
    placed = jnp.transpose(placed, (2, 0, 1, 3, 4, 5)).reshape(
        patch_dev, local_bands, extent, 2, col_width
    )
    sar_real, sar_imag = row_spectrum(placed, row_upper, row_lower)
    spectra = column_spectrum(optical, col_upper, col_lower).reshape(
        patch_dev, local_bands, quarter, 2, half_count, col_width
    )
    real_part, imag_part = row_spectrum(
        jnp.squeeze(
            lax.all_to_all(spectra, "half", split_axis=4, concat_axis=2, tiled=True), axis=4
        ),
        row_upper,
        row_lower,
    )
    opt_real = real_part
    opt_imag = imag_part
    rows_at = jnp.arange(extent, dtype=jnp.int32)[:, None]
    cols_at = half_at * col_width + jnp.arange(col_width, dtype=jnp.int32)[None, :]
    keep_mask = jnp.where((rows_at == 0) & (cols_at == 0), 0.0, 1.0).astype(jnp.float32)
    opt_real = opt_real * keep_mask
    opt_imag = opt_imag * keep_mask
    sar_real = sar_real * keep_mask
    sar_imag = sar_imag * keep_mask
    cross_real = jnp.sum(opt_real * sar_real + opt_imag * sar_imag, axis=1)
    cross_imag = jnp.sum(opt_real * sar_imag - opt_imag * sar_real, axis=1)
    cross_term = jnp.stack([cross_real, cross_imag], axis=1)
    cross_sum = lax.psum_scatter(cross_term, "band", scatter_dimension=0, tiled=True)
    lag_real = (
        jnp.einsum("uk,pkc->puc", cosine_table, cross_sum[:, 0], precision=precise)
        - jnp.einsum("uk,pkc->puc", sine_table, cross_sum[:, 1], precision=precise)
    ) / extent
    lag_imag = (
        jnp.einsum("uk,pkc->puc", cosine_table, cross_sum[:, 1], precision=precise)
        + jnp.einsum("uk,pkc->puc", sine_table, cross_sum[:, 0], precision=precise)
    ) / extent
    lagged = jnp.stack([lag_real, lag_imag], axis=2).reshape(
        kept_patches, half_count, quarter, 2, col_width
    )
    pieces = lax.all_to_all(lagged, "half", split_axis=1, concat_axis=4, tiled=True)
    real_in = pieces[:, 0, :, 0, :]
    imag_in = pieces[:, 0, :, 1, :]
    correlation = (
        jnp.einsum("puc,cv->puv", real_in, cosine_table, precision=precise)
        - jnp.einsum("puc,cv->puv", imag_in, sine_table, precision=precise)
    ) / extent
    surface = correlation * norm_mine[:, None, None]
    local_rows = peaks[:, 0, :] - half_at * quarter
    row_hit = (
        local_rows[:, :, None] == jnp.arange(quarter, dtype=jnp.int32)[None, None, :]
    ).astype(jnp.float32)
    picked = jnp.einsum("pkr,prc->pkc", row_hit, surface, precision=precise)
    col_hit = (peaks[:, 1, :, None] == jnp.arange(extent, dtype=jnp.int32)[None, None, :]).astype(
        jnp.float32
    )
    local_values = jnp.sum(picked * col_hit, axis=2)
    peak_values = lax.psum(local_values, "half")
    return (surface, peak_values)


def dft_tables(extent, parts):
    points = extent // 2
    cols = points // parts // 2
    places = np.arange(extent)
    phases = (places[:, None] * places[None, :]) % extent
    cosine = np.cos(phases * (2.0 * np.pi / extent))
    sine = np.sin(phases * (2.0 * np.pi / extent))
    forward, backward = [], [[], []]
    for part in range(parts):
        for turn in range(2):
            first = (2 * part + turn) * cols
            span = slice(first, first + cols)
            real, imag = cosine[:, span].copy(), -sine[:, span]
            real_back, imag_back = 2.0 * cosine[span], -2.0 * sine[span]
            if first == 0:
                imag[:, 0] = cosine[:, points]
                real_back[0] = 1.0
                imag_back[0] = cosine[points]
            forward += [real, imag]
            backward[turn] += [real_back, imag_back]
    col_table = np.concatenate(forward, axis=1)
    back_table = np.stack([np.concatenate(b, axis=0) for b in backward])
    row_sine, lag_sine = sine[:points, :points].copy(), 2.0 * sine[:points, :points]
    row_cosine, lag_cosine = cosine[:points, :points], 2.0 * cosine[:points, :points]
    row_sine[0] = cosine[points, :points]
    lag_cosine[:, 0] = 1.0
    lag_sine[:, 0] = cosine[:points, points]


    def woven(a, b):
        both = np.stack([a.reshape(-1, BLOCK, points), b.reshape(-1, BLOCK, points)], axis=1)
        return both.reshape(points, points)

    row_table = np.stack([woven(row_cosine[i::2], row_sine[i::2]) for i in range(2)])
    lag_table = np.stack([woven(lag_cosine.T[i::2], lag_sine.T[i::2]).T for i in range(2)])
    return tuple(t.astype(jnp.bfloat16) for t in (col_table, row_table, lag_table, back_table))


def kernel(
    sizes,
    dest_hbm,
    peaks_hbm,
    sar_hbm,
    opt_hbm,
    col_hbm,
    row_hbm,
    lag_hbm,
    back_hbm,
    surface_ref,
    total_ref,
    dest_ref,
    peaks_ref,
    sar_v,
    opt_v,
    col_v,
    row_v,
    lag_v,
    back_v,
    send_0,
    send_1,
    arrived_0,
    arrived_1,
    opt_send,
    opt_in,
    opt_waves,
    sar_cols,
    sar_head,
    unfolded,
    fold_v,
    cross,
    lags,
    lag_send,
    lag_in,
    spot_send,
    spot_recv,
    last_mine,
    last_other,
    last_in,
    load_sem,
    sar_ssem,
    sar_rsem,
    opt_ssem,
    opt_rsem,
    lag_ssem,
    lag_rsem,
    last_ssem,
    last_rsem,
    spot_ssem,
    spot_rsem,
    near_sem,
    far_sem,
):
    tiles, halves, bands, patch_dev, quarter, extent, lines, peak_count = sizes
    group = tiles * halves
    parts = halves * bands
    wide = extent // parts
    side = wide // 2
    cols = wide // 4
    points = extent // 2
    per_patch = group // patch_dev
    block = BLOCK
    send, arrived = (send_0, send_1), (arrived_0, arrived_1)
    f32, bf = jnp.float32, jnp.bfloat16
    tile, half, band = lax.axis_index("tile"), lax.axis_index("half"), lax.axis_index("band")
    me = tile * halves + half
    part = half * bands + band
    other_half = 1 - half
    other_band = 1 - band

    def place(step, shift, swap):
        return (
            lax.rem(tile + step, tiles),
            lax.rem(half + shift, halves),
            lax.rem(band + swap, bands),
        )

    def device(step, shift, swap):
        return dict(zip(("tile", "half", "band"), place(step, shift, swap)))

    others = tiles * parts - 1
    near = [(0, shift, swap) for shift in (1, 0) for swap in range(bands) if shift or swap]

    loads = [
        pltpu.make_async_copy(a, b, load_sem.at[i])
        for i, (a, b) in enumerate(
            [(dest_hbm, dest_ref), (sar_hbm, sar_v), (col_hbm, col_v), (opt_hbm, opt_v),
             (row_hbm, row_v), (peaks_hbm, peaks_ref), (lag_hbm, lag_v), (back_hbm, back_v)]
        )
    ]
    for i in (3, 2, 0, 1):
        loads[i].start()

    barrier = pltpu.get_barrier_semaphore()
    first_band, last_band = jnp.int32(0), jnp.int32(bands - 1)

    def tell(semaphore, **where):
        pl.semaphore_signal(semaphore, inc=1, device_id=where, device_id_type=MESH)

    for shift in range(1, halves):
        tell(barrier, half=lax.rem(half + shift, halves), band=first_band)
    pl.when(band != first_band)(lambda: tell(barrier, band=first_band))
    for step in sorted(range(1, tiles), key=lambda s: -min(s, tiles - s)):
        for shift in range(halves):
            tell(
                barrier,
                tile=lax.rem(tile + step, tiles),
                half=lax.rem(half + shift, halves),
                band=last_band,
            )

    def remote(src, dst, ssem, rsem, peer):
        return pltpu.make_async_remote_copy(
            src_ref=src,
            dst_ref=dst,
            send_sem=ssem,
            recv_sem=rsem,
            device_id=device(*peer),
            device_id_type=MESH,
        )

    source_at = me * bands + band

    def sar_copy(turn, to_tile, to_half, to_band):
        return pltpu.make_async_remote_copy(
            src_ref=send[turn].at[to_tile * parts + to_half * bands + to_band],
            dst_ref=arrived[turn].at[source_at],
            send_sem=sar_ssem.at[turn],
            recv_sem=sar_rsem.at[turn],
            device_id={"tile": to_tile, "half": to_half, "band": to_band},
            device_id_type=MESH,
        )

    low = lax.broadcasted_iota(jnp.int32, (1, wide), 1) < side

    def pair(a, b):
        first = jnp.concatenate([a[:, :side], b[:, :side]], axis=1)
        second = jnp.concatenate([a[:, side:], b[:, side:]], axis=1)
        return first, second

    def whole(ref, count, ssem, rsem):
        ref = ref.at[pl.ds(0, count)]
        return remote(ref, ref, ssem, rsem, (0, 1, 0))

    loads[0].wait()
    own_runs = [lax.div(dest_ref[me * group + j], group) for j in range(group)]

    def block_for(run):
        found = jnp.int32(0)
        for j in range(group):
            found = jnp.where(own_runs[j] == run, j, found)
        return found

    def sar_columns(to_tile):
        if to_tile == 0:
            loads[1].wait()
        samples = jnp.concatenate(
            [
                sar_v[block_for(to_tile * halves + lax.rem(run + band, halves))]
                for run in range(halves)
            ],
            axis=0,
        )
        spectra = jnp.dot(samples, col_v[...], preferred_element_type=f32).astype(bf)
        for to in range(parts):
            at = slice(to * wide, (to + 1) * wide)
            first, second = pair(spectra[:lines, at], spectra[lines:, at])
            send_0[to_tile * parts + to] = first
            send_1[to_tile * parts + to] = second

    def sar_sends(turn, to_tile, shifts):
        for shift in shifts:
            to_half = lax.rem(half + shift, halves)
            for swap in range(bands):
                to_band = lax.rem(band + swap, bands)
                copy = sar_copy(turn, to_tile, to_half, to_band)
                if shift or swap:
                    copy.start()
                else:
                    pl.when(tile != to_tile)(copy.start)

    def opt_copy(turn, peer):
        _, to_half, to_band = place(*peer)
        return remote(
            opt_send.at[turn, to_half * bands + to_band],
            opt_in.at[turn, part],
            opt_ssem.at[turn],
            opt_rsem.at[turn],
            peer,
        )

    def opt_sends(turn):
        for peer in near:
            opt_copy(turn, peer).start()

    loads[3].wait()
    loads[2].wait()
    opt_spectra = [
        jnp.dot(opt_v[lax.rem(patch + band, patch_dev)], col_v[...], preferred_element_type=f32).astype(bf)
        for patch in range(patch_dev)
    ]
    for to in range(parts):
        at = slice(to * wide, (to + 1) * wide)
        first, second = pair(*[s[:, at] for s in opt_spectra])
        opt_send[0, to] = first
        opt_send[1, to] = second
    @pl.when(band == first_band)
    def _():
        pl.semaphore_wait(barrier, parts - 1)
        tell(near_sem, band=last_band)

    @pl.when(band == last_band)
    def _():
        pl.semaphore_wait(near_sem, 1)

    opt_sends(0)
    opt_sends(1)
    sar_columns(0)
    for i in (4, 5, 6, 7):
        loads[i].start()

    @pl.when(band == last_band)
    def _():
        pl.semaphore_wait(barrier, (tiles - 1) * parts)
        tell(far_sem, band=first_band)

    @pl.when(band == first_band)
    def _():
        pl.semaphore_wait(far_sem, 1)

    sar_sends(0, 0, (0, 1))
    for to_tile in range(1, tiles):
        sar_columns(to_tile)
        if to_tile > 1:
            sar_sends(0, to_tile, (0, 1))
        else:
            sar_sends(1, 0, (0, 1))
            sar_sends(0, 1, (0, 1))
    for to_tile in range(1, tiles):
        sar_sends(1, to_tile, (0, 1))
    arrived_0[source_at] = send_0[tile * parts + part]
    arrived_1[source_at] = send_1[tile * parts + part]
    for turn in range(2):
        opt_in[turn, part] = opt_send[turn, part]

    slot_of = []
    for run in range(halves):
        places = []
        for source in range(group):
            found = jnp.int32(0)
            for j in range(group):
                spot = dest_ref[source * group + j]
                found = jnp.where(
                    lax.div(spot, group) == tile * halves + run, lax.rem(spot, group), found
                )
            places.append(found)
        for slot in range(group):
            found = jnp.int32(0)
            for source in range(group):
                found = jnp.where(places[source] == slot, source, found)
            slot_of.append(found)

    spots = lax.broadcasted_iota(jnp.int32, (peak_count, extent), 1)
    ranks = lax.broadcasted_iota(jnp.int32, (peak_count, extent), 0)
    loads[5].wait()
    for which in range(2):
        wanted = jnp.zeros((peak_count, extent), jnp.int32)
        for j in range(peak_count):
            wanted = jnp.where(ranks == j, peaks_ref[0, which, j], wanted)
        spot_send[which * peak_count : (which + 1) * peak_count, :] = jnp.where(
            spots == wanted, 1.0, 0.0
        ).astype(bf)
    spot_copy = remote(spot_send, spot_recv, spot_ssem, spot_rsem, (0, 0, 1))
    spot_copy.start()

    lane = lax.broadcasted_iota(jnp.int32, (1, wide), 1)
    inner = lax.rem(lane, side)
    real_lane = inner < cols
    top = lax.broadcasted_iota(jnp.int32, (block, wide), 0) == 0
    edge_real = [((inner + part + turn) == 0) for turn in range(2)]
    edge_imag = [((jnp.abs(inner - cols) + part + turn) == 0) for turn in range(2)]
    weights = [
        jnp.where(edge_real[turn] | edge_imag[turn], 1.0, 2.0) * (0.5 * extent)
        for turn in range(2)
    ]

    def swapped(z):
        return pltpu.roll(z, side, 1)

    def crossed(z):
        return jnp.where(real_lane, pltpu.roll(z, wide - cols, 1), pltpu.roll(z, cols, 1))

    def turned(z):
        return jnp.where(real_lane, -pltpu.roll(z, wide - cols, 1), pltpu.roll(z, cols, 1))

    opt_energy = [0.0] * patch_dev

    def energy_of(even, odd, head, turn):
        shifted = even.astype(f32) - jnp.where(edge_real[turn], head * (2.0 / extent), 0.0)
        odd = odd.astype(f32)
        total = jnp.sum(shifted * shifted + odd * odd, axis=0, keepdims=True)
        return total * weights[turn]

    def optical(turn):
        whole(opt_in.at[turn], parts - 1, opt_ssem.at[turn], opt_rsem.at[turn]).wait_recv()
        real, imag = edge_real[turn], edge_imag[turn]
        pieces = [[opt_in[turn, run * bands + b] for b in range(bands)] for run in range(halves)]
        mixed = []
        for patch in range(patch_dev):
            near_x, far_x = [jnp.where(low, p[patch], p[1 - patch]) for p in pieces]
            mixed.append((near_x + far_x, near_x - far_x))
        for parity in range(2):
            plain = [jnp.where(imag, 0.0, m[parity]).astype(bf) for m in mixed]
            crossed_x = [
                jnp.where(real, 0.0, jnp.where(imag, m[parity], turned(m[parity]))).astype(bf)
                for m in mixed
            ]
            rows = jnp.dot(
                row_v[parity], jnp.concatenate(plain + crossed_x, axis=1), preferred_element_type=f32
            )
            for kind in range(2):
                for patch in range(patch_dev):
                    at = (kind * patch_dev + patch) * wide
                    opt_waves[turn, kind, patch, parity] = rows[:, at : at + wide]
        for patch in range(patch_dev):
            head = opt_waves[turn, 0, patch, 0, :block]
            opt_energy[patch] = opt_energy[patch] + energy_of(*mixed[patch], head[0:1], turn)
            opt_waves[turn, 0, patch, 0, :block] = jnp.where(real & top, 0.0, head)

    tall = (2 * patch_dev * wide, wide)
    fold_row = lax.broadcasted_iota(jnp.int32, tall, 0)
    fold_lane = lax.broadcasted_iota(jnp.int32, tall, 1)
    fold_v[...] = jnp.where(
        (lax.div(fold_row, wide) == lax.div(fold_lane, cols))
        & (lax.rem(fold_row, cols) == lax.rem(fold_lane, cols)),
        1.0,
        0.0,
    ).astype(bf)

    def slant(turn):
        whole(arrived[turn], others, sar_ssem.at[turn], sar_rsem.at[turn]).wait_recv()
        for slot in range(group):
            patch, at = slot // per_patch, slot % per_patch * lines
            ends = []
            for run in range(halves):
                source = slot_of[run * group + slot] * bands
                piece = jnp.where(
                    low, arrived[turn][source + run], arrived[turn][source + 1 - run]
                )
                if patch != run:
                    piece = jnp.concatenate([piece[:, side:], piece[:, :side]], axis=1)
                ends.append(piece)
            sar_cols[turn, 0, patch, at : at + lines, :] = ends[0] + ends[1]
            sar_cols[turn, 1, patch, at : at + lines, :] = ends[0] - ends[1]
        for parity in range(2):
            both = [sar_cols[turn, parity, patch] for patch in range(patch_dev)]
            rows = jnp.dot(
                row_v[parity], jnp.concatenate(both, axis=1), preferred_element_type=f32
            )
            if parity == 0:
                sar_head[turn] = rows[:8]
            for b in range(points // 2 // block):
                at = slice(2 * b * block, (2 * b + 1) * block)
                lower = slice((2 * b + 1) * block, (2 * b + 2) * block)
                sums = []
                for patch in range(patch_dev):
                    yc, ys = [rows[i, patch * wide : (patch + 1) * wide] for i in (at, lower)]
                    zc, zs = [opt_waves[turn, 0, patch, parity, i] for i in (at, lower)]
                    tc, ts = [opt_waves[turn, 1, patch, parity, i] for i in (at, lower)]
                    zs_e, ts_e, zc_d, tc_d = zs, ts, zc, tc
                    if b == 0 and parity == 0:
                        zs_e, ts_e = jnp.where(top, 0.0, zs), jnp.where(top, 0.0, ts)
                        zc_d, tc_d = jnp.where(top, zs, zc), jnp.where(top, ts, tc)
                    sums.append(
                        (
                            zc * yc + zs_e * ys,
                            tc * yc + ts_e * ys,
                            zc_d * ys - zs_e * yc,
                            tc_d * ys - ts_e * yc,
                        )
                    )
                for patch in range(patch_dev):
                    for k in range(2):
                        lanes = slice((2 * patch + k) * wide, (2 * patch + k + 1) * wide)
                        unfolded[parity, at, lanes] = sums[patch][k].astype(bf)
                        unfolded[parity, lower, lanes] = sums[patch][2 + k].astype(bf)
            cross[turn, parity] = jnp.dot(
                unfolded[parity], fold_v[...], preferred_element_type=f32
            ).astype(bf)

    def lag_copy(turn, peer):
        _, to_half, to_band = place(*peer)
        return remote(
            lag_send.at[turn, to_half * bands + to_band],
            lag_in.at[turn, part],
            lag_ssem.at[turn],
            lag_rsem.at[turn, peer[1]],
            peer,
        )

    def lag_sends(turn, shift):
        for swap in range(bands):
            if shift or swap:
                lag_copy(turn, (0, shift, swap)).start()

    def spread(turn):
        even, odd = [
            jnp.dot(lag_v[parity], cross[turn, parity], preferred_element_type=f32)
            for parity in range(2)
        ]
        flip = jnp.where(half == 0, -1.0, 1.0)
        for shift, to_half in ((1, other_half), (0, half)):
            at = pl.ds(pl.multiple_of(to_half * quarter, quarter), quarter)
            values = (even + odd * flip if shift else even - odd * flip).astype(bf)
            lags[turn, at, :] = values
            for patch, piece in enumerate(pair(values[: quarter // 2], values[quarter // 2 :])):
                lag_send[turn, to_half * bands + patch] = piece
            lag_sends(turn, shift)
        lag_in[turn, part] = lag_send[turn, part]

    def gather(turn, shift, first):
        from_half = lax.rem(half + shift, halves)
        count = bands if shift else bands - 1
        whole(lag_in.at[turn], count, lag_ssem.at[turn], lag_rsem.at[turn, shift]).wait_recv()
        upper, lower = pair(*[lag_in[turn, from_half * bands + b] for b in range(bands)])
        table = back_v[turn, pl.ds(pl.multiple_of(from_half * wide, wide), wide), :]
        values = jnp.dot(
            jnp.concatenate([upper, lower], axis=0), table, preferred_element_type=f32
        )
        if first:
            surface_ref[0] = values
        else:
            surface_ref[0] = surface_ref[0] + values

    loads[4].wait()
    optical(0)
    optical(1)
    slant(0)
    loads[6].wait()
    spread(0)
    loads[7].wait()
    slant(1)
    spread(1)

    sar_energy = [0.0] * patch_dev
    for patch in range(patch_dev):
        for turn in range(2):
            energy = energy_of(
                sar_cols[turn, 0, patch],
                sar_cols[turn, 1, patch],
                sar_head[turn, 0:1, patch * wide : (patch + 1) * wide],
                turn,
            )
            sar_energy[patch] = sar_energy[patch] + energy

    spot_copy.wait_recv()
    hits = jnp.concatenate([spot_send[...], spot_recv[...]], axis=0)
    found = 0.0
    for turn in range(2):
        picked = jnp.dot(hits, lags[turn], preferred_element_type=f32)
        rows_back = back_v[turn, pl.ds(pl.multiple_of(part * side, side), side), :]
        waves = lax.dot_general(
            hits,
            jnp.concatenate([rows_back, rows_back], axis=0),
            (((1,), (1,)), ((), ())),
            preferred_element_type=f32,
        )
        found = found + jnp.concatenate(
            [
                picked[:peak_count] * waves[peak_count : 2 * peak_count],
                picked[2 * peak_count : 3 * peak_count] * waves[3 * peak_count :],
            ],
            axis=0,
        )
    for which, patch, ref in ((0, band, last_mine), (1, other_band, last_other)):
        mine = lax.div(lane, side) == patch
        ref[0:8, :] = jnp.zeros((8, wide), f32)
        ref[0:1, :] = jnp.where(patch == 0, opt_energy[0], opt_energy[1])
        ref[1:2, :] = jnp.where(patch == 0, sar_energy[0], sar_energy[1])
        value = jnp.where(mine, found[which * peak_count : (which + 1) * peak_count], 0.0)
        ref[8 : 8 + peak_count, :] = jnp.broadcast_to(
            jnp.sum(value, axis=1, keepdims=True), (peak_count, wide)
        )
    for peer in near:
        remote(
            last_other if peer[2] else last_mine, last_in.at[part], last_ssem, last_rsem, peer
        ).start()

    gather(0, 0, True)
    gather(1, 0, False)
    gather(0, 1, False)
    gather(1, 1, False)
    whole(last_in, parts - 1, last_ssem, last_rsem).wait_recv()
    last_in[part] = last_mine[...]
    total_ref[...] = sum(last_in[i] for i in range(1, parts)) + last_in[0]
    for turn in range(2):
        whole(send[turn], others, sar_ssem.at[turn], sar_rsem.at[turn]).wait_send()
        whole(opt_in.at[turn], parts - 1, opt_ssem.at[turn], opt_rsem.at[turn]).wait_send()
        whole(lag_in.at[turn], parts - 1, lag_ssem.at[turn], lag_rsem.at[turn, 0]).wait_send()
    whole(last_in, parts - 1, last_ssem, last_rsem).wait_send()
    spot_copy.wait_send()


def finish(bands, pieces, surface_ref, total_ref, out_ref, peak_ref, scaled, sem):
    _, lines, extent = surface_ref.shape
    pixels = extent * extent
    peak_count = peak_ref.shape[1]
    width = total_ref.shape[1]
    o_all = jnp.sum(total_ref[0:1, :], axis=1, keepdims=True) / (float(pixels) * bands * pixels)
    s_all = jnp.sum(total_ref[1:2, :], axis=1, keepdims=True) / (float(pixels) * bands * pixels)
    norm = lax.rsqrt(bands * pixels * (o_all + EPSILON) * (s_all + EPSILON)) / pixels
    part = lines // pieces
    copies = []
    for i in range(pieces):
        at = pl.ds(i * part, part)
        scaled[at, :] = surface_ref[0, at, :] * norm
        copy = pltpu.make_async_copy(scaled.at[at], out_ref.at[0, at], sem.at[i])
        copy.start()
        copies.append(copy)
    values = total_ref[8 : 8 + peak_count, :] * norm
    lane = lax.broadcasted_iota(jnp.int32, (peak_count, width), 1)
    rank = lax.broadcasted_iota(jnp.int32, (peak_count, width), 0)
    row = jnp.sum(jnp.where(lane == rank, values, 0.0), axis=0, keepdims=True)
    peak_ref[...] = row[:, :peak_count]
    for copy in copies:
        copy.wait()


def fused(mesh, optical, sar, destination, peaks):
    tiles, halves, bands = mesh.shape["tile"], mesh.shape["half"], mesh.shape["band"]
    patch_dev, _, quarter, extent = optical.shape
    group = tiles * halves
    parts = halves * bands
    lines = sar.shape[1] // group
    peak_count = peaks.shape[2]
    wide = extent // parts
    points = extent // 2
    sizes = (tiles, halves, bands, patch_dev, quarter, extent, lines, peak_count)
    tables = dft_tables(extent, parts)
    bf, f32 = jnp.bfloat16, jnp.float32
    vmem = pltpu.VMEM
    dma = pltpu.SemaphoreType.DMA
    raw, totals = pl.pallas_call(
        functools.partial(kernel, sizes),
        out_shape=(
            jax.ShapeDtypeStruct((1, quarter, extent), f32),
            jax.ShapeDtypeStruct((8 + peak_count, wide), f32),
        ),
        in_specs=[pl.BlockSpec(memory_space=pltpu.HBM)] * 8,
        out_specs=(pl.BlockSpec(memory_space=pltpu.VMEM), pl.BlockSpec(memory_space=pltpu.VMEM)),
        scratch_shapes=[
            pltpu.SMEM(destination.shape, jnp.int32),
            pltpu.SMEM(peaks.shape, jnp.int32),
            vmem((group, lines, extent), bf),
            vmem((patch_dev, quarter, extent), bf),
            vmem((extent, extent), bf),
            vmem((2, points, points), bf),
            vmem((2, points, points), bf),
            vmem((2, points, extent), bf),
            vmem((tiles * parts, lines, wide), bf),
            vmem((tiles * parts, lines, wide), bf),
            vmem((group * bands, lines, wide), bf),
            vmem((group * bands, lines, wide), bf),
            vmem((2, parts, quarter, wide), bf),
            vmem((2, parts, quarter, wide), bf),
            vmem((2, 2, patch_dev, 2, points, wide), f32),
            vmem((2, 2, patch_dev, points, wide), bf),
            vmem((2, 8, patch_dev * wide), f32),
            vmem((2, points, 2 * patch_dev * wide), bf),
            vmem((2 * patch_dev * wide, wide), bf),
            vmem((2, 2, points, wide), bf),
            vmem((2, extent, wide), bf),
            vmem((2, parts, quarter // 2, wide), bf),
            vmem((2, parts, quarter // 2, wide), bf),
            vmem((2 * peak_count, extent), bf),
            vmem((2 * peak_count, extent), bf),
            vmem((8 + peak_count, wide), f32),
            vmem((8 + peak_count, wide), f32),
            vmem((parts, 8 + peak_count, wide), f32),
            dma((8,)),
            dma((2,)),
            dma((2,)),
            dma((2,)),
            dma((2,)),
            dma((2,)),
            dma((2, 2)),
            dma,
            dma,
            dma,
            dma,
            pltpu.SemaphoreType.REGULAR,
            pltpu.SemaphoreType.REGULAR,
        ],
        compiler_params=pltpu.CompilerParams(
            collective_id=0, has_side_effects=True, vmem_limit_bytes=50 * 1024 * 1024
        ),
    )(
        *[
            pltpu.with_memory_space_constraint(x, pltpu.HBM)
            for x in (
                destination,
                peaks,
                sar.reshape(group, lines, extent),
                optical.reshape(patch_dev, quarter, extent),
                *[jnp.asarray(t) for t in tables],
            )
        ]
    )
    pieces = 4
    return pl.pallas_call(
        functools.partial(finish, bands, pieces),
        out_shape=(
            jax.ShapeDtypeStruct((1, quarter, extent), f32),
            jax.ShapeDtypeStruct((1, peak_count), f32),
        ),
        in_specs=[pl.BlockSpec(memory_space=pltpu.VMEM)] * 2,
        out_specs=(pl.BlockSpec(memory_space=pltpu.HBM), pl.BlockSpec(memory_space=pltpu.VMEM)),
        scratch_shapes=[vmem((quarter, extent), f32), dma((pieces,))],
    )(*[pltpu.with_memory_space_constraint(x, pltpu.VMEM) for x in (raw, totals)])


def fits(mesh, optical, sar, peaks):
    group = mesh.shape["tile"] * mesh.shape["half"]
    patch_dev, local_bands, quarter, extent = optical.shape
    lines = sar.shape[1] // group
    return (
        mesh.shape["half"] == 2
        and mesh.shape["band"] == 2
        and patch_dev == 2
        and local_bands == 1
        and lines % 16 == 0
        and quarter * 2 == extent
        and group * lines == patch_dev * quarter
        and extent % 512 == 0
        and peaks.shape[0] == 1
        and peaks.shape[2] % 8 == 0
    )


def solution(mesh):
    def local(optical, sar, destination, peaks):
        if fits(mesh, optical, sar, peaks):
            return fused(mesh, optical, sar, destination, peaks)
        return generic(optical, sar, destination, peaks)

    in_specs = (
        P(("scene", "tile"), "band", "half", None),
        P("band", ("scene", "tile", "half"), None),
        P("scene"),
        P(("scene", "tile", "band"), None, None),
    )
    out_specs = (P(("scene", "tile", "band"), "half", None), P(("scene", "tile", "band"), None))
    return jax.shard_map(local, mesh=mesh, in_specs=in_specs, out_specs=out_specs, check_vma=False)
```

```python
import functools
import math

import jax
import jax.numpy as jnp
import numpy as np
from jax import lax
from jax.experimental import pallas as pl
from jax.experimental.pallas import tpu as pltpu
from jax.sharding import PartitionSpec as P

MESH = pl.DeviceIdType.MESH

precise = lax.Precision.HIGHEST
EPSILON = 1e-06
BLOCK = 16


def fourier_tables(extent):
    places = jnp.arange(extent, dtype=jnp.int32)
    phases = places[:, None] * places[None, :] % extent
    angles = phases.astype(jnp.float32) * (2.0 * math.pi / extent)
    return (jnp.cos(angles), jnp.sin(angles))


def fourier_pair(table):
    upper = table.astype(jnp.bfloat16)
    lower = (table - upper.astype(jnp.float32)).astype(jnp.bfloat16)
    return (upper, lower)


def column_spectrum(samples, table_upper, table_lower):
    extent = samples.shape[-1]
    values = samples.reshape(-1, extent)
    spectrum = jnp.dot(values, table_upper, preferred_element_type=jnp.float32) + jnp.dot(
        values, table_lower, preferred_element_type=jnp.float32
    )
    return spectrum.astype(jnp.bfloat16).reshape(samples.shape[:-1] + (2 * extent,))


def row_spectrum(columns, table_upper, table_lower):
    line_count = columns.shape[-3]
    stacked = jnp.concatenate([columns[..., 0, :], columns[..., 1, :]], axis=-2)
    result = jnp.einsum("kr,...rc->...kc", table_upper, stacked, preferred_element_type=jnp.float32)
    result = result + jnp.einsum(
        "kr,...rc->...kc", table_lower, stacked, preferred_element_type=jnp.float32
    )
    return (result[..., :line_count, :], result[..., line_count:, :])


def relay_blocks(parcel):
    layout = parcel.shape
    merged = parcel.reshape(layout[:1] + (layout[1] * layout[2],) + layout[3:])
    arrived = lax.all_to_all(merged, ("tile", "half"), split_axis=1, concat_axis=1, tiled=True)
    return arrived.reshape(layout)


def generic(optical, sar, destination, peaks):
    tile_count = lax.axis_size("tile")
    half_count = lax.axis_size("half")
    band_count = lax.axis_size("band")
    group_size = tile_count * half_count
    patch_dev, local_bands, quarter, extent = optical.shape
    col_width = extent // half_count
    block_lines = sar.shape[1] // group_size
    band_total = local_bands * band_count
    pixel_count = extent * extent
    patch_total = patch_dev * tile_count
    kept_patches = patch_dev // band_count
    cosine_table, sine_table = fourier_tables(extent)
    col_upper, col_lower = fourier_pair(jnp.concatenate([cosine_table, -sine_table], axis=1))
    row_full = jnp.concatenate(
        [
            jnp.concatenate([cosine_table, sine_table], axis=1),
            jnp.concatenate([-sine_table, cosine_table], axis=1),
        ],
        axis=0,
    )
    row_upper, row_lower = fourier_pair(row_full)
    tile_at = lax.axis_index("tile")
    half_at = lax.axis_index("half")
    band_at = lax.axis_index("band")
    device_at = lax.axis_index(("tile", "half"))
    own_blocks = lax.dynamic_slice_in_dim(destination, device_at * group_size, group_size)
    send_order = jnp.argsort(own_blocks // group_size)
    inverse = (
        jnp.zeros_like(destination)
        .at[destination]
        .set(jnp.arange(destination.shape[0], dtype=jnp.int32))
    )
    opt_values = optical.astype(jnp.float32)
    opt_sums = jnp.sum(opt_values, axis=(2, 3))
    opt_squares = jnp.sum(opt_values * opt_values, axis=(2, 3))
    sar_values = sar.astype(jnp.float32).reshape(local_bands, group_size, block_lines * extent)
    sar_sums = jnp.sum(sar_values, axis=2)
    sar_squares = jnp.sum(sar_values * sar_values, axis=2)
    map_device = own_blocks // group_size
    map_patch = (
        map_device // half_count * patch_dev + own_blocks % group_size * block_lines // quarter
    )
    member = (map_patch[:, None] == jnp.arange(patch_total, dtype=jnp.int32)[None, :]).astype(
        jnp.float32
    )
    sar_stats = jnp.dot(
        jnp.stack([sar_sums, sar_squares]).reshape(2 * local_bands, group_size),
        member,
        precision=precise,
        preferred_element_type=jnp.float32,
    )
    statistics = jnp.zeros((2, 2, band_total, patch_total), jnp.float32)
    opt_part = jnp.transpose(jnp.stack([opt_sums, opt_squares]), (0, 2, 1))
    statistics = lax.dynamic_update_slice(
        statistics, opt_part[None], (0, 0, band_at * local_bands, tile_at * patch_dev)
    )
    statistics = lax.dynamic_update_slice(
        statistics,
        sar_stats.reshape(2, local_bands, patch_total)[None],
        (1, 0, band_at * local_bands, 0),
    )
    totals = lax.psum(statistics, ("tile", "half", "band"))
    centered = totals[:, 1] - totals[:, 0] * totals[:, 0] / pixel_count
    energy = jnp.sum(centered, axis=1) / (band_total * pixel_count)
    norm_scale = lax.rsqrt(band_total * pixel_count * (energy[0] + EPSILON) * (energy[1] + EPSILON))
    first_patch = tile_at * patch_dev + band_at * kept_patches
    norm_mine = lax.dynamic_slice_in_dim(norm_scale, first_patch, kept_patches)
    slant_spectra = column_spectrum(sar, col_upper, col_lower).reshape(
        local_bands, group_size, block_lines, 2, half_count, col_width
    )
    outgoing = jnp.take(slant_spectra, send_order, axis=1).reshape(
        local_bands, tile_count, half_count, block_lines, 2, half_count, col_width
    )
    outgoing = jnp.transpose(outgoing, (0, 1, 5, 2, 3, 4, 6))
    arrived = relay_blocks(outgoing).reshape(
        local_bands, group_size * half_count, block_lines, 2, col_width
    )
    sources = lax.dynamic_slice_in_dim(
        inverse, tile_at * half_count * group_size, half_count * group_size
    )
    slot_index = (
        sources // group_size * half_count
        + jnp.arange(half_count * group_size, dtype=jnp.int32) // group_size
    )
    placed = jnp.take(arrived, slot_index, axis=1).reshape(
        local_bands, half_count, patch_dev, quarter, 2, col_width
    )
    placed = jnp.transpose(placed, (2, 0, 1, 3, 4, 5)).reshape(
        patch_dev, local_bands, extent, 2, col_width
    )
    sar_real, sar_imag = row_spectrum(placed, row_upper, row_lower)
    spectra = column_spectrum(optical, col_upper, col_lower).reshape(
        patch_dev, local_bands, quarter, 2, half_count, col_width
    )
    real_part, imag_part = row_spectrum(
        jnp.squeeze(
            lax.all_to_all(spectra, "half", split_axis=4, concat_axis=2, tiled=True), axis=4
        ),
        row_upper,
        row_lower,
    )
    opt_real = real_part
    opt_imag = imag_part
    rows_at = jnp.arange(extent, dtype=jnp.int32)[:, None]
    cols_at = half_at * col_width + jnp.arange(col_width, dtype=jnp.int32)[None, :]
    keep_mask = jnp.where((rows_at == 0) & (cols_at == 0), 0.0, 1.0).astype(jnp.float32)
    opt_real = opt_real * keep_mask
    opt_imag = opt_imag * keep_mask
    sar_real = sar_real * keep_mask
    sar_imag = sar_imag * keep_mask
    cross_real = jnp.sum(opt_real * sar_real + opt_imag * sar_imag, axis=1)
    cross_imag = jnp.sum(opt_real * sar_imag - opt_imag * sar_real, axis=1)
    cross_term = jnp.stack([cross_real, cross_imag], axis=1)
    cross_sum = lax.psum_scatter(cross_term, "band", scatter_dimension=0, tiled=True)
    lag_real = (
        jnp.einsum("uk,pkc->puc", cosine_table, cross_sum[:, 0], precision=precise)
        - jnp.einsum("uk,pkc->puc", sine_table, cross_sum[:, 1], precision=precise)
    ) / extent
    lag_imag = (
        jnp.einsum("uk,pkc->puc", cosine_table, cross_sum[:, 1], precision=precise)
        + jnp.einsum("uk,pkc->puc", sine_table, cross_sum[:, 0], precision=precise)
    ) / extent
    lagged = jnp.stack([lag_real, lag_imag], axis=2).reshape(
        kept_patches, half_count, quarter, 2, col_width
    )
    pieces = lax.all_to_all(lagged, "half", split_axis=1, concat_axis=4, tiled=True)
    real_in = pieces[:, 0, :, 0, :]
    imag_in = pieces[:, 0, :, 1, :]
    correlation = (
        jnp.einsum("puc,cv->puv", real_in, cosine_table, precision=precise)
        - jnp.einsum("puc,cv->puv", imag_in, sine_table, precision=precise)
    ) / extent
    surface = correlation * norm_mine[:, None, None]
    local_rows = peaks[:, 0, :] - half_at * quarter
    row_hit = (
        local_rows[:, :, None] == jnp.arange(quarter, dtype=jnp.int32)[None, None, :]
    ).astype(jnp.float32)
    picked = jnp.einsum("pkr,prc->pkc", row_hit, surface, precision=precise)
    col_hit = (peaks[:, 1, :, None] == jnp.arange(extent, dtype=jnp.int32)[None, None, :]).astype(
        jnp.float32
    )
    local_values = jnp.sum(picked * col_hit, axis=2)
    peak_values = lax.psum(local_values, "half")
    return (surface, peak_values)


def dft_tables(extent, parts):
    points = extent // 2
    cols = points // parts // 2
    places = np.arange(extent)
    phases = (places[:, None] * places[None, :]) % extent
    cosine = np.cos(phases * (2.0 * np.pi / extent))
    sine = np.sin(phases * (2.0 * np.pi / extent))
    forward, backward = [], [[], []]
    for part in range(parts):
        for turn in range(2):
            first = (2 * part + turn) * cols
            span = slice(first, first + cols)
            real, imag = cosine[:, span].copy(), -sine[:, span]
            real_back, imag_back = 2.0 * cosine[span], -2.0 * sine[span]
            if first == 0:
                imag[:, 0] = cosine[:, points]
                real_back[0] = 1.0
                imag_back[0] = cosine[points]
            forward += [real, imag]
            backward[turn] += [real_back, imag_back]
    col_table = np.concatenate(forward, axis=1)
    back_table = np.stack([np.concatenate(b, axis=0) for b in backward])
    row_sine, lag_sine = sine[:points, :points].copy(), 2.0 * sine[:points, :points]
    row_cosine, lag_cosine = cosine[:points, :points], 2.0 * cosine[:points, :points]
    row_sine[0] = cosine[points, :points]
    lag_cosine[:, 0] = 1.0
    lag_sine[:, 0] = cosine[:points, points]


    def woven(a, b):
        both = np.stack([a.reshape(-1, BLOCK, points), b.reshape(-1, BLOCK, points)], axis=1)
        return both.reshape(points, points)

    row_table = np.stack([woven(row_cosine[i::2], row_sine[i::2]) for i in range(2)])
    lag_table = np.stack([woven(lag_cosine.T[i::2], lag_sine.T[i::2]).T for i in range(2)])
    return tuple(t.astype(jnp.bfloat16) for t in (col_table, row_table, lag_table, back_table))


def kernel(
    sizes,
    dest_hbm,
    peaks_hbm,
    sar_hbm,
    opt_hbm,
    col_hbm,
    row_hbm,
    lag_hbm,
    back_hbm,
    surface_ref,
    peak_ref,
    dest_ref,
    peaks_ref,
    sar_v,
    opt_v,
    col_v,
    row_v,
    lag_v,
    back_v,
    send_0,
    send_1,
    arrived_0,
    arrived_1,
    opt_send,
    opt_in,
    opt_waves,
    sar_cols,
    sar_head,
    unfolded,
    fold_v,
    cross,
    spot_rows,
    waves,
    picked,
    lag_send,
    lag_in,
    spot_send,
    spot_recv,
    last_mine,
    last_other,
    last_in,
    load_sem,
    sar_ssem,
    sar_rsem,
    opt_ssem,
    opt_rsem,
    lag_ssem,
    lag_rsem,
    last_ssem,
    last_rsem,
    spot_ssem,
    spot_rsem,
    near_sem,
    far_sem,
):
    tiles, halves, bands, patch_dev, quarter, extent, lines, peak_count = sizes
    group = tiles * halves
    parts = halves * bands
    wide = extent // parts
    side = wide // 2
    cols = wide // 4
    points = extent // 2
    per_patch = group // patch_dev
    block = BLOCK
    send, arrived = (send_0, send_1), (arrived_0, arrived_1)
    f32, bf = jnp.float32, jnp.bfloat16
    tile, half, band = lax.axis_index("tile"), lax.axis_index("half"), lax.axis_index("band")
    me = tile * halves + half
    part = half * bands + band
    other_half = 1 - half
    other_band = 1 - band

    def place(step, shift, swap):
        return (
            lax.rem(tile + step, tiles),
            lax.rem(half + shift, halves),
            lax.rem(band + swap, bands),
        )

    def device(step, shift, swap):
        return dict(zip(("tile", "half", "band"), place(step, shift, swap)))

    others = tiles * parts - 1
    near = [(0, shift, swap) for shift in (1, 0) for swap in range(bands) if shift or swap]

    loads = [
        pltpu.make_async_copy(a, b, load_sem.at[i])
        for i, (a, b) in enumerate(
            [(dest_hbm, dest_ref), (sar_hbm, sar_v), (col_hbm, col_v), (opt_hbm, opt_v),
             (row_hbm, row_v), (peaks_hbm, peaks_ref), (lag_hbm, lag_v), (back_hbm, back_v)]
        )
    ]
    for i in (3, 2, 0, 1):
        loads[i].start()

    barrier = pltpu.get_barrier_semaphore()
    first_band, last_band = jnp.int32(0), jnp.int32(bands - 1)

    def tell(semaphore, **where):
        pl.semaphore_signal(semaphore, inc=1, device_id=where, device_id_type=MESH)

    for shift in range(1, halves):
        tell(barrier, half=lax.rem(half + shift, halves), band=first_band)
    pl.when(band != first_band)(lambda: tell(barrier, band=first_band))
    for step in sorted(range(1, tiles), key=lambda s: -min(s, tiles - s)):
        for shift in range(halves):
            tell(
                barrier,
                tile=lax.rem(tile + step, tiles),
                half=lax.rem(half + shift, halves),
                band=last_band,
            )

    def remote(src, dst, ssem, rsem, peer):
        return pltpu.make_async_remote_copy(
            src_ref=src,
            dst_ref=dst,
            send_sem=ssem,
            recv_sem=rsem,
            device_id=device(*peer),
            device_id_type=MESH,
        )

    source_at = me * bands + band

    def sar_copy(turn, to_tile, to_half, to_band):
        return pltpu.make_async_remote_copy(
            src_ref=send[turn].at[to_tile * parts + to_half * bands + to_band],
            dst_ref=arrived[turn].at[source_at],
            send_sem=sar_ssem.at[turn],
            recv_sem=sar_rsem.at[turn],
            device_id={"tile": to_tile, "half": to_half, "band": to_band},
            device_id_type=MESH,
        )

    low = lax.broadcasted_iota(jnp.int32, (1, wide), 1) < side

    def pair(a, b):
        first = jnp.concatenate([a[:, :side], b[:, :side]], axis=1)
        second = jnp.concatenate([a[:, side:], b[:, side:]], axis=1)
        return first, second

    def whole(ref, count, ssem, rsem):
        ref = ref.at[pl.ds(0, count)]
        return remote(ref, ref, ssem, rsem, (0, 1, 0))

    loads[0].wait()
    own_runs = [lax.div(dest_ref[me * group + j], group) for j in range(group)]

    def block_for(run):
        found = jnp.int32(0)
        for j in range(group):
            found = jnp.where(own_runs[j] == run, j, found)
        return found

    def sar_columns(to_tile):
        if to_tile == 0:
            loads[1].wait()
        samples = jnp.concatenate(
            [
                sar_v[block_for(to_tile * halves + lax.rem(run + band, halves))]
                for run in range(halves)
            ],
            axis=0,
        )
        spectra = jnp.dot(samples, col_v[...], preferred_element_type=f32).astype(bf)
        for to in range(parts):
            at = slice(to * wide, (to + 1) * wide)
            first, second = pair(spectra[:lines, at], spectra[lines:, at])
            send_0[to_tile * parts + to] = first
            send_1[to_tile * parts + to] = second

    def sar_sends(turn, to_tile, shifts):
        for shift in shifts:
            to_half = lax.rem(half + shift, halves)
            for swap in range(bands):
                to_band = lax.rem(band + swap, bands)
                copy = sar_copy(turn, to_tile, to_half, to_band)
                if shift or swap:
                    copy.start()
                else:
                    pl.when(tile != to_tile)(copy.start)

    def opt_copy(turn, peer):
        _, to_half, to_band = place(*peer)
        return remote(
            opt_send.at[turn, to_half * bands + to_band],
            opt_in.at[turn, part],
            opt_ssem.at[turn],
            opt_rsem.at[turn],
            peer,
        )

    def opt_sends(turn):
        for peer in near:
            opt_copy(turn, peer).start()

    loads[3].wait()
    loads[2].wait()
    opt_spectra = [
        jnp.dot(opt_v[lax.rem(patch + band, patch_dev)], col_v[...], preferred_element_type=f32).astype(bf)
        for patch in range(patch_dev)
    ]
    for to in range(parts):
        at = slice(to * wide, (to + 1) * wide)
        first, second = pair(*[s[:, at] for s in opt_spectra])
        opt_send[0, to] = first
        opt_send[1, to] = second
    @pl.when(band == first_band)
    def _():
        pl.semaphore_wait(barrier, parts - 1)
        tell(near_sem, band=last_band)

    @pl.when(band == last_band)
    def _():
        pl.semaphore_wait(near_sem, 1)

    opt_sends(0)
    opt_sends(1)
    sar_columns(0)
    for i in (4, 5, 6, 7):
        loads[i].start()

    @pl.when(band == last_band)
    def _():
        pl.semaphore_wait(barrier, (tiles - 1) * parts)
        tell(far_sem, band=first_band)

    @pl.when(band == first_band)
    def _():
        pl.semaphore_wait(far_sem, 1)

    sar_sends(0, 0, (0, 1))
    for to_tile in range(1, tiles):
        sar_columns(to_tile)
        if to_tile > 1:
            sar_sends(0, to_tile, (0, 1))
        else:
            sar_sends(1, 0, (0, 1))
            sar_sends(0, 1, (0, 1))
    for to_tile in range(1, tiles):
        sar_sends(1, to_tile, (0, 1))
    arrived_0[source_at] = send_0[tile * parts + part]
    arrived_1[source_at] = send_1[tile * parts + part]
    for turn in range(2):
        opt_in[turn, part] = opt_send[turn, part]

    slot_of = []
    for run in range(halves):
        places = []
        for source in range(group):
            found = jnp.int32(0)
            for j in range(group):
                spot = dest_ref[source * group + j]
                found = jnp.where(
                    lax.div(spot, group) == tile * halves + run, lax.rem(spot, group), found
                )
            places.append(found)
        for slot in range(group):
            found = jnp.int32(0)
            for source in range(group):
                found = jnp.where(places[source] == slot, source, found)
            slot_of.append(found)

    spots = lax.broadcasted_iota(jnp.int32, (peak_count, extent), 1)
    ranks = lax.broadcasted_iota(jnp.int32, (peak_count, extent), 0)
    loads[5].wait()
    for which in range(2):
        wanted = jnp.zeros((peak_count, extent), jnp.int32)
        for j in range(peak_count):
            wanted = jnp.where(ranks == j, peaks_ref[0, which, j], wanted)
        spot_send[which * peak_count : (which + 1) * peak_count, :] = jnp.where(
            spots == wanted, 1.0, 0.0
        ).astype(bf)
    spot_copy = remote(spot_send, spot_recv, spot_ssem, spot_rsem, (0, 0, 1))
    spot_copy.start()

    lane = lax.broadcasted_iota(jnp.int32, (1, wide), 1)
    inner = lax.rem(lane, side)
    real_lane = inner < cols
    top = lax.broadcasted_iota(jnp.int32, (block, wide), 0) == 0
    edge_real = [((inner + part + turn) == 0) for turn in range(2)]
    edge_imag = [((jnp.abs(inner - cols) + part + turn) == 0) for turn in range(2)]
    weights = [
        jnp.where(edge_real[turn] | edge_imag[turn], 1.0, 2.0) * (0.5 * extent)
        for turn in range(2)
    ]

    def swapped(z):
        return pltpu.roll(z, side, 1)

    def crossed(z):
        return jnp.where(real_lane, pltpu.roll(z, wide - cols, 1), pltpu.roll(z, cols, 1))

    def turned(z):
        return jnp.where(real_lane, -pltpu.roll(z, wide - cols, 1), pltpu.roll(z, cols, 1))

    opt_energy = [0.0] * patch_dev

    def energy_of(even, odd, head, turn):
        shifted = even.astype(f32) - jnp.where(edge_real[turn], head * (2.0 / extent), 0.0)
        odd = odd.astype(f32)
        total = jnp.sum(shifted * shifted + odd * odd, axis=0, keepdims=True)
        return total * weights[turn]

    def optical(turn):
        whole(opt_in.at[turn], parts - 1, opt_ssem.at[turn], opt_rsem.at[turn]).wait_recv()
        real, imag = edge_real[turn], edge_imag[turn]
        pieces = [[opt_in[turn, run * bands + b] for b in range(bands)] for run in range(halves)]
        mixed = []
        for patch in range(patch_dev):
            near_x, far_x = [jnp.where(low, p[patch], p[1 - patch]) for p in pieces]
            mixed.append((near_x + far_x, near_x - far_x))
        for parity in range(2):
            plain = [jnp.where(imag, 0.0, m[parity]).astype(bf) for m in mixed]
            crossed_x = [
                jnp.where(real, 0.0, jnp.where(imag, m[parity], turned(m[parity]))).astype(bf)
                for m in mixed
            ]
            rows = jnp.dot(
                row_v[parity], jnp.concatenate(plain + crossed_x, axis=1), preferred_element_type=f32
            )
            for kind in range(2):
                for patch in range(patch_dev):
                    at = (kind * patch_dev + patch) * wide
                    opt_waves[turn, kind, patch, parity] = rows[:, at : at + wide]
        for patch in range(patch_dev):
            head = opt_waves[turn, 0, patch, 0, :block]
            opt_energy[patch] = opt_energy[patch] + energy_of(*mixed[patch], head[0:1], turn)
            opt_waves[turn, 0, patch, 0, :block] = jnp.where(real & top, 0.0, head)

    tall = (2 * patch_dev * wide, wide)
    fold_row = lax.broadcasted_iota(jnp.int32, tall, 0)
    fold_lane = lax.broadcasted_iota(jnp.int32, tall, 1)
    fold_v[...] = jnp.where(
        (lax.div(fold_row, wide) == lax.div(fold_lane, cols))
        & (lax.rem(fold_row, cols) == lax.rem(fold_lane, cols)),
        1.0,
        0.0,
    ).astype(bf)

    def slant(turn):
        whole(arrived[turn], others, sar_ssem.at[turn], sar_rsem.at[turn]).wait_recv()
        for slot in range(group):
            patch, at = slot // per_patch, slot % per_patch * lines
            ends = []
            for run in range(halves):
                source = slot_of[run * group + slot] * bands
                piece = jnp.where(
                    low, arrived[turn][source + run], arrived[turn][source + 1 - run]
                )
                if patch != run:
                    piece = jnp.concatenate([piece[:, side:], piece[:, :side]], axis=1)
                ends.append(piece)
            sar_cols[turn, 0, patch, at : at + lines, :] = ends[0] + ends[1]
            sar_cols[turn, 1, patch, at : at + lines, :] = ends[0] - ends[1]
        for parity in range(2):
            both = [sar_cols[turn, parity, patch] for patch in range(patch_dev)]
            rows = jnp.dot(
                row_v[parity], jnp.concatenate(both, axis=1), preferred_element_type=f32
            )
            if parity == 0:
                sar_head[turn] = rows[:8]
            for b in range(points // 2 // block):
                at = slice(2 * b * block, (2 * b + 1) * block)
                lower = slice((2 * b + 1) * block, (2 * b + 2) * block)
                sums = []
                for patch in range(patch_dev):
                    yc, ys = [rows[i, patch * wide : (patch + 1) * wide] for i in (at, lower)]
                    zc, zs = [opt_waves[turn, 0, patch, parity, i] for i in (at, lower)]
                    tc, ts = [opt_waves[turn, 1, patch, parity, i] for i in (at, lower)]
                    zs_e, ts_e, zc_d, tc_d = zs, ts, zc, tc
                    if b == 0 and parity == 0:
                        zs_e, ts_e = jnp.where(top, 0.0, zs), jnp.where(top, 0.0, ts)
                        zc_d, tc_d = jnp.where(top, zs, zc), jnp.where(top, ts, tc)
                    sums.append(
                        (
                            zc * yc + zs_e * ys,
                            tc * yc + ts_e * ys,
                            zc_d * ys - zs_e * yc,
                            tc_d * ys - ts_e * yc,
                        )
                    )
                for patch in range(patch_dev):
                    for k in range(2):
                        lanes = slice((2 * patch + k) * wide, (2 * patch + k + 1) * wide)
                        unfolded[parity, at, lanes] = sums[patch][k].astype(bf)
                        unfolded[parity, lower, lanes] = sums[patch][2 + k].astype(bf)
            cross[turn, parity] = jnp.dot(
                unfolded[parity], fold_v[...], preferred_element_type=f32
            ).astype(bf)

    def lag_copy(turn, peer):
        _, to_half, to_band = place(*peer)
        return remote(
            lag_send.at[turn, to_half * bands + to_band],
            lag_in.at[turn, part],
            lag_ssem.at[turn],
            lag_rsem.at[turn, peer[1]],
            peer,
        )

    def lag_sends(turn, shift):
        for swap in range(bands):
            if shift or swap:
                lag_copy(turn, (0, shift, swap)).start()

    def spread(turn):
        even, odd = [
            jnp.dot(
                jnp.concatenate([lag_v[parity], spot_rows[parity]], axis=0),
                cross[turn, parity],
                preferred_element_type=f32,
            )
            for parity in range(2)
        ]
        picked[turn] = even[points:] + odd[points:]
        even, odd = even[:points], odd[:points]
        flip = jnp.where(half == 0, -1.0, 1.0)
        for shift, to_half in ((1, other_half), (0, half)):
            values = (even + odd * flip if shift else even - odd * flip).astype(bf)
            for patch, piece in enumerate(pair(values[: quarter // 2], values[quarter // 2 :])):
                lag_send[turn, to_half * bands + patch] = piece
            lag_sends(turn, shift)
        lag_in[turn, part] = lag_send[turn, part]

    def gather(turn, shift, first=False, last=False):
        from_half = lax.rem(half + shift, halves)
        count = bands if shift else bands - 1
        whole(lag_in.at[turn], count, lag_ssem.at[turn], lag_rsem.at[turn, shift]).wait_recv()
        if last:
            whole(last_in, parts - 1, last_ssem, last_rsem).wait_recv()
        upper, lower = pair(*[lag_in[turn, from_half * bands + b] for b in range(bands)])
        table = back_v[turn, pl.ds(pl.multiple_of(from_half * wide, wide), wide), :]
        values = jnp.dot(
            jnp.concatenate([upper, lower], axis=0), table, preferred_element_type=f32
        )
        if first:
            surface_ref[0] = values
        elif last:
            surface_ref[0] = (surface_ref[0] + values) * norm()
        else:
            surface_ref[0] = surface_ref[0] + values

    pixels = extent * extent

    def norm():
        total = last_in[0]
        for i in range(1, parts):
            total = total + last_in[i]
        energies = jnp.sum(total[0:8], axis=1, keepdims=True) / (float(pixels) * bands * pixels)
        energies = energies + EPSILON
        scale = lax.rsqrt(bands * pixels * energies[0:1] * energies[1:2]) / pixels
        at = lax.broadcasted_iota(jnp.int32, (peak_count, wide), 1)
        rank = lax.broadcasted_iota(jnp.int32, (peak_count, wide), 0)
        row = jnp.where(at == rank, total[8 : 8 + peak_count], 0.0)
        peak_ref[...] = (jnp.sum(row, axis=0, keepdims=True) * scale)[:, :peak_count]
        return scale

    loads[4].wait()
    loads[6].wait()
    loads[7].wait()
    spot_copy.wait_recv()
    spots_all = jnp.concatenate([spot_send[:peak_count], spot_recv[:peak_count]], axis=0)
    lags_all = jnp.concatenate([spot_send[peak_count:], spot_recv[peak_count:]], axis=0)
    upper_spots, lower_spots = spots_all[:, :points], spots_all[:, points:]
    for parity in range(2):
        spots_now = upper_spots + lower_spots if parity == 0 else upper_spots - lower_spots
        spot_rows[parity] = jnp.dot(
            spots_now, lag_v[parity], preferred_element_type=f32
        ).astype(bf)
    for turn in range(2):
        rows_back = back_v[turn, pl.ds(pl.multiple_of(part * side, side), side), :]
        waves[turn] = lax.dot_general(
            lags_all,
            jnp.concatenate([rows_back, rows_back], axis=0),
            (((1,), (1,)), ((), ())),
            preferred_element_type=f32,
        )
    optical(0)
    optical(1)
    slant(0)
    spread(0)
    slant(1)
    spread(1)

    sar_energy = [0.0] * patch_dev
    for patch in range(patch_dev):
        for turn in range(2):
            energy = energy_of(
                sar_cols[turn, 0, patch],
                sar_cols[turn, 1, patch],
                sar_head[turn, 0:1, patch * wide : (patch + 1) * wide],
                turn,
            )
            sar_energy[patch] = sar_energy[patch] + energy

    found = picked[0] * waves[0] + picked[1] * waves[1]
    for which, patch, ref in ((0, band, last_mine), (1, other_band, last_other)):
        mine = lax.div(lane, side) == patch
        ref[0:8, :] = jnp.zeros((8, wide), f32)
        ref[0:1, :] = jnp.where(patch == 0, opt_energy[0], opt_energy[1])
        ref[1:2, :] = jnp.where(patch == 0, sar_energy[0], sar_energy[1])
        value = jnp.where(mine, found[which * peak_count : (which + 1) * peak_count], 0.0)
        ref[8 : 8 + peak_count, :] = jnp.broadcast_to(
            jnp.sum(value, axis=1, keepdims=True), (peak_count, wide)
        )
    for peer in near:
        remote(
            last_other if peer[2] else last_mine, last_in.at[part], last_ssem, last_rsem, peer
        ).start()

    last_in[part] = last_mine[...]
    gather(0, 0, first=True)
    gather(1, 0)
    gather(0, 1)
    gather(1, 1, last=True)
    for turn in range(2):
        whole(send[turn], others, sar_ssem.at[turn], sar_rsem.at[turn]).wait_send()
        whole(opt_in.at[turn], parts - 1, opt_ssem.at[turn], opt_rsem.at[turn]).wait_send()
        whole(lag_in.at[turn], parts - 1, lag_ssem.at[turn], lag_rsem.at[turn, 0]).wait_send()
    whole(last_in, parts - 1, last_ssem, last_rsem).wait_send()
    spot_copy.wait_send()


def finish(surface_ref, peak_in, out_ref, peak_ref, sem):
    copies = [
        pltpu.make_async_copy(a, b, sem.at[i])
        for i, (a, b) in enumerate([(surface_ref, out_ref), (peak_in, peak_ref)])
    ]
    for copy in copies:
        copy.start()
    for copy in copies:
        copy.wait()


def fused(mesh, optical, sar, destination, peaks):
    tiles, halves, bands = mesh.shape["tile"], mesh.shape["half"], mesh.shape["band"]
    patch_dev, _, quarter, extent = optical.shape
    group = tiles * halves
    parts = halves * bands
    lines = sar.shape[1] // group
    peak_count = peaks.shape[2]
    wide = extent // parts
    points = extent // 2
    sizes = (tiles, halves, bands, patch_dev, quarter, extent, lines, peak_count)
    tables = dft_tables(extent, parts)
    bf, f32 = jnp.bfloat16, jnp.float32
    vmem = pltpu.VMEM
    dma = pltpu.SemaphoreType.DMA
    raw, values = pl.pallas_call(
        functools.partial(kernel, sizes),
        out_shape=(
            jax.ShapeDtypeStruct((1, quarter, extent), f32),
            jax.ShapeDtypeStruct((1, peak_count), f32),
        ),
        in_specs=[pl.BlockSpec(memory_space=pltpu.HBM)] * 8,
        out_specs=(pl.BlockSpec(memory_space=pltpu.VMEM), pl.BlockSpec(memory_space=pltpu.VMEM)),
        scratch_shapes=[
            pltpu.SMEM(destination.shape, jnp.int32),
            pltpu.SMEM(peaks.shape, jnp.int32),
            vmem((group, lines, extent), bf),
            vmem((patch_dev, quarter, extent), bf),
            vmem((extent, extent), bf),
            vmem((2, points, points), bf),
            vmem((2, points, points), bf),
            vmem((2, points, extent), bf),
            vmem((tiles * parts, lines, wide), bf),
            vmem((tiles * parts, lines, wide), bf),
            vmem((group * bands, lines, wide), bf),
            vmem((group * bands, lines, wide), bf),
            vmem((2, parts, quarter, wide), bf),
            vmem((2, parts, quarter, wide), bf),
            vmem((2, 2, patch_dev, 2, points, wide), f32),
            vmem((2, 2, patch_dev, points, wide), bf),
            vmem((2, 8, patch_dev * wide), f32),
            vmem((2, points, 2 * patch_dev * wide), bf),
            vmem((2 * patch_dev * wide, wide), bf),
            vmem((2, 2, points, wide), bf),
            vmem((2, 2 * peak_count, points), bf),
            vmem((2, 2 * peak_count, wide), f32),
            vmem((2, 2 * peak_count, wide), f32),
            vmem((2, parts, quarter // 2, wide), bf),
            vmem((2, parts, quarter // 2, wide), bf),
            vmem((2 * peak_count, extent), bf),
            vmem((2 * peak_count, extent), bf),
            vmem((8 + peak_count, wide), f32),
            vmem((8 + peak_count, wide), f32),
            vmem((parts, 8 + peak_count, wide), f32),
            dma((8,)),
            dma((2,)),
            dma((2,)),
            dma((2,)),
            dma((2,)),
            dma((2,)),
            dma((2, 2)),
            dma,
            dma,
            dma,
            dma,
            pltpu.SemaphoreType.REGULAR,
            pltpu.SemaphoreType.REGULAR,
        ],
        compiler_params=pltpu.CompilerParams(
            collective_id=0, has_side_effects=True, vmem_limit_bytes=50 * 1024 * 1024
        ),
    )(
        *[
            pltpu.with_memory_space_constraint(x, pltpu.HBM)
            for x in (
                destination,
                peaks,
                sar.reshape(group, lines, extent),
                optical.reshape(patch_dev, quarter, extent),
                *[jnp.asarray(t) for t in tables],
            )
        ]
    )
    return pl.pallas_call(
        finish,
        out_shape=(
            jax.ShapeDtypeStruct((1, quarter, extent), f32),
            jax.ShapeDtypeStruct((1, peak_count), f32),
        ),
        in_specs=[pl.BlockSpec(memory_space=pltpu.VMEM)] * 2,
        out_specs=(pl.BlockSpec(memory_space=pltpu.HBM), pl.BlockSpec(memory_space=pltpu.HBM)),
        scratch_shapes=[dma((2,))],
    )(*[pltpu.with_memory_space_constraint(x, pltpu.VMEM) for x in (raw, values)])


def fits(mesh, optical, sar, peaks):
    group = mesh.shape["tile"] * mesh.shape["half"]
    patch_dev, local_bands, quarter, extent = optical.shape
    lines = sar.shape[1] // group
    return (
        mesh.shape["half"] == 2
        and mesh.shape["band"] == 2
        and patch_dev == 2
        and local_bands == 1
        and lines % 16 == 0
        and quarter * 2 == extent
        and group * lines == patch_dev * quarter
        and extent % 512 == 0
        and peaks.shape[0] == 1
        and peaks.shape[2] % 8 == 0
    )


def solution(mesh):
    def local(optical, sar, destination, peaks):
        if fits(mesh, optical, sar, peaks):
            return fused(mesh, optical, sar, destination, peaks)
        return generic(optical, sar, destination, peaks)

    in_specs = (
        P(("scene", "tile"), "band", "half", None),
        P("band", ("scene", "tile", "half"), None),
        P("scene"),
        P(("scene", "tile", "band"), None, None),
    )
    out_specs = (P(("scene", "tile", "band"), "half", None), P(("scene", "tile", "band"), None))
    return jax.shard_map(local, mesh=mesh, in_specs=in_specs, out_specs=out_specs, check_vma=False)
```

```python
import functools
import math

import jax
import jax.numpy as jnp
import numpy as np
from jax import lax
from jax.experimental import pallas as pl
from jax.experimental.pallas import tpu as pltpu
from jax.sharding import PartitionSpec as P

MESH = pl.DeviceIdType.MESH

precise = lax.Precision.HIGHEST
EPSILON = 1e-06
BLOCK = 16


def fourier_tables(extent):
    places = jnp.arange(extent, dtype=jnp.int32)
    phases = places[:, None] * places[None, :] % extent
    angles = phases.astype(jnp.float32) * (2.0 * math.pi / extent)
    return (jnp.cos(angles), jnp.sin(angles))


def fourier_pair(table):
    upper = table.astype(jnp.bfloat16)
    lower = (table - upper.astype(jnp.float32)).astype(jnp.bfloat16)
    return (upper, lower)


def column_spectrum(samples, table_upper, table_lower):
    extent = samples.shape[-1]
    values = samples.reshape(-1, extent)
    spectrum = jnp.dot(values, table_upper, preferred_element_type=jnp.float32) + jnp.dot(
        values, table_lower, preferred_element_type=jnp.float32
    )
    return spectrum.astype(jnp.bfloat16).reshape(samples.shape[:-1] + (2 * extent,))


def row_spectrum(columns, table_upper, table_lower):
    line_count = columns.shape[-3]
    stacked = jnp.concatenate([columns[..., 0, :], columns[..., 1, :]], axis=-2)
    result = jnp.einsum("kr,...rc->...kc", table_upper, stacked, preferred_element_type=jnp.float32)
    result = result + jnp.einsum(
        "kr,...rc->...kc", table_lower, stacked, preferred_element_type=jnp.float32
    )
    return (result[..., :line_count, :], result[..., line_count:, :])


def relay_blocks(parcel):
    layout = parcel.shape
    merged = parcel.reshape(layout[:1] + (layout[1] * layout[2],) + layout[3:])
    arrived = lax.all_to_all(merged, ("tile", "half"), split_axis=1, concat_axis=1, tiled=True)
    return arrived.reshape(layout)


def generic(optical, sar, destination, peaks):
    tile_count = lax.axis_size("tile")
    half_count = lax.axis_size("half")
    band_count = lax.axis_size("band")
    group_size = tile_count * half_count
    patch_dev, local_bands, quarter, extent = optical.shape
    col_width = extent // half_count
    block_lines = sar.shape[1] // group_size
    band_total = local_bands * band_count
    pixel_count = extent * extent
    patch_total = patch_dev * tile_count
    kept_patches = patch_dev // band_count
    cosine_table, sine_table = fourier_tables(extent)
    col_upper, col_lower = fourier_pair(jnp.concatenate([cosine_table, -sine_table], axis=1))
    row_full = jnp.concatenate(
        [
            jnp.concatenate([cosine_table, sine_table], axis=1),
            jnp.concatenate([-sine_table, cosine_table], axis=1),
        ],
        axis=0,
    )
    row_upper, row_lower = fourier_pair(row_full)
    tile_at = lax.axis_index("tile")
    half_at = lax.axis_index("half")
    band_at = lax.axis_index("band")
    device_at = lax.axis_index(("tile", "half"))
    own_blocks = lax.dynamic_slice_in_dim(destination, device_at * group_size, group_size)
    send_order = jnp.argsort(own_blocks // group_size)
    inverse = (
        jnp.zeros_like(destination)
        .at[destination]
        .set(jnp.arange(destination.shape[0], dtype=jnp.int32))
    )
    opt_values = optical.astype(jnp.float32)
    opt_sums = jnp.sum(opt_values, axis=(2, 3))
    opt_squares = jnp.sum(opt_values * opt_values, axis=(2, 3))
    sar_values = sar.astype(jnp.float32).reshape(local_bands, group_size, block_lines * extent)
    sar_sums = jnp.sum(sar_values, axis=2)
    sar_squares = jnp.sum(sar_values * sar_values, axis=2)
    map_device = own_blocks // group_size
    map_patch = (
        map_device // half_count * patch_dev + own_blocks % group_size * block_lines // quarter
    )
    member = (map_patch[:, None] == jnp.arange(patch_total, dtype=jnp.int32)[None, :]).astype(
        jnp.float32
    )
    sar_stats = jnp.dot(
        jnp.stack([sar_sums, sar_squares]).reshape(2 * local_bands, group_size),
        member,
        precision=precise,
        preferred_element_type=jnp.float32,
    )
    statistics = jnp.zeros((2, 2, band_total, patch_total), jnp.float32)
    opt_part = jnp.transpose(jnp.stack([opt_sums, opt_squares]), (0, 2, 1))
    statistics = lax.dynamic_update_slice(
        statistics, opt_part[None], (0, 0, band_at * local_bands, tile_at * patch_dev)
    )
    statistics = lax.dynamic_update_slice(
        statistics,
        sar_stats.reshape(2, local_bands, patch_total)[None],
        (1, 0, band_at * local_bands, 0),
    )
    totals = lax.psum(statistics, ("tile", "half", "band"))
    centered = totals[:, 1] - totals[:, 0] * totals[:, 0] / pixel_count
    energy = jnp.sum(centered, axis=1) / (band_total * pixel_count)
    norm_scale = lax.rsqrt(band_total * pixel_count * (energy[0] + EPSILON) * (energy[1] + EPSILON))
    first_patch = tile_at * patch_dev + band_at * kept_patches
    norm_mine = lax.dynamic_slice_in_dim(norm_scale, first_patch, kept_patches)
    slant_spectra = column_spectrum(sar, col_upper, col_lower).reshape(
        local_bands, group_size, block_lines, 2, half_count, col_width
    )
    outgoing = jnp.take(slant_spectra, send_order, axis=1).reshape(
        local_bands, tile_count, half_count, block_lines, 2, half_count, col_width
    )
    outgoing = jnp.transpose(outgoing, (0, 1, 5, 2, 3, 4, 6))
    arrived = relay_blocks(outgoing).reshape(
        local_bands, group_size * half_count, block_lines, 2, col_width
    )
    sources = lax.dynamic_slice_in_dim(
        inverse, tile_at * half_count * group_size, half_count * group_size
    )
    slot_index = (
        sources // group_size * half_count
        + jnp.arange(half_count * group_size, dtype=jnp.int32) // group_size
    )
    placed = jnp.take(arrived, slot_index, axis=1).reshape(
        local_bands, half_count, patch_dev, quarter, 2, col_width
    )
    placed = jnp.transpose(placed, (2, 0, 1, 3, 4, 5)).reshape(
        patch_dev, local_bands, extent, 2, col_width
    )
    sar_real, sar_imag = row_spectrum(placed, row_upper, row_lower)
    spectra = column_spectrum(optical, col_upper, col_lower).reshape(
        patch_dev, local_bands, quarter, 2, half_count, col_width
    )
    real_part, imag_part = row_spectrum(
        jnp.squeeze(
            lax.all_to_all(spectra, "half", split_axis=4, concat_axis=2, tiled=True), axis=4
        ),
        row_upper,
        row_lower,
    )
    opt_real = real_part
    opt_imag = imag_part
    rows_at = jnp.arange(extent, dtype=jnp.int32)[:, None]
    cols_at = half_at * col_width + jnp.arange(col_width, dtype=jnp.int32)[None, :]
    keep_mask = jnp.where((rows_at == 0) & (cols_at == 0), 0.0, 1.0).astype(jnp.float32)
    opt_real = opt_real * keep_mask
    opt_imag = opt_imag * keep_mask
    sar_real = sar_real * keep_mask
    sar_imag = sar_imag * keep_mask
    cross_real = jnp.sum(opt_real * sar_real + opt_imag * sar_imag, axis=1)
    cross_imag = jnp.sum(opt_real * sar_imag - opt_imag * sar_real, axis=1)
    cross_term = jnp.stack([cross_real, cross_imag], axis=1)
    cross_sum = lax.psum_scatter(cross_term, "band", scatter_dimension=0, tiled=True)
    lag_real = (
        jnp.einsum("uk,pkc->puc", cosine_table, cross_sum[:, 0], precision=precise)
        - jnp.einsum("uk,pkc->puc", sine_table, cross_sum[:, 1], precision=precise)
    ) / extent
    lag_imag = (
        jnp.einsum("uk,pkc->puc", cosine_table, cross_sum[:, 1], precision=precise)
        + jnp.einsum("uk,pkc->puc", sine_table, cross_sum[:, 0], precision=precise)
    ) / extent
    lagged = jnp.stack([lag_real, lag_imag], axis=2).reshape(
        kept_patches, half_count, quarter, 2, col_width
    )
    pieces = lax.all_to_all(lagged, "half", split_axis=1, concat_axis=4, tiled=True)
    real_in = pieces[:, 0, :, 0, :]
    imag_in = pieces[:, 0, :, 1, :]
    correlation = (
        jnp.einsum("puc,cv->puv", real_in, cosine_table, precision=precise)
        - jnp.einsum("puc,cv->puv", imag_in, sine_table, precision=precise)
    ) / extent
    surface = correlation * norm_mine[:, None, None]
    local_rows = peaks[:, 0, :] - half_at * quarter
    row_hit = (
        local_rows[:, :, None] == jnp.arange(quarter, dtype=jnp.int32)[None, None, :]
    ).astype(jnp.float32)
    picked = jnp.einsum("pkr,prc->pkc", row_hit, surface, precision=precise)
    col_hit = (peaks[:, 1, :, None] == jnp.arange(extent, dtype=jnp.int32)[None, None, :]).astype(
        jnp.float32
    )
    local_values = jnp.sum(picked * col_hit, axis=2)
    peak_values = lax.psum(local_values, "half")
    return (surface, peak_values)


def dft_tables(extent, parts):
    points = extent // 2
    cols = points // parts // 2
    places = np.arange(extent)
    phases = (places[:, None] * places[None, :]) % extent
    cosine = np.cos(phases * (2.0 * np.pi / extent))
    sine = np.sin(phases * (2.0 * np.pi / extent))
    forward, backward = [], [[], []]
    for part in range(parts):
        for turn in range(2):
            first = (2 * part + turn) * cols
            span = slice(first, first + cols)
            real, imag = cosine[:, span].copy(), -sine[:, span]
            real_back, imag_back = 2.0 * cosine[span], -2.0 * sine[span]
            if first == 0:
                imag[:, 0] = cosine[:, points]
                real_back[0] = 1.0
                imag_back[0] = cosine[points]
            forward += [real, imag]
            backward[turn] += [real_back, imag_back]
    col_table = np.concatenate(forward, axis=1)
    back_table = np.stack([np.concatenate(b, axis=0) for b in backward])
    row_sine, lag_sine = sine[:points, :points].copy(), 2.0 * sine[:points, :points]
    row_cosine, lag_cosine = cosine[:points, :points], 2.0 * cosine[:points, :points]
    row_sine[0] = cosine[points, :points]
    lag_cosine[:, 0] = 1.0
    lag_sine[:, 0] = cosine[:points, points]


    def woven(a, b):
        both = np.stack([a.reshape(-1, BLOCK, points), b.reshape(-1, BLOCK, points)], axis=1)
        return both.reshape(points, points)

    row_table = np.stack([woven(row_cosine[i::2], row_sine[i::2]) for i in range(2)])
    lag_table = np.stack([woven(lag_cosine.T[i::2], lag_sine.T[i::2]).T for i in range(2)])
    return tuple(t.astype(jnp.bfloat16) for t in (col_table, row_table, lag_table, back_table))


def kernel(
    sizes,
    dest_hbm,
    peaks_hbm,
    sar_hbm,
    opt_hbm,
    col_hbm,
    row_hbm,
    lag_hbm,
    back_hbm,
    surface_ref,
    peak_ref,
    dest_ref,
    peaks_ref,
    sar_v,
    opt_v,
    col_v,
    row_v,
    lag_v,
    back_v,
    send_0,
    send_1,
    arrived_0,
    arrived_1,
    opt_send,
    opt_in,
    opt_waves,
    sar_cols,
    cross,
    spot_rows,
    waves,
    picked,
    lag_send,
    lag_in,
    spot_send,
    spot_recv,
    last_mine,
    last_other,
    last_in,
    load_sem,
    sar_ssem,
    sar_rsem,
    opt_ssem,
    opt_rsem,
    lag_ssem,
    lag_rsem,
    last_ssem,
    last_rsem,
    spot_ssem,
    spot_rsem,
    near_sem,
    far_sem,
):
    tiles, halves, bands, patch_dev, quarter, extent, lines, peak_count = sizes
    group = tiles * halves
    parts = halves * bands
    wide = extent // parts
    side = wide // 2
    cols = wide // 4
    points = extent // 2
    per_patch = group // patch_dev
    block = BLOCK
    send, arrived = (send_0, send_1), (arrived_0, arrived_1)
    f32, bf = jnp.float32, jnp.bfloat16
    tile, half, band = lax.axis_index("tile"), lax.axis_index("half"), lax.axis_index("band")
    me = tile * halves + half
    part = half * bands + band
    other_half = 1 - half
    other_band = 1 - band

    def place(step, shift, swap):
        return (
            lax.rem(tile + step, tiles),
            lax.rem(half + shift, halves),
            lax.rem(band + swap, bands),
        )

    def device(step, shift, swap):
        return dict(zip(("tile", "half", "band"), place(step, shift, swap)))

    others = tiles * parts - 1
    near = [(0, shift, swap) for shift in (1, 0) for swap in range(bands) if shift or swap]

    loads = [
        pltpu.make_async_copy(a, b, load_sem.at[i])
        for i, (a, b) in enumerate(
            [(dest_hbm, dest_ref), (sar_hbm, sar_v), (col_hbm, col_v), (opt_hbm, opt_v),
             (row_hbm, row_v), (peaks_hbm, peaks_ref), (lag_hbm, lag_v), (back_hbm, back_v)]
        )
    ]
    for i in (3, 2, 0, 1):
        loads[i].start()

    barrier = pltpu.get_barrier_semaphore()
    first_band, last_band = jnp.int32(0), jnp.int32(bands - 1)

    def tell(semaphore, **where):
        pl.semaphore_signal(semaphore, inc=1, device_id=where, device_id_type=MESH)

    for shift in range(1, halves):
        tell(barrier, half=lax.rem(half + shift, halves), band=first_band)
    pl.when(band != first_band)(lambda: tell(barrier, band=first_band))
    for step in sorted(range(1, tiles), key=lambda s: -min(s, tiles - s)):
        for shift in range(halves):
            tell(
                barrier,
                tile=lax.rem(tile + step, tiles),
                half=lax.rem(half + shift, halves),
                band=last_band,
            )

    def remote(src, dst, ssem, rsem, peer):
        return pltpu.make_async_remote_copy(
            src_ref=src,
            dst_ref=dst,
            send_sem=ssem,
            recv_sem=rsem,
            device_id=device(*peer),
            device_id_type=MESH,
        )

    source_at = me * bands + band

    def sar_copy(turn, to_tile, to_half, to_band):
        return pltpu.make_async_remote_copy(
            src_ref=send[turn].at[to_tile * parts + to_half * bands + to_band],
            dst_ref=arrived[turn].at[source_at],
            send_sem=sar_ssem.at[turn],
            recv_sem=sar_rsem.at[turn],
            device_id={"tile": to_tile, "half": to_half, "band": to_band},
            device_id_type=MESH,
        )

    low = lax.broadcasted_iota(jnp.int32, (1, wide), 1) < side

    def pair(a, b):
        first = jnp.concatenate([a[:, :side], b[:, :side]], axis=1)
        second = jnp.concatenate([a[:, side:], b[:, side:]], axis=1)
        return first, second

    def whole(ref, count, ssem, rsem):
        ref = ref.at[pl.ds(0, count)]
        return remote(ref, ref, ssem, rsem, (0, 1, 0))

    loads[0].wait()
    own_runs = [lax.div(dest_ref[me * group + j], group) for j in range(group)]

    def block_for(run):
        found = jnp.int32(0)
        for j in range(group):
            found = jnp.where(own_runs[j] == run, j, found)
        return found

    def sar_columns(to_tile):
        if to_tile == 0:
            loads[1].wait()
        samples = jnp.concatenate(
            [
                sar_v[block_for(to_tile * halves + lax.rem(run + band, halves))]
                for run in range(halves)
            ],
            axis=0,
        )
        spectra = jnp.dot(samples, col_v[...], preferred_element_type=f32).astype(bf)
        for to in range(parts):
            at = slice(to * wide, (to + 1) * wide)
            first, second = pair(spectra[:lines, at], spectra[lines:, at])
            send_0[to_tile * parts + to] = first
            send_1[to_tile * parts + to] = second

    def sar_sends(turn, to_tile, shifts):
        for shift in shifts:
            to_half = lax.rem(half + shift, halves)
            for swap in range(bands):
                to_band = lax.rem(band + swap, bands)
                copy = sar_copy(turn, to_tile, to_half, to_band)
                if shift or swap:
                    copy.start()
                else:
                    pl.when(tile != to_tile)(copy.start)

    def opt_copy(turn, peer):
        _, to_half, to_band = place(*peer)
        return remote(
            opt_send.at[turn, to_half * bands + to_band],
            opt_in.at[turn, part],
            opt_ssem.at[turn],
            opt_rsem.at[turn],
            peer,
        )

    def opt_sends(turn):
        for peer in near:
            opt_copy(turn, peer).start()

    loads[3].wait()
    loads[2].wait()
    opt_spectra = [
        jnp.dot(opt_v[lax.rem(patch + band, patch_dev)], col_v[...], preferred_element_type=f32).astype(bf)
        for patch in range(patch_dev)
    ]
    for to in range(parts):
        at = slice(to * wide, (to + 1) * wide)
        first, second = pair(*[s[:, at] for s in opt_spectra])
        opt_send[0, to] = first
        opt_send[1, to] = second
    @pl.when(band == first_band)
    def _():
        pl.semaphore_wait(barrier, parts - 1)
        tell(near_sem, band=last_band)

    @pl.when(band == last_band)
    def _():
        pl.semaphore_wait(near_sem, 1)

    opt_sends(0)
    opt_sends(1)
    sar_columns(0)
    for i in (4, 5, 6, 7):
        loads[i].start()

    @pl.when(band == last_band)
    def _():
        pl.semaphore_wait(barrier, (tiles - 1) * parts)
        tell(far_sem, band=first_band)

    @pl.when(band == first_band)
    def _():
        pl.semaphore_wait(far_sem, 1)

    sar_sends(0, 0, (1, 0))
    for to_tile in range(1, tiles):
        sar_columns(to_tile)
        if to_tile > 1:
            sar_sends(0, to_tile, (1, 0))
        else:
            sar_sends(1, 0, (1, 0))
            sar_sends(0, 1, (1, 0))
    for to_tile in range(1, tiles):
        sar_sends(1, to_tile, (1, 0))
    arrived_0[source_at] = send_0[tile * parts + part]
    arrived_1[source_at] = send_1[tile * parts + part]
    for turn in range(2):
        opt_in[turn, part] = opt_send[turn, part]

    slot_of = []
    for run in range(halves):
        places = []
        for source in range(group):
            found = jnp.int32(0)
            for j in range(group):
                spot = dest_ref[source * group + j]
                found = jnp.where(
                    lax.div(spot, group) == tile * halves + run, lax.rem(spot, group), found
                )
            places.append(found)
        for slot in range(group):
            found = jnp.int32(0)
            for source in range(group):
                found = jnp.where(places[source] == slot, source, found)
            slot_of.append(found)

    spots = lax.broadcasted_iota(jnp.int32, (peak_count, extent), 1)
    ranks = lax.broadcasted_iota(jnp.int32, (peak_count, extent), 0)
    loads[5].wait()
    for which in range(2):
        wanted = jnp.zeros((peak_count, extent), jnp.int32)
        for j in range(peak_count):
            wanted = jnp.where(ranks == j, peaks_ref[0, which, j], wanted)
        spot_send[which * peak_count : (which + 1) * peak_count, :] = jnp.where(
            spots == wanted, 1.0, 0.0
        ).astype(bf)
    spot_copy = remote(spot_send, spot_recv, spot_ssem, spot_rsem, (0, 0, 1))
    spot_copy.start()

    lane = lax.broadcasted_iota(jnp.int32, (1, wide), 1)
    inner = lax.rem(lane, side)
    real_lane = inner < cols
    top = lax.broadcasted_iota(jnp.int32, (block, wide), 0) == 0
    edge_real = [((inner + part + turn) == 0) for turn in range(2)]
    edge_imag = [((jnp.abs(inner - cols) + part + turn) == 0) for turn in range(2)]
    weights = [
        jnp.where(edge_real[turn] | edge_imag[turn], 1.0, 2.0) * (0.5 * extent)
        for turn in range(2)
    ]

    def swapped(z):
        return pltpu.roll(z, side, 1)

    def crossed(z):
        return jnp.where(real_lane, pltpu.roll(z, wide - cols, 1), pltpu.roll(z, cols, 1))

    def turned(z):
        return jnp.where(real_lane, -pltpu.roll(z, wide - cols, 1), pltpu.roll(z, cols, 1))

    opt_energy = [0.0] * patch_dev

    def energy_of(even, odd, head, turn):
        shifted = even.astype(f32) - jnp.where(edge_real[turn], head * (2.0 / extent), 0.0)
        odd = odd.astype(f32)
        total = jnp.sum(shifted * shifted + odd * odd, axis=0, keepdims=True)
        return total * weights[turn]

    def optical(turn):
        whole(opt_in.at[turn], parts - 1, opt_ssem.at[turn], opt_rsem.at[turn]).wait_recv()
        real, imag = edge_real[turn], edge_imag[turn]
        pieces = [[opt_in[turn, run * bands + b] for b in range(bands)] for run in range(halves)]
        mixed = []
        for patch in range(patch_dev):
            near_x, far_x = [jnp.where(low, p[patch], p[1 - patch]) for p in pieces]
            mixed.append((near_x + far_x, near_x - far_x))
        for parity in range(2):
            plain = [jnp.where(imag, 0.0, m[parity]).astype(bf) for m in mixed]
            crossed_x = [
                jnp.where(real, 0.0, jnp.where(imag, m[parity], turned(m[parity]))).astype(bf)
                for m in mixed
            ]
            rows = jnp.dot(
                row_v[parity], jnp.concatenate(plain + crossed_x, axis=1), preferred_element_type=f32
            )
            for kind in range(2):
                for patch in range(patch_dev):
                    at = (kind * patch_dev + patch) * wide
                    opt_waves[turn, kind, patch, parity] = rows[:, at : at + wide]
        for patch in range(patch_dev):
            head = opt_waves[turn, 0, patch, 0, :block]
            opt_energy[patch] = opt_energy[patch] + energy_of(*mixed[patch], head[0:1], turn)
            opt_waves[turn, 0, patch, 0, :block] = jnp.where(real & top, 0.0, head)

    def fold(a, b, c, d):
        def halve(u, v):
            return jnp.where(low, u, v) + swapped(jnp.where(low, v, u))

        u, v = halve(a, c), halve(b, d)
        return (jnp.where(real_lane, u, v) + crossed(jnp.where(real_lane, v, u))).astype(bf)

    sar_energy = [0.0] * patch_dev

    def slant(turn):
        whole(arrived[turn], others, sar_ssem.at[turn], sar_rsem.at[turn]).wait_recv()
        for slot in range(group):
            patch, at = slot // per_patch, slot % per_patch * lines
            ends = []
            for run in range(halves):
                source = slot_of[run * group + slot] * bands
                piece = jnp.where(
                    low, arrived[turn][source + run], arrived[turn][source + 1 - run]
                )
                if patch != run:
                    piece = jnp.concatenate([piece[:, side:], piece[:, :side]], axis=1)
                ends.append(piece)
            sar_cols[turn, 0, patch, at : at + lines, :] = ends[0] + ends[1]
            sar_cols[turn, 1, patch, at : at + lines, :] = ends[0] - ends[1]
        for parity in range(2):
            both = [sar_cols[turn, parity, patch] for patch in range(patch_dev)]
            rows = jnp.dot(
                row_v[parity], jnp.concatenate(both, axis=1), preferred_element_type=f32
            )
            if parity == 0:
                for patch in range(patch_dev):
                    energy = energy_of(
                        sar_cols[turn, 0, patch],
                        sar_cols[turn, 1, patch],
                        rows[0:1, patch * wide : (patch + 1) * wide],
                        turn,
                    )
                    sar_energy[patch] = sar_energy[patch] + energy
            for b in range(points // 2 // block):
                at = slice(2 * b * block, (2 * b + 1) * block)
                lower = slice((2 * b + 1) * block, (2 * b + 2) * block)
                sums = []
                for patch in range(patch_dev):
                    yc, ys = [rows[i, patch * wide : (patch + 1) * wide] for i in (at, lower)]
                    zc, zs = [opt_waves[turn, 0, patch, parity, i] for i in (at, lower)]
                    tc, ts = [opt_waves[turn, 1, patch, parity, i] for i in (at, lower)]
                    zs_e, ts_e, zc_d, tc_d = zs, ts, zc, tc
                    if b == 0 and parity == 0:
                        zs_e, ts_e = jnp.where(top, 0.0, zs), jnp.where(top, 0.0, ts)
                        zc_d, tc_d = jnp.where(top, zs, zc), jnp.where(top, ts, tc)
                    sums.append(
                        (
                            zc * yc + zs_e * ys,
                            tc * yc + ts_e * ys,
                            zc_d * ys - zs_e * yc,
                            tc_d * ys - ts_e * yc,
                        )
                    )
                one, two = sums
                cross[turn, parity, at, :] = fold(one[0], one[1], two[0], two[1])
                cross[turn, parity, lower, :] = fold(one[2], one[3], two[2], two[3])

    def lag_copy(turn, peer):
        _, to_half, to_band = place(*peer)
        return remote(
            lag_send.at[turn, to_half * bands + to_band],
            lag_in.at[turn, part],
            lag_ssem.at[turn],
            lag_rsem.at[turn, peer[1]],
            peer,
        )

    def lag_sends(turn, shift):
        for swap in range(bands):
            if shift or swap:
                lag_copy(turn, (0, shift, swap)).start()

    def send_last():
        found = picked[0] * waves[0] + picked[1] * waves[1]
        for which, patch, ref in ((0, band, last_mine), (1, other_band, last_other)):
            mine = lax.div(lane, side) == patch
            ref[0:8, :] = jnp.zeros((8, wide), f32)
            ref[0:1, :] = jnp.where(patch == 0, opt_energy[0], opt_energy[1])
            ref[1:2, :] = jnp.where(patch == 0, sar_energy[0], sar_energy[1])
            value = jnp.where(mine, found[which * peak_count : (which + 1) * peak_count], 0.0)
            ref[8 : 8 + peak_count, :] = jnp.broadcast_to(
                jnp.sum(value, axis=1, keepdims=True), (peak_count, wide)
            )
        for peer in near:
            remote(
                last_other if peer[2] else last_mine, last_in.at[part], last_ssem, last_rsem, peer
            ).start()
        last_in[part] = last_mine[...]

    def spread(turn):
        even, odd = [
            jnp.dot(
                jnp.concatenate([spot_rows[parity], lag_v[parity]], axis=0),
                cross[turn, parity],
                preferred_element_type=f32,
            )
            for parity in range(2)
        ]
        picked[turn] = even[: 2 * peak_count] + odd[: 2 * peak_count]
        even, odd = even[2 * peak_count :], odd[2 * peak_count :]
        if turn:
            send_last()
        flip = jnp.where(half == 0, -1.0, 1.0)
        for shift, to_half in ((1, other_half), (0, half)):
            values = (even + odd * flip if shift else even - odd * flip).astype(bf)
            for patch, piece in enumerate(pair(values[: quarter // 2], values[quarter // 2 :])):
                lag_send[turn, to_half * bands + patch] = piece
            lag_sends(turn, shift)
        lag_in[turn, part] = lag_send[turn, part]

    def gather(turn, shift, first=False, last=False):
        from_half = lax.rem(half + shift, halves)
        if last:
            whole(last_in, parts - 1, last_ssem, last_rsem).wait_recv()
            scale = norm()
        count = bands if shift else bands - 1
        whole(lag_in.at[turn], count, lag_ssem.at[turn], lag_rsem.at[turn, shift]).wait_recv()
        upper, lower = pair(*[lag_in[turn, from_half * bands + b] for b in range(bands)])
        table = back_v[turn, pl.ds(pl.multiple_of(from_half * wide, wide), wide), :]
        values = jnp.dot(
            jnp.concatenate([upper, lower], axis=0), table, preferred_element_type=f32
        )
        if first:
            surface_ref[0] = values
        elif last:
            surface_ref[0] = (surface_ref[0] + values) * scale
        else:
            surface_ref[0] = surface_ref[0] + values

    pixels = extent * extent

    def norm():
        total = last_in[0]
        for i in range(1, parts):
            total = total + last_in[i]
        energies = jnp.sum(total[0:8], axis=1, keepdims=True) / (float(pixels) * bands * pixels)
        energies = energies + EPSILON
        scale = lax.rsqrt(bands * pixels * energies[0:1] * energies[1:2]) / pixels
        at = lax.broadcasted_iota(jnp.int32, (peak_count, wide), 1)
        rank = lax.broadcasted_iota(jnp.int32, (peak_count, wide), 0)
        row = jnp.where(at == rank, total[8 : 8 + peak_count], 0.0)
        peak_ref[...] = (jnp.sum(row, axis=0, keepdims=True) * scale)[:, :peak_count]
        return scale

    loads[4].wait()
    loads[6].wait()
    loads[7].wait()
    spot_copy.wait_recv()
    spots_all = jnp.concatenate([spot_send[:peak_count], spot_recv[:peak_count]], axis=0)
    lags_all = jnp.concatenate([spot_send[peak_count:], spot_recv[peak_count:]], axis=0)
    upper_spots, lower_spots = spots_all[:, :points], spots_all[:, points:]
    for parity in range(2):
        spots_now = upper_spots + lower_spots if parity == 0 else upper_spots - lower_spots
        spot_rows[parity] = jnp.dot(
            spots_now, lag_v[parity], preferred_element_type=f32
        ).astype(bf)
    for turn in range(2):
        rows_back = back_v[turn, pl.ds(pl.multiple_of(part * side, side), side), :]
        waves[turn] = lax.dot_general(
            lags_all,
            jnp.concatenate([rows_back, rows_back], axis=0),
            (((1,), (1,)), ((), ())),
            preferred_element_type=f32,
        )
    optical(0)
    optical(1)
    slant(0)
    spread(0)
    slant(1)
    spread(1)

    gather(0, 0, first=True)
    gather(1, 0)
    gather(0, 1)
    gather(1, 1, last=True)
    for turn in range(2):
        whole(send[turn], others, sar_ssem.at[turn], sar_rsem.at[turn]).wait_send()
        whole(opt_in.at[turn], parts - 1, opt_ssem.at[turn], opt_rsem.at[turn]).wait_send()
        whole(lag_in.at[turn], parts - 1, lag_ssem.at[turn], lag_rsem.at[turn, 0]).wait_send()
    whole(last_in, parts - 1, last_ssem, last_rsem).wait_send()
    spot_copy.wait_send()


def finish(surface_ref, peak_in, out_ref, peak_ref, sem):
    copies = [
        pltpu.make_async_copy(a, b, sem.at[i])
        for i, (a, b) in enumerate([(surface_ref, out_ref), (peak_in, peak_ref)])
    ]
    for copy in copies:
        copy.start()
    for copy in copies:
        copy.wait()


def fused(mesh, optical, sar, destination, peaks):
    tiles, halves, bands = mesh.shape["tile"], mesh.shape["half"], mesh.shape["band"]
    patch_dev, _, quarter, extent = optical.shape
    group = tiles * halves
    parts = halves * bands
    lines = sar.shape[1] // group
    peak_count = peaks.shape[2]
    wide = extent // parts
    points = extent // 2
    sizes = (tiles, halves, bands, patch_dev, quarter, extent, lines, peak_count)
    tables = dft_tables(extent, parts)
    bf, f32 = jnp.bfloat16, jnp.float32
    vmem = pltpu.VMEM
    dma = pltpu.SemaphoreType.DMA
    raw, values = pl.pallas_call(
        functools.partial(kernel, sizes),
        out_shape=(
            jax.ShapeDtypeStruct((1, quarter, extent), f32),
            jax.ShapeDtypeStruct((1, peak_count), f32),
        ),
        in_specs=[pl.BlockSpec(memory_space=pltpu.HBM)] * 8,
        out_specs=(pl.BlockSpec(memory_space=pltpu.VMEM), pl.BlockSpec(memory_space=pltpu.VMEM)),
        scratch_shapes=[
            pltpu.SMEM(destination.shape, jnp.int32),
            pltpu.SMEM(peaks.shape, jnp.int32),
            vmem((group, lines, extent), bf),
            vmem((patch_dev, quarter, extent), bf),
            vmem((extent, extent), bf),
            vmem((2, points, points), bf),
            vmem((2, points, points), bf),
            vmem((2, points, extent), bf),
            vmem((tiles * parts, lines, wide), bf),
            vmem((tiles * parts, lines, wide), bf),
            vmem((group * bands, lines, wide), bf),
            vmem((group * bands, lines, wide), bf),
            vmem((2, parts, quarter, wide), bf),
            vmem((2, parts, quarter, wide), bf),
            vmem((2, 2, patch_dev, 2, points, wide), f32),
            vmem((2, 2, patch_dev, points, wide), bf),
            vmem((2, 2, points, wide), bf),
            vmem((2, 2 * peak_count, points), bf),
            vmem((2, 2 * peak_count, wide), f32),
            vmem((2, 2 * peak_count, wide), f32),
            vmem((2, parts, quarter // 2, wide), bf),
            vmem((2, parts, quarter // 2, wide), bf),
            vmem((2 * peak_count, extent), bf),
            vmem((2 * peak_count, extent), bf),
            vmem((8 + peak_count, wide), f32),
            vmem((8 + peak_count, wide), f32),
            vmem((parts, 8 + peak_count, wide), f32),
            dma((8,)),
            dma((2,)),
            dma((2,)),
            dma((2,)),
            dma((2,)),
            dma((2,)),
            dma((2, 2)),
            dma,
            dma,
            dma,
            dma,
            pltpu.SemaphoreType.REGULAR,
            pltpu.SemaphoreType.REGULAR,
        ],
        compiler_params=pltpu.CompilerParams(
            collective_id=0, has_side_effects=True, vmem_limit_bytes=50 * 1024 * 1024
        ),
    )(
        *[
            pltpu.with_memory_space_constraint(x, pltpu.HBM)
            for x in (
                destination,
                peaks,
                sar.reshape(group, lines, extent),
                optical.reshape(patch_dev, quarter, extent),
                *[jnp.asarray(t) for t in tables],
            )
        ]
    )
    return pl.pallas_call(
        finish,
        out_shape=(
            jax.ShapeDtypeStruct((1, quarter, extent), f32),
            jax.ShapeDtypeStruct((1, peak_count), f32),
        ),
        in_specs=[pl.BlockSpec(memory_space=pltpu.VMEM)] * 2,
        out_specs=(pl.BlockSpec(memory_space=pltpu.HBM), pl.BlockSpec(memory_space=pltpu.HBM)),
        scratch_shapes=[dma((2,))],
    )(*[pltpu.with_memory_space_constraint(x, pltpu.VMEM) for x in (raw, values)])


def fits(mesh, optical, sar, peaks):
    group = mesh.shape["tile"] * mesh.shape["half"]
    patch_dev, local_bands, quarter, extent = optical.shape
    lines = sar.shape[1] // group
    return (
        mesh.shape["half"] == 2
        and mesh.shape["band"] == 2
        and patch_dev == 2
        and local_bands == 1
        and lines % 16 == 0
        and mesh.shape["tile"] > 1
        and quarter * 2 == extent
        and group * lines == patch_dev * quarter
        and extent % 512 == 0
        and peaks.shape[0] == 1
        and peaks.shape[2] % 8 == 0
    )


def solution(mesh):
    def local(optical, sar, destination, peaks):
        if fits(mesh, optical, sar, peaks):
            return fused(mesh, optical, sar, destination, peaks)
        return generic(optical, sar, destination, peaks)

    in_specs = (
        P(("scene", "tile"), "band", "half", None),
        P("band", ("scene", "tile", "half"), None),
        P("scene"),
        P(("scene", "tile", "band"), None, None),
    )
    out_specs = (P(("scene", "tile", "band"), "half", None), P(("scene", "tile", "band"), None))
    return jax.shard_map(local, mesh=mesh, in_specs=in_specs, out_specs=out_specs, check_vma=False)
```

```python
import functools
import math

import jax
import jax.numpy as jnp
import numpy as np
from jax import lax
from jax.experimental import pallas as pl
from jax.experimental.pallas import tpu as pltpu
from jax.sharding import PartitionSpec as P

MESH = pl.DeviceIdType.MESH

precise = lax.Precision.HIGHEST
EPSILON = 1e-06
BLOCK = 16


def fourier_tables(extent):
    places = jnp.arange(extent, dtype=jnp.int32)
    phases = places[:, None] * places[None, :] % extent
    angles = phases.astype(jnp.float32) * (2.0 * math.pi / extent)
    return (jnp.cos(angles), jnp.sin(angles))


def fourier_pair(table):
    upper = table.astype(jnp.bfloat16)
    lower = (table - upper.astype(jnp.float32)).astype(jnp.bfloat16)
    return (upper, lower)


def column_spectrum(samples, table_upper, table_lower):
    extent = samples.shape[-1]
    values = samples.reshape(-1, extent)
    spectrum = jnp.dot(values, table_upper, preferred_element_type=jnp.float32) + jnp.dot(
        values, table_lower, preferred_element_type=jnp.float32
    )
    return spectrum.astype(jnp.bfloat16).reshape(samples.shape[:-1] + (2 * extent,))


def row_spectrum(columns, table_upper, table_lower):
    line_count = columns.shape[-3]
    stacked = jnp.concatenate([columns[..., 0, :], columns[..., 1, :]], axis=-2)
    result = jnp.einsum("kr,...rc->...kc", table_upper, stacked, preferred_element_type=jnp.float32)
    result = result + jnp.einsum(
        "kr,...rc->...kc", table_lower, stacked, preferred_element_type=jnp.float32
    )
    return (result[..., :line_count, :], result[..., line_count:, :])


def relay_blocks(parcel):
    layout = parcel.shape
    merged = parcel.reshape(layout[:1] + (layout[1] * layout[2],) + layout[3:])
    arrived = lax.all_to_all(merged, ("tile", "half"), split_axis=1, concat_axis=1, tiled=True)
    return arrived.reshape(layout)


def generic(optical, sar, destination, peaks):
    tile_count = lax.axis_size("tile")
    half_count = lax.axis_size("half")
    band_count = lax.axis_size("band")
    group_size = tile_count * half_count
    patch_dev, local_bands, quarter, extent = optical.shape
    col_width = extent // half_count
    block_lines = sar.shape[1] // group_size
    band_total = local_bands * band_count
    pixel_count = extent * extent
    patch_total = patch_dev * tile_count
    kept_patches = patch_dev // band_count
    cosine_table, sine_table = fourier_tables(extent)
    col_upper, col_lower = fourier_pair(jnp.concatenate([cosine_table, -sine_table], axis=1))
    row_full = jnp.concatenate(
        [
            jnp.concatenate([cosine_table, sine_table], axis=1),
            jnp.concatenate([-sine_table, cosine_table], axis=1),
        ],
        axis=0,
    )
    row_upper, row_lower = fourier_pair(row_full)
    tile_at = lax.axis_index("tile")
    half_at = lax.axis_index("half")
    band_at = lax.axis_index("band")
    device_at = lax.axis_index(("tile", "half"))
    own_blocks = lax.dynamic_slice_in_dim(destination, device_at * group_size, group_size)
    send_order = jnp.argsort(own_blocks // group_size)
    inverse = (
        jnp.zeros_like(destination)
        .at[destination]
        .set(jnp.arange(destination.shape[0], dtype=jnp.int32))
    )
    opt_values = optical.astype(jnp.float32)
    opt_sums = jnp.sum(opt_values, axis=(2, 3))
    opt_squares = jnp.sum(opt_values * opt_values, axis=(2, 3))
    sar_values = sar.astype(jnp.float32).reshape(local_bands, group_size, block_lines * extent)
    sar_sums = jnp.sum(sar_values, axis=2)
    sar_squares = jnp.sum(sar_values * sar_values, axis=2)
    map_device = own_blocks // group_size
    map_patch = (
        map_device // half_count * patch_dev + own_blocks % group_size * block_lines // quarter
    )
    member = (map_patch[:, None] == jnp.arange(patch_total, dtype=jnp.int32)[None, :]).astype(
        jnp.float32
    )
    sar_stats = jnp.dot(
        jnp.stack([sar_sums, sar_squares]).reshape(2 * local_bands, group_size),
        member,
        precision=precise,
        preferred_element_type=jnp.float32,
    )
    statistics = jnp.zeros((2, 2, band_total, patch_total), jnp.float32)
    opt_part = jnp.transpose(jnp.stack([opt_sums, opt_squares]), (0, 2, 1))
    statistics = lax.dynamic_update_slice(
        statistics, opt_part[None], (0, 0, band_at * local_bands, tile_at * patch_dev)
    )
    statistics = lax.dynamic_update_slice(
        statistics,
        sar_stats.reshape(2, local_bands, patch_total)[None],
        (1, 0, band_at * local_bands, 0),
    )
    totals = lax.psum(statistics, ("tile", "half", "band"))
    centered = totals[:, 1] - totals[:, 0] * totals[:, 0] / pixel_count
    energy = jnp.sum(centered, axis=1) / (band_total * pixel_count)
    norm_scale = lax.rsqrt(band_total * pixel_count * (energy[0] + EPSILON) * (energy[1] + EPSILON))
    first_patch = tile_at * patch_dev + band_at * kept_patches
    norm_mine = lax.dynamic_slice_in_dim(norm_scale, first_patch, kept_patches)
    slant_spectra = column_spectrum(sar, col_upper, col_lower).reshape(
        local_bands, group_size, block_lines, 2, half_count, col_width
    )
    outgoing = jnp.take(slant_spectra, send_order, axis=1).reshape(
        local_bands, tile_count, half_count, block_lines, 2, half_count, col_width
    )
    outgoing = jnp.transpose(outgoing, (0, 1, 5, 2, 3, 4, 6))
    arrived = relay_blocks(outgoing).reshape(
        local_bands, group_size * half_count, block_lines, 2, col_width
    )
    sources = lax.dynamic_slice_in_dim(
        inverse, tile_at * half_count * group_size, half_count * group_size
    )
    slot_index = (
        sources // group_size * half_count
        + jnp.arange(half_count * group_size, dtype=jnp.int32) // group_size
    )
    placed = jnp.take(arrived, slot_index, axis=1).reshape(
        local_bands, half_count, patch_dev, quarter, 2, col_width
    )
    placed = jnp.transpose(placed, (2, 0, 1, 3, 4, 5)).reshape(
        patch_dev, local_bands, extent, 2, col_width
    )
    sar_real, sar_imag = row_spectrum(placed, row_upper, row_lower)
    spectra = column_spectrum(optical, col_upper, col_lower).reshape(
        patch_dev, local_bands, quarter, 2, half_count, col_width
    )
    real_part, imag_part = row_spectrum(
        jnp.squeeze(
            lax.all_to_all(spectra, "half", split_axis=4, concat_axis=2, tiled=True), axis=4
        ),
        row_upper,
        row_lower,
    )
    opt_real = real_part
    opt_imag = imag_part
    rows_at = jnp.arange(extent, dtype=jnp.int32)[:, None]
    cols_at = half_at * col_width + jnp.arange(col_width, dtype=jnp.int32)[None, :]
    keep_mask = jnp.where((rows_at == 0) & (cols_at == 0), 0.0, 1.0).astype(jnp.float32)
    opt_real = opt_real * keep_mask
    opt_imag = opt_imag * keep_mask
    sar_real = sar_real * keep_mask
    sar_imag = sar_imag * keep_mask
    cross_real = jnp.sum(opt_real * sar_real + opt_imag * sar_imag, axis=1)
    cross_imag = jnp.sum(opt_real * sar_imag - opt_imag * sar_real, axis=1)
    cross_term = jnp.stack([cross_real, cross_imag], axis=1)
    cross_sum = lax.psum_scatter(cross_term, "band", scatter_dimension=0, tiled=True)
    lag_real = (
        jnp.einsum("uk,pkc->puc", cosine_table, cross_sum[:, 0], precision=precise)
        - jnp.einsum("uk,pkc->puc", sine_table, cross_sum[:, 1], precision=precise)
    ) / extent
    lag_imag = (
        jnp.einsum("uk,pkc->puc", cosine_table, cross_sum[:, 1], precision=precise)
        + jnp.einsum("uk,pkc->puc", sine_table, cross_sum[:, 0], precision=precise)
    ) / extent
    lagged = jnp.stack([lag_real, lag_imag], axis=2).reshape(
        kept_patches, half_count, quarter, 2, col_width
    )
    pieces = lax.all_to_all(lagged, "half", split_axis=1, concat_axis=4, tiled=True)
    real_in = pieces[:, 0, :, 0, :]
    imag_in = pieces[:, 0, :, 1, :]
    correlation = (
        jnp.einsum("puc,cv->puv", real_in, cosine_table, precision=precise)
        - jnp.einsum("puc,cv->puv", imag_in, sine_table, precision=precise)
    ) / extent
    surface = correlation * norm_mine[:, None, None]
    local_rows = peaks[:, 0, :] - half_at * quarter
    row_hit = (
        local_rows[:, :, None] == jnp.arange(quarter, dtype=jnp.int32)[None, None, :]
    ).astype(jnp.float32)
    picked = jnp.einsum("pkr,prc->pkc", row_hit, surface, precision=precise)
    col_hit = (peaks[:, 1, :, None] == jnp.arange(extent, dtype=jnp.int32)[None, None, :]).astype(
        jnp.float32
    )
    local_values = jnp.sum(picked * col_hit, axis=2)
    peak_values = lax.psum(local_values, "half")
    return (surface, peak_values)


def dft_tables(extent, parts):
    points = extent // 2
    cols = points // parts // 2
    places = np.arange(extent)
    phases = (places[:, None] * places[None, :]) % extent
    cosine = np.cos(phases * (2.0 * np.pi / extent))
    sine = np.sin(phases * (2.0 * np.pi / extent))
    forward, backward = [], [[], []]
    for part in range(parts):
        for turn in range(2):
            first = (2 * part + turn) * cols
            span = slice(first, first + cols)
            real, imag = cosine[:, span].copy(), -sine[:, span]
            real_back, imag_back = 2.0 * cosine[span], -2.0 * sine[span]
            if first == 0:
                imag[:, 0] = cosine[:, points]
                real_back[0] = 1.0
                imag_back[0] = cosine[points]
            forward += [real, imag]
            backward[turn] += [real_back, imag_back]
    col_table = np.concatenate(forward, axis=1)
    back_table = np.stack([np.concatenate(b, axis=0) for b in backward])
    row_sine, lag_sine = sine[:points, :points].copy(), 2.0 * sine[:points, :points]
    row_cosine, lag_cosine = cosine[:points, :points], 2.0 * cosine[:points, :points]
    row_sine[0] = cosine[points, :points]
    lag_cosine[:, 0] = 1.0
    lag_sine[:, 0] = cosine[:points, points]


    def woven(a, b):
        both = np.stack([a.reshape(-1, BLOCK, points), b.reshape(-1, BLOCK, points)], axis=1)
        return both.reshape(points, points)

    row_table = np.stack([woven(row_cosine[i::2], row_sine[i::2]) for i in range(2)])
    lag_table = np.stack([woven(lag_cosine.T[i::2], lag_sine.T[i::2]).T for i in range(2)])
    return tuple(t.astype(jnp.bfloat16) for t in (col_table, row_table, lag_table, back_table))


def kernel(
    sizes,
    dest_hbm,
    peaks_hbm,
    sar_hbm,
    opt_hbm,
    col_hbm,
    row_hbm,
    lag_hbm,
    back_hbm,
    surface_ref,
    peak_ref,
    dest_ref,
    peaks_ref,
    sar_v,
    opt_v,
    col_v,
    row_v,
    lag_v,
    back_v,
    send_0,
    send_1,
    arrived_0,
    arrived_1,
    opt_send,
    opt_in,
    opt_waves,
    sar_cols,
    cross,
    spot_rows,
    waves,
    picked,
    lag_send,
    lag_in,
    spot_send,
    spot_recv,
    last_mine,
    last_other,
    last_in,
    load_sem,
    sar_ssem,
    sar_rsem,
    opt_ssem,
    opt_rsem,
    lag_ssem,
    lag_rsem,
    last_ssem,
    last_rsem,
    spot_ssem,
    spot_rsem,
    near_sem,
    far_sem,
):
    tiles, halves, bands, patch_dev, quarter, extent, lines, peak_count = sizes
    group = tiles * halves
    parts = halves * bands
    wide = extent // parts
    side = wide // 2
    cols = wide // 4
    points = extent // 2
    per_patch = group // patch_dev
    block = BLOCK
    send, arrived = (send_0, send_1), (arrived_0, arrived_1)
    f32, bf = jnp.float32, jnp.bfloat16
    tile, half, band = lax.axis_index("tile"), lax.axis_index("half"), lax.axis_index("band")
    me = tile * halves + half
    part = half * bands + band
    other_half = 1 - half
    other_band = 1 - band

    def place(step, shift, swap):
        return (
            lax.rem(tile + step, tiles),
            lax.rem(half + shift, halves),
            lax.rem(band + swap, bands),
        )

    def device(step, shift, swap):
        return dict(zip(("tile", "half", "band"), place(step, shift, swap)))

    others = tiles * parts - 1
    near = [(0, shift, swap) for shift in (1, 0) for swap in range(bands) if shift or swap]

    loads = [
        pltpu.make_async_copy(a, b, load_sem.at[i])
        for i, (a, b) in enumerate(
            [(dest_hbm, dest_ref), (sar_hbm, sar_v), (col_hbm, col_v), (opt_hbm, opt_v),
             (row_hbm, row_v), (peaks_hbm, peaks_ref), (lag_hbm, lag_v), (back_hbm, back_v)]
        )
    ]
    for i in (3, 2, 0, 1):
        loads[i].start()

    barrier = pltpu.get_barrier_semaphore()
    first_band, last_band = jnp.int32(0), jnp.int32(bands - 1)

    def tell(semaphore, **where):
        pl.semaphore_signal(semaphore, inc=1, device_id=where, device_id_type=MESH)

    for shift in range(1, halves):
        tell(barrier, half=lax.rem(half + shift, halves), band=first_band)
    pl.when(band != first_band)(lambda: tell(barrier, band=first_band))
    for step in sorted(range(1, tiles), key=lambda s: -min(s, tiles - s)):
        for shift in range(halves):
            tell(
                barrier,
                tile=lax.rem(tile + step, tiles),
                half=lax.rem(half + shift, halves),
                band=last_band,
            )

    def remote(src, dst, ssem, rsem, peer):
        return pltpu.make_async_remote_copy(
            src_ref=src,
            dst_ref=dst,
            send_sem=ssem,
            recv_sem=rsem,
            device_id=device(*peer),
            device_id_type=MESH,
        )

    source_at = me * bands + band

    def sar_copy(turn, to_tile, to_half, to_band):
        return pltpu.make_async_remote_copy(
            src_ref=send[turn].at[to_tile * parts + to_half * bands + to_band],
            dst_ref=arrived[turn].at[source_at],
            send_sem=sar_ssem.at[turn],
            recv_sem=sar_rsem.at[turn],
            device_id={"tile": to_tile, "half": to_half, "band": to_band},
            device_id_type=MESH,
        )

    low = lax.broadcasted_iota(jnp.int32, (1, wide), 1) < side

    def pair(a, b):
        first = jnp.concatenate([a[:, :side], b[:, :side]], axis=1)
        second = jnp.concatenate([a[:, side:], b[:, side:]], axis=1)
        return first, second

    def whole(ref, count, ssem, rsem):
        ref = ref.at[pl.ds(0, count)]
        return remote(ref, ref, ssem, rsem, (0, 1, 0))

    loads[0].wait()
    own_runs = [lax.div(dest_ref[me * group + j], group) for j in range(group)]

    def block_for(run):
        found = jnp.int32(0)
        for j in range(group):
            found = jnp.where(own_runs[j] == run, j, found)
        return found

    def sar_columns(to_tile):
        if to_tile == 0:
            loads[1].wait()
        samples = jnp.concatenate(
            [
                sar_v[block_for(to_tile * halves + lax.rem(run + band, halves))]
                for run in range(halves)
            ],
            axis=0,
        )
        spectra = jnp.dot(samples, col_v[...], preferred_element_type=f32).astype(bf)
        for to in range(parts):
            at = slice(to * wide, (to + 1) * wide)
            first, second = pair(spectra[:lines, at], spectra[lines:, at])
            send_0[to_tile * parts + to] = first
            send_1[to_tile * parts + to] = second

    def sar_sends(turn, to_tile, shifts):
        for shift in shifts:
            to_half = lax.rem(half + shift, halves)
            for to_band in reversed(range(bands)):
                copy = sar_copy(turn, to_tile, to_half, jnp.int32(to_band))
                if shift:
                    copy.start()
                else:
                    pl.when((tile != to_tile) | (band != to_band))(copy.start)

    def opt_copy(turn, peer):
        _, to_half, to_band = place(*peer)
        return remote(
            opt_send.at[turn, to_half * bands + to_band],
            opt_in.at[turn, part],
            opt_ssem.at[turn],
            opt_rsem.at[turn],
            peer,
        )

    def to_core(copy_of, turn, to_band):
        return copy_of(turn, (0, 1, lax.rem(to_band + bands - band, bands)))

    def opt_sends(turn):
        for to_band in reversed(range(bands)):
            to_core(opt_copy, turn, to_band).start()
        opt_copy(turn, (0, 0, 1)).start()

    loads[3].wait()
    loads[2].wait()
    opt_spectra = [
        jnp.dot(opt_v[lax.rem(patch + band, patch_dev)], col_v[...], preferred_element_type=f32).astype(bf)
        for patch in range(patch_dev)
    ]
    for to in range(parts):
        at = slice(to * wide, (to + 1) * wide)
        first, second = pair(*[s[:, at] for s in opt_spectra])
        opt_send[0, to] = first
        opt_send[1, to] = second
    @pl.when(band == first_band)
    def _():
        pl.semaphore_wait(barrier, parts - 1)
        tell(near_sem, band=last_band)

    @pl.when(band == last_band)
    def _():
        pl.semaphore_wait(near_sem, 1)

    opt_sends(0)
    opt_sends(1)
    sar_columns(0)
    for i in (4, 5, 6, 7):
        loads[i].start()

    @pl.when(band == last_band)
    def _():
        pl.semaphore_wait(barrier, (tiles - 1) * parts)
        tell(far_sem, band=first_band)

    @pl.when(band == first_band)
    def _():
        pl.semaphore_wait(far_sem, 1)

    sar_sends(0, 0, (1, 0))
    for to_tile in range(1, tiles):
        sar_columns(to_tile)
        if to_tile > 1:
            sar_sends(0, to_tile, (1, 0))
        else:
            sar_sends(1, 0, (1, 0))
            sar_sends(0, 1, (1, 0))
    for to_tile in range(1, tiles):
        sar_sends(1, to_tile, (1, 0))
    arrived_0[source_at] = send_0[tile * parts + part]
    arrived_1[source_at] = send_1[tile * parts + part]
    for turn in range(2):
        opt_in[turn, part] = opt_send[turn, part]

    slot_of = []
    for run in range(halves):
        places = []
        for source in range(group):
            found = jnp.int32(0)
            for j in range(group):
                spot = dest_ref[source * group + j]
                found = jnp.where(
                    lax.div(spot, group) == tile * halves + run, lax.rem(spot, group), found
                )
            places.append(found)
        for slot in range(group):
            found = jnp.int32(0)
            for source in range(group):
                found = jnp.where(places[source] == slot, source, found)
            slot_of.append(found)

    spots = lax.broadcasted_iota(jnp.int32, (peak_count, extent), 1)
    ranks = lax.broadcasted_iota(jnp.int32, (peak_count, extent), 0)
    loads[5].wait()
    for which in range(2):
        wanted = jnp.zeros((peak_count, extent), jnp.int32)
        for j in range(peak_count):
            wanted = jnp.where(ranks == j, peaks_ref[0, which, j], wanted)
        spot_send[which * peak_count : (which + 1) * peak_count, :] = jnp.where(
            spots == wanted, 1.0, 0.0
        ).astype(bf)
    spot_copy = remote(spot_send, spot_recv, spot_ssem, spot_rsem, (0, 0, 1))
    spot_copy.start()

    lane = lax.broadcasted_iota(jnp.int32, (1, wide), 1)
    inner = lax.rem(lane, side)
    real_lane = inner < cols
    top = lax.broadcasted_iota(jnp.int32, (block, wide), 0) == 0
    edge_real = [((inner + part + turn) == 0) for turn in range(2)]
    edge_imag = [((jnp.abs(inner - cols) + part + turn) == 0) for turn in range(2)]
    weights = [
        jnp.where(edge_real[turn] | edge_imag[turn], 1.0, 2.0) * (0.5 * extent)
        for turn in range(2)
    ]

    def swapped(z):
        return pltpu.roll(z, side, 1)

    def crossed(z):
        return jnp.where(real_lane, pltpu.roll(z, wide - cols, 1), pltpu.roll(z, cols, 1))

    def turned(z):
        return jnp.where(real_lane, -pltpu.roll(z, wide - cols, 1), pltpu.roll(z, cols, 1))

    opt_energy = [0.0] * patch_dev

    def energy_of(even, odd, head, turn):
        shifted = even.astype(f32) - jnp.where(edge_real[turn], head * (2.0 / extent), 0.0)
        odd = odd.astype(f32)
        total = jnp.sum(shifted * shifted + odd * odd, axis=0, keepdims=True)
        return total * weights[turn]

    def optical(turn):
        whole(opt_in.at[turn], parts - 1, opt_ssem.at[turn], opt_rsem.at[turn]).wait_recv()
        real, imag = edge_real[turn], edge_imag[turn]
        pieces = [[opt_in[turn, run * bands + b] for b in range(bands)] for run in range(halves)]
        mixed = []
        for patch in range(patch_dev):
            near_x, far_x = [jnp.where(low, p[patch], p[1 - patch]) for p in pieces]
            mixed.append((near_x + far_x, near_x - far_x))
        for parity in range(2):
            plain = [jnp.where(imag, 0.0, m[parity]).astype(bf) for m in mixed]
            crossed_x = [
                jnp.where(real, 0.0, jnp.where(imag, m[parity], turned(m[parity]))).astype(bf)
                for m in mixed
            ]
            rows = jnp.dot(
                row_v[parity], jnp.concatenate(plain + crossed_x, axis=1), preferred_element_type=f32
            )
            for kind in range(2):
                for patch in range(patch_dev):
                    at = (kind * patch_dev + patch) * wide
                    opt_waves[turn, kind, patch, parity] = rows[:, at : at + wide]
        for patch in range(patch_dev):
            head = opt_waves[turn, 0, patch, 0, :block]
            opt_energy[patch] = opt_energy[patch] + energy_of(*mixed[patch], head[0:1], turn)
            opt_waves[turn, 0, patch, 0, :block] = jnp.where(real & top, 0.0, head)

    def fold(a, b, c, d):
        def halve(u, v):
            return jnp.where(low, u, v) + swapped(jnp.where(low, v, u))

        u, v = halve(a, c), halve(b, d)
        return (jnp.where(real_lane, u, v) + crossed(jnp.where(real_lane, v, u))).astype(bf)

    sar_energy = [0.0] * patch_dev

    def slant(turn):
        whole(arrived[turn], others, sar_ssem.at[turn], sar_rsem.at[turn]).wait_recv()
        for slot in range(group):
            patch, at = slot // per_patch, slot % per_patch * lines
            ends = []
            for run in range(halves):
                source = slot_of[run * group + slot] * bands
                piece = jnp.where(
                    low, arrived[turn][source + run], arrived[turn][source + 1 - run]
                )
                if patch != run:
                    piece = jnp.concatenate([piece[:, side:], piece[:, :side]], axis=1)
                ends.append(piece)
            sar_cols[turn, 0, patch, at : at + lines, :] = ends[0] + ends[1]
            sar_cols[turn, 1, patch, at : at + lines, :] = ends[0] - ends[1]
        for parity in range(2):
            both = [sar_cols[turn, parity, patch] for patch in range(patch_dev)]
            rows = jnp.dot(
                row_v[parity], jnp.concatenate(both, axis=1), preferred_element_type=f32
            )
            if parity == 0:
                for patch in range(patch_dev):
                    energy = energy_of(
                        sar_cols[turn, 0, patch],
                        sar_cols[turn, 1, patch],
                        rows[0:1, patch * wide : (patch + 1) * wide],
                        turn,
                    )
                    sar_energy[patch] = sar_energy[patch] + energy
            for b in range(points // 2 // block):
                at = slice(2 * b * block, (2 * b + 1) * block)
                lower = slice((2 * b + 1) * block, (2 * b + 2) * block)
                sums = []
                for patch in range(patch_dev):
                    yc, ys = [rows[i, patch * wide : (patch + 1) * wide] for i in (at, lower)]
                    zc, zs = [opt_waves[turn, 0, patch, parity, i] for i in (at, lower)]
                    tc, ts = [opt_waves[turn, 1, patch, parity, i] for i in (at, lower)]
                    zs_e, ts_e, zc_d, tc_d = zs, ts, zc, tc
                    if b == 0 and parity == 0:
                        zs_e, ts_e = jnp.where(top, 0.0, zs), jnp.where(top, 0.0, ts)
                        zc_d, tc_d = jnp.where(top, zs, zc), jnp.where(top, ts, tc)
                    sums.append(
                        (
                            zc * yc + zs_e * ys,
                            tc * yc + ts_e * ys,
                            zc_d * ys - zs_e * yc,
                            tc_d * ys - ts_e * yc,
                        )
                    )
                one, two = sums
                cross[turn, parity, at, :] = fold(one[0], one[1], two[0], two[1])
                cross[turn, parity, lower, :] = fold(one[2], one[3], two[2], two[3])

    def lag_copy(turn, peer):
        _, to_half, to_band = place(*peer)
        return remote(
            lag_send.at[turn, to_half * bands + to_band],
            lag_in.at[turn, part],
            lag_ssem.at[turn],
            lag_rsem.at[turn, peer[1]],
            peer,
        )

    def lag_sends(turn, shift):
        for swap in range(bands):
            if shift or swap:
                lag_copy(turn, (0, shift, swap)).start()

    def send_last():
        found = picked[0] * waves[0] + picked[1] * waves[1]
        for which, patch, ref in ((0, band, last_mine), (1, other_band, last_other)):
            mine = lax.div(lane, side) == patch
            ref[0:8, :] = jnp.zeros((8, wide), f32)
            ref[0:1, :] = jnp.where(patch == 0, opt_energy[0], opt_energy[1])
            ref[1:2, :] = jnp.where(patch == 0, sar_energy[0], sar_energy[1])
            value = jnp.where(mine, found[which * peak_count : (which + 1) * peak_count], 0.0)
            ref[8 : 8 + peak_count, :] = jnp.broadcast_to(
                jnp.sum(value, axis=1, keepdims=True), (peak_count, wide)
            )
        for peer in near:
            remote(
                last_other if peer[2] else last_mine, last_in.at[part], last_ssem, last_rsem, peer
            ).start()
        last_in[part] = last_mine[...]

    def spread(turn):
        even, odd = [
            jnp.dot(
                jnp.concatenate([spot_rows[parity], lag_v[parity]], axis=0),
                cross[turn, parity],
                preferred_element_type=f32,
            )
            for parity in range(2)
        ]
        picked[turn] = even[: 2 * peak_count] + odd[: 2 * peak_count]
        even, odd = even[2 * peak_count :], odd[2 * peak_count :]
        if turn:
            send_last()
        flip = jnp.where(half == 0, -1.0, 1.0)
        for shift, to_half in ((1, other_half), (0, half)):
            values = (even + odd * flip if shift else even - odd * flip).astype(bf)
            for patch, piece in enumerate(pair(values[: quarter // 2], values[quarter // 2 :])):
                lag_send[turn, to_half * bands + patch] = piece
            lag_sends(turn, shift)
        lag_in[turn, part] = lag_send[turn, part]

    def gather(turn, shift, first=False, last=False):
        from_half = lax.rem(half + shift, halves)
        if last:
            whole(last_in, parts - 1, last_ssem, last_rsem).wait_recv()
            scale = norm()
        count = bands if shift else bands - 1
        whole(lag_in.at[turn], count, lag_ssem.at[turn], lag_rsem.at[turn, shift]).wait_recv()
        upper, lower = pair(*[lag_in[turn, from_half * bands + b] for b in range(bands)])
        table = back_v[turn, pl.ds(pl.multiple_of(from_half * wide, wide), wide), :]
        values = jnp.dot(
            jnp.concatenate([upper, lower], axis=0), table, preferred_element_type=f32
        )
        if first:
            surface_ref[0] = values
        elif last:
            surface_ref[0] = (surface_ref[0] + values) * scale
        else:
            surface_ref[0] = surface_ref[0] + values

    pixels = extent * extent

    def norm():
        total = last_in[0]
        for i in range(1, parts):
            total = total + last_in[i]
        energies = jnp.sum(total[0:8], axis=1, keepdims=True) / (float(pixels) * bands * pixels)
        energies = energies + EPSILON
        scale = lax.rsqrt(bands * pixels * energies[0:1] * energies[1:2]) / pixels
        at = lax.broadcasted_iota(jnp.int32, (peak_count, wide), 1)
        rank = lax.broadcasted_iota(jnp.int32, (peak_count, wide), 0)
        row = jnp.where(at == rank, total[8 : 8 + peak_count], 0.0)
        peak_ref[...] = (jnp.sum(row, axis=0, keepdims=True) * scale)[:, :peak_count]
        return scale

    loads[4].wait()
    loads[6].wait()
    loads[7].wait()
    spot_copy.wait_recv()
    spots_all = jnp.concatenate([spot_send[:peak_count], spot_recv[:peak_count]], axis=0)
    lags_all = jnp.concatenate([spot_send[peak_count:], spot_recv[peak_count:]], axis=0)
    upper_spots, lower_spots = spots_all[:, :points], spots_all[:, points:]
    for parity in range(2):
        spots_now = upper_spots + lower_spots if parity == 0 else upper_spots - lower_spots
        spot_rows[parity] = jnp.dot(
            spots_now, lag_v[parity], preferred_element_type=f32
        ).astype(bf)
    for turn in range(2):
        rows_back = back_v[turn, pl.ds(pl.multiple_of(part * side, side), side), :]
        waves[turn] = lax.dot_general(
            lags_all,
            jnp.concatenate([rows_back, rows_back], axis=0),
            (((1,), (1,)), ((), ())),
            preferred_element_type=f32,
        )
    optical(0)
    optical(1)
    slant(0)
    spread(0)
    slant(1)
    spread(1)

    gather(0, 0, first=True)
    gather(1, 0)
    gather(0, 1)
    gather(1, 1, last=True)
    for turn in range(2):
        whole(send[turn], others, sar_ssem.at[turn], sar_rsem.at[turn]).wait_send()
        whole(opt_in.at[turn], parts - 1, opt_ssem.at[turn], opt_rsem.at[turn]).wait_send()
        whole(lag_in.at[turn], parts - 1, lag_ssem.at[turn], lag_rsem.at[turn, 0]).wait_send()
    whole(last_in, parts - 1, last_ssem, last_rsem).wait_send()
    spot_copy.wait_send()


def finish(surface_ref, peak_in, out_ref, peak_ref, sem):
    copies = [
        pltpu.make_async_copy(a, b, sem.at[i])
        for i, (a, b) in enumerate([(surface_ref, out_ref), (peak_in, peak_ref)])
    ]
    for copy in copies:
        copy.start()
    for copy in copies:
        copy.wait()


def fused(mesh, optical, sar, destination, peaks):
    tiles, halves, bands = mesh.shape["tile"], mesh.shape["half"], mesh.shape["band"]
    patch_dev, _, quarter, extent = optical.shape
    group = tiles * halves
    parts = halves * bands
    lines = sar.shape[1] // group
    peak_count = peaks.shape[2]
    wide = extent // parts
    points = extent // 2
    sizes = (tiles, halves, bands, patch_dev, quarter, extent, lines, peak_count)
    tables = dft_tables(extent, parts)
    bf, f32 = jnp.bfloat16, jnp.float32
    vmem = pltpu.VMEM
    dma = pltpu.SemaphoreType.DMA
    raw, values = pl.pallas_call(
        functools.partial(kernel, sizes),
        out_shape=(
            jax.ShapeDtypeStruct((1, quarter, extent), f32),
            jax.ShapeDtypeStruct((1, peak_count), f32),
        ),
        in_specs=[pl.BlockSpec(memory_space=pltpu.HBM)] * 8,
        out_specs=(pl.BlockSpec(memory_space=pltpu.VMEM), pl.BlockSpec(memory_space=pltpu.VMEM)),
        scratch_shapes=[
            pltpu.SMEM(destination.shape, jnp.int32),
            pltpu.SMEM(peaks.shape, jnp.int32),
            vmem((group, lines, extent), bf),
            vmem((patch_dev, quarter, extent), bf),
            vmem((extent, extent), bf),
            vmem((2, points, points), bf),
            vmem((2, points, points), bf),
            vmem((2, points, extent), bf),
            vmem((tiles * parts, lines, wide), bf),
            vmem((tiles * parts, lines, wide), bf),
            vmem((group * bands, lines, wide), bf),
            vmem((group * bands, lines, wide), bf),
            vmem((2, parts, quarter, wide), bf),
            vmem((2, parts, quarter, wide), bf),
            vmem((2, 2, patch_dev, 2, points, wide), f32),
            vmem((2, 2, patch_dev, points, wide), bf),
            vmem((2, 2, points, wide), bf),
            vmem((2, 2 * peak_count, points), bf),
            vmem((2, 2 * peak_count, wide), f32),
            vmem((2, 2 * peak_count, wide), f32),
            vmem((2, parts, quarter // 2, wide), bf),
            vmem((2, parts, quarter // 2, wide), bf),
            vmem((2 * peak_count, extent), bf),
            vmem((2 * peak_count, extent), bf),
            vmem((8 + peak_count, wide), f32),
            vmem((8 + peak_count, wide), f32),
            vmem((parts, 8 + peak_count, wide), f32),
            dma((8,)),
            dma((2,)),
            dma((2,)),
            dma((2,)),
            dma((2,)),
            dma((2,)),
            dma((2, 2)),
            dma,
            dma,
            dma,
            dma,
            pltpu.SemaphoreType.REGULAR,
            pltpu.SemaphoreType.REGULAR,
        ],
        compiler_params=pltpu.CompilerParams(
            collective_id=0, has_side_effects=True, vmem_limit_bytes=50 * 1024 * 1024
        ),
    )(
        *[
            pltpu.with_memory_space_constraint(x, pltpu.HBM)
            for x in (
                destination,
                peaks,
                sar.reshape(group, lines, extent),
                optical.reshape(patch_dev, quarter, extent),
                *[jnp.asarray(t) for t in tables],
            )
        ]
    )
    return pl.pallas_call(
        finish,
        out_shape=(
            jax.ShapeDtypeStruct((1, quarter, extent), f32),
            jax.ShapeDtypeStruct((1, peak_count), f32),
        ),
        in_specs=[pl.BlockSpec(memory_space=pltpu.VMEM)] * 2,
        out_specs=(pl.BlockSpec(memory_space=pltpu.HBM), pl.BlockSpec(memory_space=pltpu.HBM)),
        scratch_shapes=[dma((2,))],
    )(*[pltpu.with_memory_space_constraint(x, pltpu.VMEM) for x in (raw, values)])


def fits(mesh, optical, sar, peaks):
    group = mesh.shape["tile"] * mesh.shape["half"]
    patch_dev, local_bands, quarter, extent = optical.shape
    lines = sar.shape[1] // group
    return (
        mesh.shape["half"] == 2
        and mesh.shape["band"] == 2
        and patch_dev == 2
        and local_bands == 1
        and lines % 16 == 0
        and mesh.shape["tile"] > 1
        and quarter * 2 == extent
        and group * lines == patch_dev * quarter
        and extent % 512 == 0
        and peaks.shape[0] == 1
        and peaks.shape[2] % 8 == 0
    )


def solution(mesh):
    def local(optical, sar, destination, peaks):
        if fits(mesh, optical, sar, peaks):
            return fused(mesh, optical, sar, destination, peaks)
        return generic(optical, sar, destination, peaks)

    in_specs = (
        P(("scene", "tile"), "band", "half", None),
        P("band", ("scene", "tile", "half"), None),
        P("scene"),
        P(("scene", "tile", "band"), None, None),
    )
    out_specs = (P(("scene", "tile", "band"), "half", None), P(("scene", "tile", "band"), None))
    return jax.shard_map(local, mesh=mesh, in_specs=in_specs, out_specs=out_specs, check_vma=False)
```

```python
import functools
import math

import jax
import jax.numpy as jnp
import numpy as np
from jax import lax
from jax.experimental import pallas as pl
from jax.experimental.pallas import tpu as pltpu
from jax.sharding import PartitionSpec as P

MESH = pl.DeviceIdType.MESH

precise = lax.Precision.HIGHEST
EPSILON = 1e-06
BLOCK = 16


def fourier_tables(extent):
    places = jnp.arange(extent, dtype=jnp.int32)
    phases = places[:, None] * places[None, :] % extent
    angles = phases.astype(jnp.float32) * (2.0 * math.pi / extent)
    return (jnp.cos(angles), jnp.sin(angles))


def fourier_pair(table):
    upper = table.astype(jnp.bfloat16)
    lower = (table - upper.astype(jnp.float32)).astype(jnp.bfloat16)
    return (upper, lower)


def column_spectrum(samples, table_upper, table_lower):
    extent = samples.shape[-1]
    values = samples.reshape(-1, extent)
    spectrum = jnp.dot(values, table_upper, preferred_element_type=jnp.float32) + jnp.dot(
        values, table_lower, preferred_element_type=jnp.float32
    )
    return spectrum.astype(jnp.bfloat16).reshape(samples.shape[:-1] + (2 * extent,))


def row_spectrum(columns, table_upper, table_lower):
    line_count = columns.shape[-3]
    stacked = jnp.concatenate([columns[..., 0, :], columns[..., 1, :]], axis=-2)
    result = jnp.einsum("kr,...rc->...kc", table_upper, stacked, preferred_element_type=jnp.float32)
    result = result + jnp.einsum(
        "kr,...rc->...kc", table_lower, stacked, preferred_element_type=jnp.float32
    )
    return (result[..., :line_count, :], result[..., line_count:, :])


def relay_blocks(parcel):
    layout = parcel.shape
    merged = parcel.reshape(layout[:1] + (layout[1] * layout[2],) + layout[3:])
    arrived = lax.all_to_all(merged, ("tile", "half"), split_axis=1, concat_axis=1, tiled=True)
    return arrived.reshape(layout)


def generic(optical, sar, destination, peaks):
    tile_count = lax.axis_size("tile")
    half_count = lax.axis_size("half")
    band_count = lax.axis_size("band")
    group_size = tile_count * half_count
    patch_dev, local_bands, quarter, extent = optical.shape
    col_width = extent // half_count
    block_lines = sar.shape[1] // group_size
    band_total = local_bands * band_count
    pixel_count = extent * extent
    patch_total = patch_dev * tile_count
    kept_patches = patch_dev // band_count
    cosine_table, sine_table = fourier_tables(extent)
    col_upper, col_lower = fourier_pair(jnp.concatenate([cosine_table, -sine_table], axis=1))
    row_full = jnp.concatenate(
        [
            jnp.concatenate([cosine_table, sine_table], axis=1),
            jnp.concatenate([-sine_table, cosine_table], axis=1),
        ],
        axis=0,
    )
    row_upper, row_lower = fourier_pair(row_full)
    tile_at = lax.axis_index("tile")
    half_at = lax.axis_index("half")
    band_at = lax.axis_index("band")
    device_at = lax.axis_index(("tile", "half"))
    own_blocks = lax.dynamic_slice_in_dim(destination, device_at * group_size, group_size)
    send_order = jnp.argsort(own_blocks // group_size)
    inverse = (
        jnp.zeros_like(destination)
        .at[destination]
        .set(jnp.arange(destination.shape[0], dtype=jnp.int32))
    )
    opt_values = optical.astype(jnp.float32)
    opt_sums = jnp.sum(opt_values, axis=(2, 3))
    opt_squares = jnp.sum(opt_values * opt_values, axis=(2, 3))
    sar_values = sar.astype(jnp.float32).reshape(local_bands, group_size, block_lines * extent)
    sar_sums = jnp.sum(sar_values, axis=2)
    sar_squares = jnp.sum(sar_values * sar_values, axis=2)
    map_device = own_blocks // group_size
    map_patch = (
        map_device // half_count * patch_dev + own_blocks % group_size * block_lines // quarter
    )
    member = (map_patch[:, None] == jnp.arange(patch_total, dtype=jnp.int32)[None, :]).astype(
        jnp.float32
    )
    sar_stats = jnp.dot(
        jnp.stack([sar_sums, sar_squares]).reshape(2 * local_bands, group_size),
        member,
        precision=precise,
        preferred_element_type=jnp.float32,
    )
    statistics = jnp.zeros((2, 2, band_total, patch_total), jnp.float32)
    opt_part = jnp.transpose(jnp.stack([opt_sums, opt_squares]), (0, 2, 1))
    statistics = lax.dynamic_update_slice(
        statistics, opt_part[None], (0, 0, band_at * local_bands, tile_at * patch_dev)
    )
    statistics = lax.dynamic_update_slice(
        statistics,
        sar_stats.reshape(2, local_bands, patch_total)[None],
        (1, 0, band_at * local_bands, 0),
    )
    totals = lax.psum(statistics, ("tile", "half", "band"))
    centered = totals[:, 1] - totals[:, 0] * totals[:, 0] / pixel_count
    energy = jnp.sum(centered, axis=1) / (band_total * pixel_count)
    norm_scale = lax.rsqrt(band_total * pixel_count * (energy[0] + EPSILON) * (energy[1] + EPSILON))
    first_patch = tile_at * patch_dev + band_at * kept_patches
    norm_mine = lax.dynamic_slice_in_dim(norm_scale, first_patch, kept_patches)
    slant_spectra = column_spectrum(sar, col_upper, col_lower).reshape(
        local_bands, group_size, block_lines, 2, half_count, col_width
    )
    outgoing = jnp.take(slant_spectra, send_order, axis=1).reshape(
        local_bands, tile_count, half_count, block_lines, 2, half_count, col_width
    )
    outgoing = jnp.transpose(outgoing, (0, 1, 5, 2, 3, 4, 6))
    arrived = relay_blocks(outgoing).reshape(
        local_bands, group_size * half_count, block_lines, 2, col_width
    )
    sources = lax.dynamic_slice_in_dim(
        inverse, tile_at * half_count * group_size, half_count * group_size
    )
    slot_index = (
        sources // group_size * half_count
        + jnp.arange(half_count * group_size, dtype=jnp.int32) // group_size
    )
    placed = jnp.take(arrived, slot_index, axis=1).reshape(
        local_bands, half_count, patch_dev, quarter, 2, col_width
    )
    placed = jnp.transpose(placed, (2, 0, 1, 3, 4, 5)).reshape(
        patch_dev, local_bands, extent, 2, col_width
    )
    sar_real, sar_imag = row_spectrum(placed, row_upper, row_lower)
    spectra = column_spectrum(optical, col_upper, col_lower).reshape(
        patch_dev, local_bands, quarter, 2, half_count, col_width
    )
    real_part, imag_part = row_spectrum(
        jnp.squeeze(
            lax.all_to_all(spectra, "half", split_axis=4, concat_axis=2, tiled=True), axis=4
        ),
        row_upper,
        row_lower,
    )
    opt_real = real_part
    opt_imag = imag_part
    rows_at = jnp.arange(extent, dtype=jnp.int32)[:, None]
    cols_at = half_at * col_width + jnp.arange(col_width, dtype=jnp.int32)[None, :]
    keep_mask = jnp.where((rows_at == 0) & (cols_at == 0), 0.0, 1.0).astype(jnp.float32)
    opt_real = opt_real * keep_mask
    opt_imag = opt_imag * keep_mask
    sar_real = sar_real * keep_mask
    sar_imag = sar_imag * keep_mask
    cross_real = jnp.sum(opt_real * sar_real + opt_imag * sar_imag, axis=1)
    cross_imag = jnp.sum(opt_real * sar_imag - opt_imag * sar_real, axis=1)
    cross_term = jnp.stack([cross_real, cross_imag], axis=1)
    cross_sum = lax.psum_scatter(cross_term, "band", scatter_dimension=0, tiled=True)
    lag_real = (
        jnp.einsum("uk,pkc->puc", cosine_table, cross_sum[:, 0], precision=precise)
        - jnp.einsum("uk,pkc->puc", sine_table, cross_sum[:, 1], precision=precise)
    ) / extent
    lag_imag = (
        jnp.einsum("uk,pkc->puc", cosine_table, cross_sum[:, 1], precision=precise)
        + jnp.einsum("uk,pkc->puc", sine_table, cross_sum[:, 0], precision=precise)
    ) / extent
    lagged = jnp.stack([lag_real, lag_imag], axis=2).reshape(
        kept_patches, half_count, quarter, 2, col_width
    )
    pieces = lax.all_to_all(lagged, "half", split_axis=1, concat_axis=4, tiled=True)
    real_in = pieces[:, 0, :, 0, :]
    imag_in = pieces[:, 0, :, 1, :]
    correlation = (
        jnp.einsum("puc,cv->puv", real_in, cosine_table, precision=precise)
        - jnp.einsum("puc,cv->puv", imag_in, sine_table, precision=precise)
    ) / extent
    surface = correlation * norm_mine[:, None, None]
    local_rows = peaks[:, 0, :] - half_at * quarter
    row_hit = (
        local_rows[:, :, None] == jnp.arange(quarter, dtype=jnp.int32)[None, None, :]
    ).astype(jnp.float32)
    picked = jnp.einsum("pkr,prc->pkc", row_hit, surface, precision=precise)
    col_hit = (peaks[:, 1, :, None] == jnp.arange(extent, dtype=jnp.int32)[None, None, :]).astype(
        jnp.float32
    )
    local_values = jnp.sum(picked * col_hit, axis=2)
    peak_values = lax.psum(local_values, "half")
    return (surface, peak_values)


def dft_tables(extent, parts):
    points = extent // 2
    cols = points // parts // 2
    places = np.arange(extent)
    phases = (places[:, None] * places[None, :]) % extent
    cosine = np.cos(phases * (2.0 * np.pi / extent))
    sine = np.sin(phases * (2.0 * np.pi / extent))
    forward, backward = [], [[], []]
    for part in range(parts):
        for turn in range(2):
            first = (2 * part + turn) * cols
            span = slice(first, first + cols)
            real, imag = cosine[:, span].copy(), -sine[:, span]
            real_back, imag_back = 2.0 * cosine[span], -2.0 * sine[span]
            if first == 0:
                imag[:, 0] = cosine[:, points]
                real_back[0] = 1.0
                imag_back[0] = cosine[points]
            forward += [real, imag]
            backward[turn] += [real_back, imag_back]
    col_table = np.concatenate(forward, axis=1)
    back_table = np.stack([np.concatenate(b, axis=0) for b in backward])
    row_sine, lag_sine = sine[:points, :points].copy(), 2.0 * sine[:points, :points]
    row_cosine, lag_cosine = cosine[:points, :points], 2.0 * cosine[:points, :points]
    row_sine[0] = cosine[points, :points]
    lag_cosine[:, 0] = 1.0
    lag_sine[:, 0] = cosine[:points, points]


    def woven(a, b):
        both = np.stack([a.reshape(-1, BLOCK, points), b.reshape(-1, BLOCK, points)], axis=1)
        return both.reshape(points, points)

    row_table = np.stack([woven(row_cosine[i::2], row_sine[i::2]) for i in range(2)])
    lag_table = np.stack([woven(lag_cosine.T[i::2], lag_sine.T[i::2]).T for i in range(2)])
    return tuple(t.astype(jnp.bfloat16) for t in (col_table, row_table, lag_table, back_table))


def kernel(
    sizes,
    dest_hbm,
    peaks_hbm,
    sar_hbm,
    opt_hbm,
    col_hbm,
    row_hbm,
    lag_hbm,
    back_hbm,
    surface_ref,
    peak_ref,
    dest_ref,
    peaks_ref,
    sar_v,
    opt_v,
    col_v,
    row_v,
    lag_v,
    back_v,
    send_0,
    send_1,
    arrived_0,
    arrived_1,
    opt_send,
    opt_in,
    opt_waves,
    sar_cols,
    cross,
    spot_rows,
    waves,
    picked,
    lag_send,
    lag_in,
    spot_send,
    spot_recv,
    last_mine,
    last_other,
    last_in,
    load_sem,
    sar_ssem,
    sar_rsem,
    opt_ssem,
    opt_rsem,
    lag_ssem,
    lag_rsem,
    last_ssem,
    last_rsem,
    spot_ssem,
    spot_rsem,
    near_sem,
    far_sem,
):
    tiles, halves, bands, patch_dev, quarter, extent, lines, peak_count = sizes
    group = tiles * halves
    parts = halves * bands
    wide = extent // parts
    side = wide // 2
    cols = wide // 4
    points = extent // 2
    per_patch = group // patch_dev
    block = BLOCK
    send, arrived = (send_0, send_1), (arrived_0, arrived_1)
    f32, bf = jnp.float32, jnp.bfloat16
    tile, half, band = lax.axis_index("tile"), lax.axis_index("half"), lax.axis_index("band")
    me = tile * halves + half
    part = half * bands + band
    other_half = 1 - half
    other_band = 1 - band

    def place(step, shift, swap):
        return (
            lax.rem(tile + step, tiles),
            lax.rem(half + shift, halves),
            lax.rem(band + swap, bands),
        )

    def device(step, shift, swap):
        return dict(zip(("tile", "half", "band"), place(step, shift, swap)))

    others = tiles * parts - 1
    near = [(0, shift, swap) for shift in (1, 0) for swap in range(bands) if shift or swap]

    loads = [
        pltpu.make_async_copy(a, b, load_sem.at[i])
        for i, (a, b) in enumerate(
            [(dest_hbm, dest_ref), (sar_hbm, sar_v), (col_hbm, col_v), (opt_hbm, opt_v),
             (row_hbm, row_v), (peaks_hbm, peaks_ref), (lag_hbm, lag_v), (back_hbm, back_v)]
        )
    ]
    for i in (3, 2, 0, 1):
        loads[i].start()

    barrier = pltpu.get_barrier_semaphore()
    first_band, last_band = jnp.int32(0), jnp.int32(bands - 1)

    def tell(semaphore, **where):
        pl.semaphore_signal(semaphore, inc=1, device_id=where, device_id_type=MESH)

    for shift in range(1, halves):
        tell(barrier, half=lax.rem(half + shift, halves), band=first_band)
    pl.when(band != first_band)(lambda: tell(barrier, band=first_band))
    for step in sorted(range(1, tiles), key=lambda s: -min(s, tiles - s)):
        for shift in range(halves):
            tell(
                barrier,
                tile=lax.rem(tile + step, tiles),
                half=lax.rem(half + shift, halves),
                band=last_band,
            )

    def remote(src, dst, ssem, rsem, peer):
        return pltpu.make_async_remote_copy(
            src_ref=src,
            dst_ref=dst,
            send_sem=ssem,
            recv_sem=rsem,
            device_id=device(*peer),
            device_id_type=MESH,
        )

    source_at = me * bands + band

    def sar_copy(turn, to_tile, to_half, to_band):
        return pltpu.make_async_remote_copy(
            src_ref=send[turn].at[to_tile * parts + to_half * bands + to_band],
            dst_ref=arrived[turn].at[source_at],
            send_sem=sar_ssem.at[turn],
            recv_sem=sar_rsem.at[turn],
            device_id={"tile": to_tile, "half": to_half, "band": to_band},
            device_id_type=MESH,
        )

    low = lax.broadcasted_iota(jnp.int32, (1, wide), 1) < side

    def pair(a, b):
        first = jnp.concatenate([a[:, :side], b[:, :side]], axis=1)
        second = jnp.concatenate([a[:, side:], b[:, side:]], axis=1)
        return first, second

    def whole(ref, count, ssem, rsem):
        ref = ref.at[pl.ds(0, count)]
        return remote(ref, ref, ssem, rsem, (0, 1, 0))

    loads[0].wait()
    own_runs = [lax.div(dest_ref[me * group + j], group) for j in range(group)]

    def block_for(run):
        found = jnp.int32(0)
        for j in range(group):
            found = jnp.where(own_runs[j] == run, j, found)
        return found

    def sar_columns(to_tile):
        if to_tile == 0:
            loads[1].wait()
        samples = jnp.concatenate(
            [
                sar_v[block_for(to_tile * halves + lax.rem(run + band, halves))]
                for run in range(halves)
            ],
            axis=0,
        )
        spectra = jnp.dot(samples, col_v[...], preferred_element_type=f32).astype(bf)
        for to in range(parts):
            at = slice(to * wide, (to + 1) * wide)
            first, second = pair(spectra[:lines, at], spectra[lines:, at])
            send_0[to_tile * parts + to] = first
            send_1[to_tile * parts + to] = second

    def sar_sends(turn, to_tile, shifts):
        for shift in shifts:
            to_half = lax.rem(half + shift, halves)
            for to_band in reversed(range(bands)):
                copy = sar_copy(turn, to_tile, to_half, jnp.int32(to_band))
                if shift:
                    copy.start()
                else:
                    pl.when((tile != to_tile) | (band != to_band))(copy.start)

    def opt_copy(turn, peer):
        _, to_half, to_band = place(*peer)
        return remote(
            opt_send.at[turn, to_half * bands + to_band],
            opt_in.at[turn, part],
            opt_ssem.at[turn],
            opt_rsem.at[turn],
            peer,
        )

    def to_core(copy_of, turn, to_band):
        return copy_of(turn, (0, 1, lax.rem(to_band + bands - band, bands)))

    def opt_sends(turn):
        for to_band in reversed(range(bands)):
            to_core(opt_copy, turn, to_band).start()
        opt_copy(turn, (0, 0, 1)).start()

    loads[3].wait()
    loads[2].wait()
    opt_spectra = [
        jnp.dot(opt_v[lax.rem(patch + band, patch_dev)], col_v[...], preferred_element_type=f32).astype(bf)
        for patch in range(patch_dev)
    ]
    for to in range(parts):
        at = slice(to * wide, (to + 1) * wide)
        first, second = pair(*[s[:, at] for s in opt_spectra])
        opt_send[0, to] = first
        opt_send[1, to] = second
    @pl.when(band == first_band)
    def _():
        pl.semaphore_wait(barrier, parts - 1)
        tell(near_sem, band=last_band)

    @pl.when(band == last_band)
    def _():
        pl.semaphore_wait(near_sem, 1)

    opt_sends(0)
    opt_sends(1)
    sar_columns(0)
    for i in (4, 5, 6, 7):
        loads[i].start()

    @pl.when(band == last_band)
    def _():
        pl.semaphore_wait(barrier, (tiles - 1) * parts)
        tell(far_sem, band=first_band)

    @pl.when(band == first_band)
    def _():
        pl.semaphore_wait(far_sem, 1)

    sar_sends(0, 0, (1, 0))
    sar_sends(1, 0, (1, 0))
    sar_columns(1)
    sar_sends(0, 1, (1, 0))
    sar_columns(3)
    sar_sends(0, 3, (1, 0))
    sar_columns(2)
    sar_sends(0, 2, (1, 0))
    sar_sends(1, 1, (1, 0))
    sar_sends(1, 3, (1, 0))
    sar_sends(1, 2, (1, 0))
    arrived_0[source_at] = send_0[tile * parts + part]
    arrived_1[source_at] = send_1[tile * parts + part]
    for turn in range(2):
        opt_in[turn, part] = opt_send[turn, part]

    slot_of = []
    for run in range(halves):
        places = []
        for source in range(group):
            found = jnp.int32(0)
            for j in range(group):
                spot = dest_ref[source * group + j]
                found = jnp.where(
                    lax.div(spot, group) == tile * halves + run, lax.rem(spot, group), found
                )
            places.append(found)
        for slot in range(group):
            found = jnp.int32(0)
            for source in range(group):
                found = jnp.where(places[source] == slot, source, found)
            slot_of.append(found)

    spots = lax.broadcasted_iota(jnp.int32, (peak_count, extent), 1)
    ranks = lax.broadcasted_iota(jnp.int32, (peak_count, extent), 0)
    loads[5].wait()
    for which in range(2):
        wanted = jnp.zeros((peak_count, extent), jnp.int32)
        for j in range(peak_count):
            wanted = jnp.where(ranks == j, peaks_ref[0, which, j], wanted)
        spot_send[which * peak_count : (which + 1) * peak_count, :] = jnp.where(
            spots == wanted, 1.0, 0.0
        ).astype(bf)
    spot_copy = remote(spot_send, spot_recv, spot_ssem, spot_rsem, (0, 0, 1))
    spot_copy.start()

    lane = lax.broadcasted_iota(jnp.int32, (1, wide), 1)
    inner = lax.rem(lane, side)
    real_lane = inner < cols
    top = lax.broadcasted_iota(jnp.int32, (block, wide), 0) == 0
    edge_real = [((inner + part + turn) == 0) for turn in range(2)]
    edge_imag = [((jnp.abs(inner - cols) + part + turn) == 0) for turn in range(2)]
    weights = [
        jnp.where(edge_real[turn] | edge_imag[turn], 1.0, 2.0) * (0.5 * extent)
        for turn in range(2)
    ]

    def swapped(z):
        return pltpu.roll(z, side, 1)

    def crossed(z):
        return jnp.where(real_lane, pltpu.roll(z, wide - cols, 1), pltpu.roll(z, cols, 1))

    def turned(z):
        return jnp.where(real_lane, -pltpu.roll(z, wide - cols, 1), pltpu.roll(z, cols, 1))

    opt_energy = [0.0] * patch_dev

    def energy_of(even, odd, head, turn):
        shifted = even.astype(f32) - jnp.where(edge_real[turn], head * (2.0 / extent), 0.0)
        odd = odd.astype(f32)
        total = jnp.sum(shifted * shifted + odd * odd, axis=0, keepdims=True)
        return total * weights[turn]

    def optical(turn):
        whole(opt_in.at[turn], parts - 1, opt_ssem.at[turn], opt_rsem.at[turn]).wait_recv()
        real, imag = edge_real[turn], edge_imag[turn]
        pieces = [[opt_in[turn, run * bands + b] for b in range(bands)] for run in range(halves)]
        mixed = []
        for patch in range(patch_dev):
            near_x, far_x = [jnp.where(low, p[patch], p[1 - patch]) for p in pieces]
            mixed.append((near_x + far_x, near_x - far_x))
        for parity in range(2):
            plain = [jnp.where(imag, 0.0, m[parity]).astype(bf) for m in mixed]
            crossed_x = [
                jnp.where(real, 0.0, jnp.where(imag, m[parity], turned(m[parity]))).astype(bf)
                for m in mixed
            ]
            rows = jnp.dot(
                row_v[parity], jnp.concatenate(plain + crossed_x, axis=1), preferred_element_type=f32
            )
            for kind in range(2):
                for patch in range(patch_dev):
                    at = (kind * patch_dev + patch) * wide
                    opt_waves[turn, kind, patch, parity] = rows[:, at : at + wide]
        for patch in range(patch_dev):
            head = opt_waves[turn, 0, patch, 0, :block]
            opt_energy[patch] = opt_energy[patch] + energy_of(*mixed[patch], head[0:1], turn)
            opt_waves[turn, 0, patch, 0, :block] = jnp.where(real & top, 0.0, head)

    def fold(a, b, c, d):
        def halve(u, v):
            return jnp.where(low, u, v) + swapped(jnp.where(low, v, u))

        u, v = halve(a, c), halve(b, d)
        return (jnp.where(real_lane, u, v) + crossed(jnp.where(real_lane, v, u))).astype(bf)

    sar_energy = [0.0] * patch_dev

    def slant(turn):
        whole(arrived[turn], others, sar_ssem.at[turn], sar_rsem.at[turn]).wait_recv()
        for slot in range(group):
            patch, at = slot // per_patch, slot % per_patch * lines
            ends = []
            for run in range(halves):
                source = slot_of[run * group + slot] * bands
                piece = jnp.where(
                    low, arrived[turn][source + run], arrived[turn][source + 1 - run]
                )
                if patch != run:
                    piece = jnp.concatenate([piece[:, side:], piece[:, :side]], axis=1)
                ends.append(piece)
            sar_cols[turn, 0, patch, at : at + lines, :] = ends[0] + ends[1]
            sar_cols[turn, 1, patch, at : at + lines, :] = ends[0] - ends[1]
        for parity in range(2):
            both = [sar_cols[turn, parity, patch] for patch in range(patch_dev)]
            rows = jnp.dot(
                row_v[parity], jnp.concatenate(both, axis=1), preferred_element_type=f32
            )
            if parity == 0:
                for patch in range(patch_dev):
                    energy = energy_of(
                        sar_cols[turn, 0, patch],
                        sar_cols[turn, 1, patch],
                        rows[0:1, patch * wide : (patch + 1) * wide],
                        turn,
                    )
                    sar_energy[patch] = sar_energy[patch] + energy
            for b in range(points // 2 // block):
                at = slice(2 * b * block, (2 * b + 1) * block)
                lower = slice((2 * b + 1) * block, (2 * b + 2) * block)
                sums = []
                for patch in range(patch_dev):
                    yc, ys = [rows[i, patch * wide : (patch + 1) * wide] for i in (at, lower)]
                    zc, zs = [opt_waves[turn, 0, patch, parity, i] for i in (at, lower)]
                    tc, ts = [opt_waves[turn, 1, patch, parity, i] for i in (at, lower)]
                    zs_e, ts_e, zc_d, tc_d = zs, ts, zc, tc
                    if b == 0 and parity == 0:
                        zs_e, ts_e = jnp.where(top, 0.0, zs), jnp.where(top, 0.0, ts)
                        zc_d, tc_d = jnp.where(top, zs, zc), jnp.where(top, ts, tc)
                    sums.append(
                        (
                            zc * yc + zs_e * ys,
                            tc * yc + ts_e * ys,
                            zc_d * ys - zs_e * yc,
                            tc_d * ys - ts_e * yc,
                        )
                    )
                one, two = sums
                cross[turn, parity, at, :] = fold(one[0], one[1], two[0], two[1])
                cross[turn, parity, lower, :] = fold(one[2], one[3], two[2], two[3])

    def lag_copy(turn, peer):
        _, to_half, to_band = place(*peer)
        return remote(
            lag_send.at[turn, to_half * bands + to_band],
            lag_in.at[turn, part],
            lag_ssem.at[turn],
            lag_rsem.at[turn, peer[1]],
            peer,
        )

    def lag_sends(turn, shift):
        for swap in range(bands):
            if shift or swap:
                lag_copy(turn, (0, shift, swap)).start()

    def send_last():
        found = picked[0] * waves[0] + picked[1] * waves[1]
        for which, patch, ref in ((0, band, last_mine), (1, other_band, last_other)):
            mine = lax.div(lane, side) == patch
            ref[0:8, :] = jnp.zeros((8, wide), f32)
            ref[0:1, :] = jnp.where(patch == 0, opt_energy[0], opt_energy[1])
            ref[1:2, :] = jnp.where(patch == 0, sar_energy[0], sar_energy[1])
            value = jnp.where(mine, found[which * peak_count : (which + 1) * peak_count], 0.0)
            ref[8 : 8 + peak_count, :] = jnp.broadcast_to(
                jnp.sum(value, axis=1, keepdims=True), (peak_count, wide)
            )
        for peer in near:
            remote(
                last_other if peer[2] else last_mine, last_in.at[part], last_ssem, last_rsem, peer
            ).start()
        last_in[part] = last_mine[...]

    def spread(turn):
        even, odd = [
            jnp.dot(
                jnp.concatenate([spot_rows[parity], lag_v[parity]], axis=0),
                cross[turn, parity],
                preferred_element_type=f32,
            )
            for parity in range(2)
        ]
        picked[turn] = even[: 2 * peak_count] + odd[: 2 * peak_count]
        even, odd = even[2 * peak_count :], odd[2 * peak_count :]
        if turn:
            send_last()
        flip = jnp.where(half == 0, -1.0, 1.0)
        for shift, to_half in ((1, other_half), (0, half)):
            values = (even + odd * flip if shift else even - odd * flip).astype(bf)
            for patch, piece in enumerate(pair(values[: quarter // 2], values[quarter // 2 :])):
                lag_send[turn, to_half * bands + patch] = piece
            lag_sends(turn, shift)
        lag_in[turn, part] = lag_send[turn, part]

    def gather(turn, shift, first=False, last=False):
        from_half = lax.rem(half + shift, halves)
        if last:
            whole(last_in, parts - 1, last_ssem, last_rsem).wait_recv()
            scale = norm()
        count = bands if shift else bands - 1
        whole(lag_in.at[turn], count, lag_ssem.at[turn], lag_rsem.at[turn, shift]).wait_recv()
        upper, lower = pair(*[lag_in[turn, from_half * bands + b] for b in range(bands)])
        table = back_v[turn, pl.ds(pl.multiple_of(from_half * wide, wide), wide), :]
        values = jnp.dot(
            jnp.concatenate([upper, lower], axis=0), table, preferred_element_type=f32
        )
        if first:
            surface_ref[0] = values
        elif last:
            surface_ref[0] = (surface_ref[0] + values) * scale
        else:
            surface_ref[0] = surface_ref[0] + values

    pixels = extent * extent

    def norm():
        total = last_in[0]
        for i in range(1, parts):
            total = total + last_in[i]
        energies = jnp.sum(total[0:8], axis=1, keepdims=True) / (float(pixels) * bands * pixels)
        energies = energies + EPSILON
        scale = lax.rsqrt(bands * pixels * energies[0:1] * energies[1:2]) / pixels
        at = lax.broadcasted_iota(jnp.int32, (peak_count, wide), 1)
        rank = lax.broadcasted_iota(jnp.int32, (peak_count, wide), 0)
        row = jnp.where(at == rank, total[8 : 8 + peak_count], 0.0)
        peak_ref[...] = (jnp.sum(row, axis=0, keepdims=True) * scale)[:, :peak_count]
        return scale

    loads[4].wait()
    loads[6].wait()
    loads[7].wait()
    spot_copy.wait_recv()
    spots_all = jnp.concatenate([spot_send[:peak_count], spot_recv[:peak_count]], axis=0)
    lags_all = jnp.concatenate([spot_send[peak_count:], spot_recv[peak_count:]], axis=0)
    upper_spots, lower_spots = spots_all[:, :points], spots_all[:, points:]
    for parity in range(2):
        spots_now = upper_spots + lower_spots if parity == 0 else upper_spots - lower_spots
        spot_rows[parity] = jnp.dot(
            spots_now, lag_v[parity], preferred_element_type=f32
        ).astype(bf)
    for turn in range(2):
        rows_back = back_v[turn, pl.ds(pl.multiple_of(part * side, side), side), :]
        waves[turn] = lax.dot_general(
            lags_all,
            jnp.concatenate([rows_back, rows_back], axis=0),
            (((1,), (1,)), ((), ())),
            preferred_element_type=f32,
        )
    optical(0)
    optical(1)
    slant(0)
    spread(0)
    slant(1)
    spread(1)

    gather(0, 0, first=True)
    gather(1, 0)
    gather(0, 1)
    gather(1, 1, last=True)
    for turn in range(2):
        whole(send[turn], others, sar_ssem.at[turn], sar_rsem.at[turn]).wait_send()
        whole(opt_in.at[turn], parts - 1, opt_ssem.at[turn], opt_rsem.at[turn]).wait_send()
        whole(lag_in.at[turn], parts - 1, lag_ssem.at[turn], lag_rsem.at[turn, 0]).wait_send()
    whole(last_in, parts - 1, last_ssem, last_rsem).wait_send()
    spot_copy.wait_send()


def finish(surface_ref, peak_in, out_ref, peak_ref, sem):
    copies = [
        pltpu.make_async_copy(a, b, sem.at[i])
        for i, (a, b) in enumerate([(surface_ref, out_ref), (peak_in, peak_ref)])
    ]
    for copy in copies:
        copy.start()
    for copy in copies:
        copy.wait()


def fused(mesh, optical, sar, destination, peaks):
    tiles, halves, bands = mesh.shape["tile"], mesh.shape["half"], mesh.shape["band"]
    patch_dev, _, quarter, extent = optical.shape
    group = tiles * halves
    parts = halves * bands
    lines = sar.shape[1] // group
    peak_count = peaks.shape[2]
    wide = extent // parts
    points = extent // 2
    sizes = (tiles, halves, bands, patch_dev, quarter, extent, lines, peak_count)
    tables = dft_tables(extent, parts)
    bf, f32 = jnp.bfloat16, jnp.float32
    vmem = pltpu.VMEM
    dma = pltpu.SemaphoreType.DMA
    raw, values = pl.pallas_call(
        functools.partial(kernel, sizes),
        out_shape=(
            jax.ShapeDtypeStruct((1, quarter, extent), f32),
            jax.ShapeDtypeStruct((1, peak_count), f32),
        ),
        in_specs=[pl.BlockSpec(memory_space=pltpu.HBM)] * 8,
        out_specs=(pl.BlockSpec(memory_space=pltpu.VMEM), pl.BlockSpec(memory_space=pltpu.VMEM)),
        scratch_shapes=[
            pltpu.SMEM(destination.shape, jnp.int32),
            pltpu.SMEM(peaks.shape, jnp.int32),
            vmem((group, lines, extent), bf),
            vmem((patch_dev, quarter, extent), bf),
            vmem((extent, extent), bf),
            vmem((2, points, points), bf),
            vmem((2, points, points), bf),
            vmem((2, points, extent), bf),
            vmem((tiles * parts, lines, wide), bf),
            vmem((tiles * parts, lines, wide), bf),
            vmem((group * bands, lines, wide), bf),
            vmem((group * bands, lines, wide), bf),
            vmem((2, parts, quarter, wide), bf),
            vmem((2, parts, quarter, wide), bf),
            vmem((2, 2, patch_dev, 2, points, wide), f32),
            vmem((2, 2, patch_dev, points, wide), bf),
            vmem((2, 2, points, wide), bf),
            vmem((2, 2 * peak_count, points), bf),
            vmem((2, 2 * peak_count, wide), f32),
            vmem((2, 2 * peak_count, wide), f32),
            vmem((2, parts, quarter // 2, wide), bf),
            vmem((2, parts, quarter // 2, wide), bf),
            vmem((2 * peak_count, extent), bf),
            vmem((2 * peak_count, extent), bf),
            vmem((8 + peak_count, wide), f32),
            vmem((8 + peak_count, wide), f32),
            vmem((parts, 8 + peak_count, wide), f32),
            dma((8,)),
            dma((2,)),
            dma((2,)),
            dma((2,)),
            dma((2,)),
            dma((2,)),
            dma((2, 2)),
            dma,
            dma,
            dma,
            dma,
            pltpu.SemaphoreType.REGULAR,
            pltpu.SemaphoreType.REGULAR,
        ],
        compiler_params=pltpu.CompilerParams(
            collective_id=0, has_side_effects=True, vmem_limit_bytes=50 * 1024 * 1024
        ),
    )(
        *[
            pltpu.with_memory_space_constraint(x, pltpu.HBM)
            for x in (
                destination,
                peaks,
                sar.reshape(group, lines, extent),
                optical.reshape(patch_dev, quarter, extent),
                *[jnp.asarray(t) for t in tables],
            )
        ]
    )
    return pl.pallas_call(
        finish,
        out_shape=(
            jax.ShapeDtypeStruct((1, quarter, extent), f32),
            jax.ShapeDtypeStruct((1, peak_count), f32),
        ),
        in_specs=[pl.BlockSpec(memory_space=pltpu.VMEM)] * 2,
        out_specs=(pl.BlockSpec(memory_space=pltpu.HBM), pl.BlockSpec(memory_space=pltpu.HBM)),
        scratch_shapes=[dma((2,))],
    )(*[pltpu.with_memory_space_constraint(x, pltpu.VMEM) for x in (raw, values)])


def fits(mesh, optical, sar, peaks):
    group = mesh.shape["tile"] * mesh.shape["half"]
    patch_dev, local_bands, quarter, extent = optical.shape
    lines = sar.shape[1] // group
    return (
        mesh.shape["half"] == 2
        and mesh.shape["band"] == 2
        and patch_dev == 2
        and local_bands == 1
        and lines % 16 == 0
        and mesh.shape["tile"] > 1
        and quarter * 2 == extent
        and group * lines == patch_dev * quarter
        and extent % 512 == 0
        and peaks.shape[0] == 1
        and peaks.shape[2] % 8 == 0
    )


def solution(mesh):
    def local(optical, sar, destination, peaks):
        if fits(mesh, optical, sar, peaks):
            return fused(mesh, optical, sar, destination, peaks)
        return generic(optical, sar, destination, peaks)

    in_specs = (
        P(("scene", "tile"), "band", "half", None),
        P("band", ("scene", "tile", "half"), None),
        P("scene"),
        P(("scene", "tile", "band"), None, None),
    )
    out_specs = (P(("scene", "tile", "band"), "half", None), P(("scene", "tile", "band"), None))
    return jax.shard_map(local, mesh=mesh, in_specs=in_specs, out_specs=out_specs, check_vma=False)
```
